256 devices in a mesh: col: 32 (over z, y), row: 8 (over x, core).
Axes of the slice: x: 4, y: 4, z: 8, core: 2. Of those that a mesh axis runs over, the one named last changes fastest.
Arguments:
- psi_start: float32 [2048, 3, 3, 2048], P('row', None, None, 'col')
- left_env: float32 [2048, 5, 2048], P('row')
- right_env: float32 [2048, 5, 2048], P('col')
- mpo_pair: float32 [5, 5, 3, 3, 3, 3], replicated
Outputs:
- output 1: float32 [4], replicated
- output 2: float32 [4], replicated
- output 3: float32 [2048, 3, 3, 2048], P('row', None, None, 'col')
All inputs are finite; a program needn't handle non-finite values.
Results may differ from the reference program's by a relative error of at most 0.001.
Values sent between devices are 32-bit elements.
A program may use at most 768 MiB of HBM per device.

```python
import jax
import jax.numpy as jnp
from jax import lax

BOND_DIM = 2048
PHYS_DIM = 3
MPO_DIM = 5
LANCZOS_STEPS = 4

FULL_PREC = lax.Precision.HIGHEST


def symmetric_env(key_rand, key_diag):
    rand_part = jax.random.normal(key_rand, (BOND_DIM, MPO_DIM, BOND_DIM), jnp.float32)
    sym_part = (rand_part + jnp.transpose(rand_part, (2, 1, 0))) * (2.0 * BOND_DIM) ** -0.5
    diag_part = jax.random.normal(key_diag, (MPO_DIM,), jnp.float32)
    identity = jnp.eye(BOND_DIM, dtype=jnp.float32)
    return sym_part + identity[:, None, :] * diag_part[None, :, None]


def symmetric_mpo(key_rand, key_diag):
    loc_dim = PHYS_DIM * PHYS_DIM
    rand_part = jax.random.normal(key_rand, (MPO_DIM, MPO_DIM, loc_dim, loc_dim), jnp.float32)
    diag_part = jax.random.normal(key_diag, (MPO_DIM, MPO_DIM), jnp.float32)
    identity = jnp.eye(loc_dim, dtype=jnp.float32)
    sym_part = (rand_part + jnp.swapaxes(rand_part, 2, 3)) * 0.5 ** 0.5
    full_mpo = (sym_part + diag_part[:, :, None, None] * identity) / (MPO_DIM * PHYS_DIM)
    return full_mpo.reshape(MPO_DIM, MPO_DIM, PHYS_DIM, PHYS_DIM, PHYS_DIM, PHYS_DIM)


def setup_inputs(seed: int = 0) -> dict:
    key_list = jax.random.split(jax.random.key(seed), 7)
    psi_start = jax.random.normal(key_list[0], (BOND_DIM, PHYS_DIM, PHYS_DIM, BOND_DIM), jnp.float32)
    return {'psi_start': psi_start, 'left_env': symmetric_env(key_list[1], key_list[2]), 'right_env': symmetric_env(key_list[3], key_list[4]), 'mpo_pair': symmetric_mpo(key_list[5], key_list[6])}


def apply_ham(left_env, right_env, mpo_pair, vec_in):
    block_count = 8
    block_len = BOND_DIM // block_count
    left_blocks = jnp.transpose(left_env.reshape(BOND_DIM, MPO_DIM, block_count, block_len), (2, 0, 1, 3))

    def one_block(left_blk):
        stage_one = jnp.einsum('alc,asub->lcsub', left_blk.astype(jnp.float32), vec_in.astype(jnp.float32), precision=FULL_PREC)
        stage_two = jnp.einsum('lrsutq,lcsub->rctqb', mpo_pair.astype(jnp.float32), stage_one, precision=FULL_PREC)
        return jnp.einsum('rctqb,bre->ctqe', stage_two, right_env.astype(jnp.float32), precision=FULL_PREC)

    out_blocks = lax.map(one_block, left_blocks)
    return out_blocks.reshape(BOND_DIM, PHYS_DIM, PHYS_DIM, BOND_DIM)


def reference(psi_start, left_env, right_env, mpo_pair):
    num_elems = float(PHYS_DIM * PHYS_DIM * BOND_DIM * BOND_DIM)

    def mean_dot(left_vec, right_vec):
        return jnp.sum(left_vec * right_vec) / num_elems

    start_vec = psi_start * lax.rsqrt(mean_dot(psi_start, psi_start))

    def lanczos_step(carry, unused):
        prev_vec, cur_vec, prev_beta = carry
        h_vec = apply_ham(left_env, right_env, mpo_pair, cur_vec)
        alpha_j = mean_dot(cur_vec, h_vec)
        residual = h_vec - alpha_j * cur_vec - prev_beta * prev_vec
        beta_j = jnp.sqrt(mean_dot(residual, residual))
        return (cur_vec, residual / beta_j, beta_j), (alpha_j, beta_j)

    init_carry = (jnp.zeros_like(start_vec), start_vec, jnp.zeros((), jnp.float32))
    final_carry, history = lax.scan(lanczos_step, init_carry, None, length=LANCZOS_STEPS)
    return history[0], history[1], final_carry[1]
```

```python
import functools

import jax
import jax.numpy as jnp
from jax import lax
from jax.experimental import pallas as pl
from jax.experimental.pallas import tpu as pltpu
from jax.sharding import Mesh, PartitionSpec as P

LANCZOS_STEPS = 4
FULL_PREC = lax.Precision.HIGHEST
MESH_IDS = pl.DeviceIdType.MESH


def fine_mesh(mesh):
    col_size, row_size = mesh.shape['col'], mesh.shape['row']
    y_size, core_size = 4, 2
    shape = (col_size // y_size, y_size, row_size // core_size, core_size)
    return Mesh(mesh.devices.reshape(shape), ('z', 'y', 'x', 'k'))


def sum_kernel(sizes, val_ref, out_ref, held, slots, send_sem, recv_sem):
    n_z, n_y, n_x, n_k = sizes
    y, z = lax.axis_index('y'), lax.axis_index('z')
    xk = lax.axis_index('x') * n_k + lax.axis_index('k')

    phases = (
        (n_y, y, lambda i: {'y': i}),
        (n_x * n_k, xk, lambda i: {'x': i // n_k, 'k': lax.rem(i, n_k)}),
        (n_z, z, lambda i: {'z': i}),
    )
    barrier = pltpu.get_barrier_semaphore()
    total = 0
    for count, me, device in phases:
        for d in range(1, count):
            pl.semaphore_signal(barrier, inc=1, device_id=device(lax.rem(me + d, count)), device_id_type=MESH_IDS)
            total += 1
    pl.semaphore_wait(barrier, total)

    value = val_ref[...]
    base = 0
    for count, me, device in phases:
        held[base] = value
        copies = []
        for d in range(1, count):
            copy = pltpu.make_async_remote_copy(
                src_ref=held.at[base], dst_ref=slots.at[base + me],
                send_sem=send_sem.at[base + d], recv_sem=recv_sem.at[base + me],
                device_id=device(lax.rem(me + d, count)), device_id_type=MESH_IDS)
            copy.start()
            copies.append(copy)
        slots[base + me] = value
        for d in range(1, count):
            other = lax.rem(me + d, count)
            pltpu.make_async_remote_copy(
                src_ref=held.at[base], dst_ref=slots.at[base + other],
                send_sem=send_sem.at[base + d], recv_sem=recv_sem.at[base + other],
                device_id=device(other), device_id_type=MESH_IDS).wait_recv()
        value = slots[base]
        for i in range(1, count):
            value = value + slots[base + i]
        for copy in copies:
            copy.wait_send()
        base += count
    out_ref[...] = value


def all_sum(mesh, value):
    sizes = tuple(mesh.shape[name] for name in ('z', 'y', 'x', 'k'))
    slots = sizes[1] + sizes[2] * sizes[3] + sizes[0]
    tile = jnp.broadcast_to(value, (8, 128))
    out = pl.pallas_call(
        functools.partial(sum_kernel, sizes),
        out_shape=jax.ShapeDtypeStruct((8, 128), jnp.float32),
        in_specs=[pl.BlockSpec(memory_space=pltpu.VMEM)],
        out_specs=pl.BlockSpec(memory_space=pltpu.VMEM),
        scratch_shapes=[
            pltpu.VMEM((slots, 8, 128), jnp.float32),
            pltpu.VMEM((slots, 8, 128), jnp.float32),
            pltpu.SemaphoreType.DMA((slots,)),
            pltpu.SemaphoreType.DMA((slots,)),
        ],
        compiler_params=pltpu.CompilerParams(collective_id=0, has_side_effects=True),
    )(tile)
    return out[0, 0]


def solution(mesh):
    grid = fine_mesh(mesh)
    n_dev = grid.size
    n_y = grid.shape['y']

    def local_run(psi_blk, left_blk, right_blk, mpo_pair):
        num_elems = float(psi_blk.size * n_dev)
        rows = psi_blk.shape[0] // n_y
        mine = lax.axis_index('y') * rows
        left_rows = lax.dynamic_slice_in_dim(left_blk, mine, rows, 0)
        full_len = left_blk.shape[2]
        parts = (rows, left_blk.shape[1], grid.shape['x'], grid.shape['k'], n_y, rows)
        left_rows = left_rows.reshape(parts).transpose(0, 1, 4, 2, 3, 5).reshape(rows, left_blk.shape[1], full_len)
        right_rows = lax.all_gather(right_blk, 'y', axis=0, tiled=True)

        def mean_dot(left_vec, right_vec):
            return all_sum(grid, jnp.sum(left_vec * right_vec)) / num_elems

        def apply_ham(vec_blk):
            gathered = lax.all_gather(vec_blk, ('y', 'x', 'k'), axis=0, tiled=True)
            stage_one = jnp.einsum('cla,asub->lcsub', left_rows, gathered, precision=FULL_PREC, preferred_element_type=jnp.float32)
            stage_two = jnp.einsum('lrsutq,lcsub->rctqb', mpo_pair, stage_one, precision=FULL_PREC, preferred_element_type=jnp.float32)
            part_out = jnp.einsum('rctqb,bre->ctqe', stage_two, right_rows, precision=FULL_PREC, preferred_element_type=jnp.float32)
            return lax.psum_scatter(part_out, 'z', scatter_dimension=3, tiled=True)

        start = lax.all_to_all(psi_blk, 'y', 0, 3, tiled=True)
        cur_vec = start * lax.rsqrt(mean_dot(psi_blk, psi_blk))
        prev_vec = cur_vec
        alpha_list = []
        beta_list = []
        for step_idx in range(LANCZOS_STEPS):
            h_vec = apply_ham(cur_vec)
            alpha_j = mean_dot(cur_vec, h_vec)
            residual = h_vec - alpha_j * cur_vec
            if step_idx > 0:
                residual = residual - beta_list[-1] * prev_vec
            beta_j = jnp.sqrt(mean_dot(residual, residual))
            alpha_list.append(alpha_j)
            beta_list.append(beta_j)
            prev_vec = cur_vec
            cur_vec = residual / beta_j
        result = lax.all_to_all(cur_vec, 'y', 3, 0, tiled=True)
        return jnp.stack(alpha_list), jnp.stack(beta_list), result

    return jax.shard_map(
        local_run, mesh=grid,
        in_specs=(P(('x', 'k'), None, None, ('z', 'y')), P(('x', 'k'), None, None), P(('z', 'y'), None, None), P()),
        out_specs=(P(), P(), P(('x', 'k'), None, None, ('z', 'y'))), check_vma=False)
```

```python
import functools
import itertools

import jax
import jax.numpy as jnp
from jax import lax
from jax.experimental import pallas as pl
from jax.experimental.pallas import tpu as pltpu
from jax.sharding import Mesh, PartitionSpec as P

LANCZOS_STEPS = 4
FULL_PREC = lax.Precision.HIGHEST
MESH_IDS = pl.DeviceIdType.MESH
RING = 4
CORES = 2
PARTS = 4
NUM_SLOTS = RING * RING


def fine_mesh(mesh):
    shape = (mesh.shape['col'] // RING, RING, mesh.shape['row'] // CORES, CORES)
    return Mesh(mesh.devices.reshape(shape), ('z', 'y', 'x', 'k'))


def tree_axes(part):
    return ('x', 'y') if part < 2 else ('y', 'x')


def tree_sends(part, df, ds):
    first, second = tree_axes(part)
    way = 1 if part % 2 == 0 else -1
    sends = []
    if ds == 0:
        if df == 0:
            sends += [((first, 1), (part, 3, 0)), ((first, -1), (part, 1, 0))]
        if df == (3 if way == 1 else 1):
            sends.append(((first, way), (part, 2, 0)))
        sends += [((second, 1), (part, df, 3)), ((second, -1), (part, df, 1))]
    if ds == (3 if way == 1 else 1):
        sends.append(((second, way), (part, df, 2)))
    return sends


def slot_xy(message):
    part, df, ds = message
    return (df, ds) if part < 2 else (ds, df)


def gather_order():
    free = {link: 0.0 for link in itertools.product('xy', (1, -1))}
    arrival = {}

    def issue(now, sends):
        for link, message in sends:
            free[link] = max(free[link], now) + 1.0
            arrival[message] = free[link] + 0.6

    own = [tree_sends(part, 0, 0) for part in range(PARTS)]
    issue(0.0, [s for sends in own for s in sends[:2]])
    issue(0.0, [s for sends in own for s in sends[2:]])
    order = []
    while len(order) < 15 * PARTS:
        now, message = min((t, m) for m, t in arrival.items() if m not in order)
        order.append(message)
        issue(now, tree_sends(*message))
    return order


ORDER = gather_order()
NUM_MSGS = len(ORDER)
GROUPS = [ORDER[i:i + 4] for i in range(0, NUM_MSGS, 4)]
LAST_GROUP = {}
for group_idx, group in enumerate(GROUPS):
    for message in group:
        LAST_GROUP[slot_xy(message)] = group_idx
SLOTS = [(0, 0)] + sorted(LAST_GROUP, key=lambda xy: (LAST_GROUP[xy], xy))
CHUNK = 4
NUM_CHUNKS = NUM_SLOTS // CHUNK


def dot(lhs, rhs):
    return jnp.dot(lhs, rhs, precision=FULL_PREC, preferred_element_type=jnp.float32)


def lanczos_kernel(
        num_elems, num_z, psi_ref, left_ref, right_ref, w_ref, out_ref, scal_ref,
        gath, right_full, left_own, left_perm, acc, mid, ring, part_sum, h_buf, v_buf, turn_in, turn_mid, turn_out,
        red_held, red_slots,
        ag_send, ag_recv, sib_send, sib_recv, rs_send, rs_recv, red_send, red_recv, turn_send, turn_recv,
        env_send, env_recv, load_sem, ag_credit, rs_credit):
    phys, rows, cols = h_buf.shape[1:]
    bonds = right_full.shape[0]
    piece = rows // PARTS
    octs = rows // 8
    z, y, x, k = (lax.axis_index(name) for name in ('z', 'y', 'x', 'k'))
    xk = x * CORES + k
    other = 1 - k

    def step_to(axis, sign):
        pos = {'x': x, 'y': y}[axis]
        return {axis: lax.rem(pos + RING + sign, RING)}

    phases = (
        (num_z, z, lambda i: {'z': i}),
        (RING, y, lambda i: {'y': i}),
        (RING * CORES, xk, lambda i: {'x': i // CORES, 'k': lax.rem(i, CORES)}),
    )
    bases = (0, num_z, num_z + RING)
    barrier = pltpu.get_barrier_semaphore()
    total = 0
    for count, me, device in phases:
        for d in range(1, count):
            pl.semaphore_signal(barrier, inc=1, device_id=device(lax.rem(me + d, count)), device_id_type=MESH_IDS)
            total += 1

    load_left = pltpu.make_async_copy(
        left_ref.at[:, pl.ds(pl.multiple_of(y * rows, rows), rows), :], left_own, load_sem.at[0])
    load_left.start()
    own_rows = pl.multiple_of(y * rows, rows)
    load_right = pltpu.make_async_copy(right_ref, right_full.at[:, pl.ds(own_rows, rows), :], load_sem.at[1])
    load_right.start()
    pl.semaphore_wait(barrier, total)

    def sum_start(which, phase, value):
        count, me, device = phases[phase]
        red_held[which, phase] = value
        for d in range(1, count):
            pltpu.make_async_remote_copy(
                src_ref=red_held.at[which, phase], dst_ref=red_slots.at[which, bases[phase] + me],
                send_sem=red_send.at[which, bases[phase] + d], recv_sem=red_recv.at[which, bases[phase] + me],
                device_id=device(lax.rem(me + d, count)), device_id_type=MESH_IDS).start()
        red_slots[which, bases[phase] + me] = value

    def sum_finish(which, phase):
        count, me, device = phases[phase]
        for d in range(1, count):
            peer = lax.rem(me + d, count)
            copy = pltpu.make_async_remote_copy(
                src_ref=red_held.at[which, phase], dst_ref=red_slots.at[which, bases[phase] + peer],
                send_sem=red_send.at[which, bases[phase] + d], recv_sem=red_recv.at[which, bases[phase] + peer],
                device_id=device(peer), device_id_type=MESH_IDS)
            copy.wait_send()
            copy.wait_recv()
        value = red_slots[which, bases[phase]]
        for i in range(1, count):
            value = value + red_slots[which, bases[phase] + i]
        return value

    def mean_of(value):
        return jnp.broadcast_to(jnp.sum(value, axis=(0, 1), keepdims=True) * (1.0 / num_elems), (8, 128))

    def fold(values):
        lanes = values.reshape(-1, 8, cols).sum(0)
        tile = lanes[:, :128]
        for c in range(128, cols, 128):
            tile = tile + lanes[:, c:c + 128]
        return tile

    def gather_copy(link, message):
        axis, sign = link
        dx, dy = slot_xy(message)
        sx = (dx + sign) % RING if axis == 'x' else dx
        sy = (dy + sign) % RING if axis == 'y' else dy
        index = ORDER.index(message)
        span = pl.ds(message[0] * piece, piece)
        return pltpu.make_async_remote_copy(
            src_ref=gath.at[0, SLOTS.index((sx, sy)), :, span, :], dst_ref=gath.at[0, SLOTS.index((dx, dy)), :, span, :],
            send_sem=ag_send.at[index], recv_sem=ag_recv.at[index],
            device_id=step_to(axis, sign), device_id_type=MESH_IDS)

    all_sends = {}
    for message in [(part, 0, 0) for part in range(PARTS)] + ORDER:
        for link, sent in tree_sends(*message):
            all_sends[sent] = link

    def sibling_copy(slot):
        return pltpu.make_async_remote_copy(
            src_ref=gath.at[0, slot], dst_ref=gath.at[1, slot],
            send_sem=sib_send.at[slot], recv_sem=sib_recv.at[slot],
            device_id={'k': other}, device_id_type=MESH_IDS)

    def send_own(part):
        for link, sent in tree_sends(part, 0, 0):
            gather_copy(link, sent).start()

    def turn_copy(src, dst, index, d, device):
        return pltpu.make_async_remote_copy(
            src_ref=src, dst_ref=dst, send_sem=turn_send.at[d], recv_sem=turn_recv.at[index],
            device_id=device, device_id_type=MESH_IDS)

    per_tile = 128 // rows
    for d in range(1, RING):
        peer = lax.rem(y + d, RING)
        lanes = pl.ds(pl.multiple_of((peer // per_tile) * 128, 128), 128)
        turn_copy(psi_ref.at[:, :, lanes], turn_in.at[y], y, d, {'y': peer}).start()
    turn_in[y] = psi_ref[:, :, pl.ds(pl.multiple_of((y // per_tile) * 128, 128), 128)]
    h_buf[1] = jnp.zeros(h_buf.shape[1:], jnp.float32)
    v_buf[...] = jnp.zeros(v_buf.shape, jnp.float32)
    for d in range(1, RING):
        peer = lax.rem(y + d, RING)
        copy = turn_copy(psi_ref.at[:, :, pl.ds(0, 128)], turn_in.at[peer], peer, d, {'y': peer})
        copy.wait_send()
        copy.wait_recv()
    sub = pl.ds(pl.multiple_of(lax.rem(y, per_tile) * rows, rows), rows)

    def turn_body(p, c):
        block = jnp.concatenate([turn_in[i, p] for i in range(RING)], axis=0)
        turn_mid[0] = jnp.transpose(block)
        mine = turn_mid[0, sub, :]
        h_buf[0, p] = mine
        gath[0, 0, p] = mine
        return c

    lax.fori_loop(0, phys, turn_body, 0)
    for part in range(PARTS):
        send_own(part)
    sibling_copy(0).start()

    load_left.wait()
    bonds_l = left_own.shape[0]
    lane = lax.broadcasted_iota(jnp.int32, (bonds_l * rows, 128), 1)
    for tile in range(left_perm.shape[1] // 128):
        halves = []
        for h in range(2):
            column = tile * 128 + h * rows
            chunk, rest = divmod(column, CHUNK * CORES * rows)
            dk, rest = divmod(rest, CHUNK * rows)
            dx, dy = SLOTS[chunk * CHUNK + rest // rows]
            block = (lax.rem(x + dx, RING) * CORES + lax.rem(k + dk, CORES)) * RING + lax.rem(y + dy, RING)
            first = pl.multiple_of((block // 2) * 128, 128)
            values = left_own[:, :, pl.ds(first, 128)].reshape(bonds_l * rows, 128)
            halves.append(jnp.where(lax.rem(block, 2) == h, values, pltpu.roll(values, rows, 1)))
        left_perm[:, tile * 128:(tile + 1) * 128] = jnp.where(lane < rows, halves[0], halves[1])

    def stage_one(chunk, lo, hi):
        def body(p, c):
            rhs = jnp.concatenate(
                [gath[dk, chunk * CHUNK + i, p] for dk in range(CORES) for i in range(CHUNK)], axis=0)
            depth = CHUNK * CORES * rows
            res = dot(left_perm[:, chunk * depth:(chunk + 1) * depth], rhs).reshape(bonds_l, octs, 8, cols)
            if chunk == 0:
                acc[p] = res
            else:
                acc[p] = acc[p] + res
            return c
        lax.fori_loop(lo, hi, body, 0)

    def wait_sibling(chunk):
        for i in range(CHUNK):
            sibling_copy(chunk * CHUNK + i).wait_recv()

    half = rows // 2
    quarter = rows // 4

    def env_view(row, count, i):
        off = jnp.where(lax.rem(i, 2) == 0, -(i // 2 + 1), i // 2 + 1) * jnp.where(i == num_z - 1, 0, 1)
        block = lax.rem(z + num_z + off, num_z)
        return right_full.at[:, pl.ds(pl.multiple_of(row, 8), count), pl.ds(pl.multiple_of(block * cols, cols), cols)]

    def env_copy(kind, i, row, count, device):
        view = env_view(row, count, i)
        return pltpu.make_async_remote_copy(
            src_ref=view, dst_ref=view, send_sem=env_send.at[kind, i], recv_sem=env_recv.at[kind, i],
            device_id=device, device_id_type=MESH_IDS)

    up, down, far = (lax.rem(y + d, RING) for d in (1, 3, 2))

    def env_row(owner, core):
        return owner * rows + core * half

    def env_start(i, c):
        env_copy(0, i, env_row(y, k), half, {'y': up}).start()
        env_copy(1, i, env_row(y, k), half, {'y': down}).start()
        return c

    def env_pass(i, c):
        env_copy(0, i, env_row(down, k), half, {'y': up}).wait_recv()
        env_copy(2, i, env_row(down, k), quarter, {'y': up}).start()
        env_copy(4, i, env_row(down, k), half, {'k': other}).start()
        env_copy(1, i, env_row(up, k), half, {'y': down}).wait_recv()
        env_copy(3, i, env_row(up, k) + quarter, quarter, {'y': down}).start()
        env_copy(5, i, env_row(up, k), half, {'k': other}).start()
        return c

    def env_end(i, c):
        env_copy(2, i, env_row(far, k), quarter, {'y': up}).wait_recv()
        env_copy(3, i, env_row(far, k) + quarter, quarter, {'y': down}).wait_recv()
        env_copy(6, i, env_row(far, k), half, {'k': other}).start()
        return c

    def env_done(i, c):
        env_copy(4, i, env_row(down, other), half, {'k': other}).wait_recv()
        env_copy(5, i, env_row(up, other), half, {'k': other}).wait_recv()
        env_copy(6, i, env_row(far, other), half, {'k': other}).wait_recv()
        for kind, row, count in ((0, env_row(y, k), half), (1, env_row(y, k), half), (2, env_row(down, k), quarter),
                                 (3, env_row(up, k) + quarter, quarter), (4, env_row(down, k), half),
                                 (5, env_row(up, k), half), (6, env_row(far, k), half)):
            env_copy(kind, i, row, count, {'k': other}).wait_send()
        return c

    def way(s):
        return 1 - 2 * lax.rem(s, 2)

    def ring_block(s, t):
        return lax.rem(z + 2 * num_z - way(s) * (1 + t), num_z)

    def ring_copy(s, t):
        return pltpu.make_async_remote_copy(
            src_ref=ring.at[s, t], dst_ref=ring.at[s, t + 1], send_sem=rs_send.at[s, t], recv_sem=rs_recv.at[s, t + 1],
            device_id={'z': lax.rem(z + num_z + way(s), num_z)}, device_id_type=MESH_IDS)

    per_part = piece // 8

    def last_stage(s, t):
        lhs = mid[:, pl.ds(s * per_part, per_part)].reshape(phys * piece, bonds * cols)
        first = pl.multiple_of(ring_block(s, t) * cols, cols)
        rhs = right_full[:, :, pl.ds(first, cols)].reshape(bonds * cols, cols)
        return dot(lhs, rhs).reshape(phys, piece, cols)

    def ring_first(s, c):
        def middle(i, c2):
            o = s * per_part + i
            res = dot(w_ref[...], acc[:, :, o].reshape(phys * bonds_l * 8, cols)).reshape(bonds, phys, 8, cols)
            for r in range(bonds):
                mid[:, o, :, r * cols:(r + 1) * cols] = res[r]
            return c2
        lax.fori_loop(0, per_part, middle, 0)
        ring[s, 0] = last_stage(s, 0)
        ring_copy(s, 0).start()
        return c

    def ring_second(s, c):
        part_sum[s] = last_stage(s, 1)
        return c

    def ring_hop(i, c):
        t, s = 1 + i // PARTS, lax.rem(i, PARTS)
        ring_copy(s, t - 1).wait_recv()
        ring[s, t] = ring[s, t] + part_sum[s]
        ring_copy(s, t).start()
        part_sum[s] = last_stage(s, t + 1)
        return c

    def new_direction(cur, alpha, beta_prev):
        nxt = 1 - cur
        a, b = alpha[0:1, 0:1], beta_prev[0:1, 0:1]
        total = jnp.zeros((8, 128), jnp.float32)
        for p in range(phys):
            w = h_buf[cur, p] - a * v_buf[cur, p] - b * v_buf[nxt, p]
            v_buf[nxt, p] = w
            total = total + fold(w * w)
        return total

    def step(j, carry):
        alpha_part, beta_prev = carry
        cur = lax.rem(j, 2)
        nxt = 1 - cur
        sum_start(0, 0, alpha_part)
        state = {}
        for g, group in enumerate(GROUPS):
            for message in group:
                gather_copy(all_sends[message], message).wait_recv()
                for link, sent in tree_sends(*message):
                    gather_copy(link, sent).start()
            for xy, last in LAST_GROUP.items():
                if last == g:
                    sibling_copy(SLOTS.index(xy)).start()
            if g == 1:
                sum_start(0, 1, sum_finish(0, 0))
            if g == 4:
                wait_sibling(0)
            if g in (4, 5, 6):
                stage_one(0, (g - 4) * phys // 3, (g - 3) * phys // 3)
            if g == 6:
                sum_start(0, 2, sum_finish(0, 1))
            if g == 9:
                wait_sibling(1)
            if g in (9, 10, 11):
                stage_one(1, (g - 9) * phys // 3, (g - 8) * phys // 3)
            if g == 11:
                alpha = mean_of(sum_finish(0, 2))
                scal_ref[0, j] = alpha
                sum_start(1, 0, new_direction(cur, alpha, beta_prev))
            if g == 13:
                wait_sibling(2)
                stage_one(2, 0, phys // 3)
                sum_start(1, 1, sum_finish(1, 0))

        @pl.when(j == 0)
        def _():
            load_right.wait()
            lax.fori_loop(0, num_z, env_start, 0)

        stage_one(2, phys // 3, phys)
        wait_sibling(3)
        stage_one(3, 0, phys)
        for message, link in all_sends.items():
            gather_copy(link, message).wait_send()
        for slot in range(NUM_SLOTS):
            sibling_copy(slot).wait_send()

        @pl.when(j < LANCZOS_STEPS - 1)
        def _():
            for axis, sign in itertools.product('xy', (1, -1)):
                pl.semaphore_signal(ag_credit, inc=1, device_id=step_to(axis, sign), device_id_type=MESH_IDS)
            pl.semaphore_signal(ag_credit, inc=1, device_id={'k': other}, device_id_type=MESH_IDS)

        @pl.when(j == 0)
        def _():
            lax.fori_loop(0, num_z, env_pass, 0)
            lax.fori_loop(0, num_z, env_end, 0)
            lax.fori_loop(0, num_z, env_done, 0)

        @pl.when(j > 0)
        def _():
            pl.semaphore_wait(rs_credit, 2)

        lax.fori_loop(0, PARTS, ring_first, 0)
        sum_start(1, 2, sum_finish(1, 1))
        lax.fori_loop(0, PARTS, ring_second, 0)
        lax.fori_loop(0, PARTS * (num_z - 2), ring_hop, 0)
        beta = jnp.sqrt(mean_of(sum_finish(1, 2)))
        scal_ref[1, j] = beta

        @pl.when(j < LANCZOS_STEPS - 1)
        def _():
            pl.semaphore_wait(ag_credit, 5)

        alpha = scal_ref[0, j]
        a, b, inv = alpha[0:1, 0:1], beta_prev[0:1, 0:1], (1.0 / beta)[0:1, 0:1]
        new_part = jnp.zeros((8, 128), jnp.float32)
        for s in range(PARTS):
            ring_copy(s, num_z - 2).wait_recv()
            span = slice(s * piece, (s + 1) * piece)
            for p in range(phys):
                g_new = ring[s, num_z - 1, p] + part_sum[s, p]
                h_new = (g_new - a * h_buf[cur, p, span, :] - b * h_buf[nxt, p, span, :]) * inv
                v_new = v_buf[nxt, p, span, :] * inv
                h_buf[nxt, p, span, :] = h_new
                gath[0, 0, p, span, :] = h_new
                v_buf[nxt, p, span, :] = v_new
                new_part = new_part + fold(v_new * h_new)

            @pl.when(j < LANCZOS_STEPS - 1)
            def _():
                send_own(s)

        @pl.when(j < LANCZOS_STEPS - 1)
        def _():
            sibling_copy(0).start()

        for s in range(PARTS):
            for t in range(num_z - 1):
                ring_copy(s, t).wait_send()

        @pl.when(j < LANCZOS_STEPS - 1)
        def _():
            for sign in (1, num_z - 1):
                pl.semaphore_signal(
                    rs_credit, inc=1, device_id={'z': lax.rem(z + sign, num_z)}, device_id_type=MESH_IDS)

        return new_part, jnp.where(j > 0, beta, 0.0)

    zero = jnp.zeros((8, 128), jnp.float32)
    alpha_part, beta_prev = lax.fori_loop(0, LANCZOS_STEPS, step, (zero, zero))

    def sum_now(which, value):
        for phase in range(3):
            sum_start(which, phase, value)
            value = sum_finish(which, phase)
        return mean_of(value)

    cur = LANCZOS_STEPS % 2
    alpha = sum_now(0, alpha_part)
    scal_ref[0, LANCZOS_STEPS] = alpha
    beta = jnp.sqrt(sum_now(1, new_direction(cur, alpha, beta_prev)))
    scal_ref[1, LANCZOS_STEPS] = beta
    inv = (1.0 / beta)[0:1, 0:1]
    turn_mid[0] = jnp.zeros((128, RING * rows), jnp.float32)

    def unturn_body(p, c):
        turn_mid[0, sub, :] = v_buf[1 - cur, p] * inv
        turned = jnp.transpose(turn_mid[0])
        for i in range(RING):
            turn_out[i, p] = turned[i * rows:(i + 1) * rows, :]
        return c

    lax.fori_loop(0, phys, unturn_body, 0)
    for d in range(1, RING):
        peer = lax.rem(y + d, RING)
        turn_copy(turn_out.at[peer], turn_in.at[y], y, d, {'y': peer}).start()
    turn_in[y] = turn_out[y]
    for d in range(1, RING):
        peer = lax.rem(y + d, RING)
        copy = turn_copy(turn_out.at[peer], turn_in.at[peer], peer, d, {'y': peer})
        copy.wait_send()
        copy.wait_recv()
    first_lanes = lax.broadcasted_iota(jnp.int32, (phys, rows, 128), 2) < rows
    for pair in range(RING // per_tile):
        out_ref[:, :, pair * 128:(pair + 1) * 128] = jnp.where(first_lanes, turn_in[2 * pair], turn_in[2 * pair + 1])


def solution(mesh):
    grid = fine_mesh(mesh)
    num_z = grid.shape['z']

    def local_run(psi_blk, left_blk, right_blk, mpo_pair):
        full_rows, n_s, n_u, local_cols = psi_blk.shape
        phys = n_s * n_u
        rows = full_rows // RING
        cols = local_cols * RING
        bonds_l, bonds_r = left_blk.shape[1], right_blk.shape[1]
        full_a, full_b = left_blk.shape[2], right_blk.shape[2]
        psi = psi_blk.transpose(1, 2, 3, 0).reshape(phys, local_cols, full_rows)
        left = left_blk.transpose(1, 0, 2)
        right = right_blk.transpose(1, 0, 2)
        w_flat = mpo_pair.reshape(bonds_l, bonds_r, phys, phys).transpose(1, 3, 2, 0)
        w_flat = w_flat.reshape(bonds_r * phys, 1, phys * bonds_l, 1) * jnp.eye(8, dtype=jnp.float32)[None, :, None, :]
        w_flat = w_flat.reshape(bonds_r * phys * 8, phys * bonds_l * 8)
        red = num_z + RING + RING * CORES
        f32 = jnp.float32
        out, scal = pl.pallas_call(
            functools.partial(lanczos_kernel, float(psi_blk.size * grid.size), num_z),
            out_shape=(
                jax.ShapeDtypeStruct((phys, local_cols, full_rows), f32),
                jax.ShapeDtypeStruct((2, LANCZOS_STEPS + 1, 8, 128), f32),
            ),
            in_specs=[
                pl.BlockSpec(memory_space=pltpu.VMEM),
                pl.BlockSpec(memory_space=pl.ANY),
                pl.BlockSpec(memory_space=pl.ANY),
                pl.BlockSpec(memory_space=pltpu.VMEM),
            ],
            out_specs=(pl.BlockSpec(memory_space=pltpu.VMEM), pl.BlockSpec(memory_space=pltpu.VMEM)),
            scratch_shapes=[
                pltpu.VMEM((CORES, NUM_SLOTS, phys, rows, cols), f32),
                pltpu.VMEM((bonds_r, cols, full_b), f32),
                pltpu.VMEM((bonds_l, rows, full_a), f32),
                pltpu.VMEM((bonds_l * rows, full_a), f32),
                pltpu.VMEM((phys, bonds_l, rows // 8, 8, cols), f32),
                pltpu.VMEM((phys, rows // 8, 8, bonds_r * cols), f32),
                pltpu.VMEM((PARTS, num_z, phys, rows // PARTS, cols), f32),
                pltpu.VMEM((PARTS, phys, rows // PARTS, cols), f32),
                pltpu.VMEM((2, phys, rows, cols), f32),
                pltpu.VMEM((2, phys, rows, cols), f32),
                pltpu.VMEM((RING, phys, local_cols, 128), f32),
                pltpu.VMEM((1, 128, cols), f32),
                pltpu.VMEM((RING, phys, local_cols, 128), f32),
                pltpu.VMEM((2, 3, 8, 128), f32),
                pltpu.VMEM((2, red, 8, 128), f32),
                pltpu.SemaphoreType.DMA((NUM_MSGS,)),
                pltpu.SemaphoreType.DMA((NUM_MSGS,)),
                pltpu.SemaphoreType.DMA((NUM_SLOTS,)),
                pltpu.SemaphoreType.DMA((NUM_SLOTS,)),
                pltpu.SemaphoreType.DMA((PARTS, num_z)),
                pltpu.SemaphoreType.DMA((PARTS, num_z)),
                pltpu.SemaphoreType.DMA((2, red)),
                pltpu.SemaphoreType.DMA((2, red)),
                pltpu.SemaphoreType.DMA((RING,)),
                pltpu.SemaphoreType.DMA((RING,)),
                pltpu.SemaphoreType.DMA((7, num_z)),
                pltpu.SemaphoreType.DMA((7, num_z)),
                pltpu.SemaphoreType.DMA((2,)),
                pltpu.SemaphoreType.REGULAR,
                pltpu.SemaphoreType.REGULAR,
            ],
            compiler_params=pltpu.CompilerParams(
                collective_id=0, has_side_effects=True, vmem_limit_bytes=67043328),
        )(psi, left, right, w_flat)
        result = out.reshape(n_s, n_u, local_cols, full_rows).transpose(3, 0, 1, 2)
        return scal[0, 1:, 0, 0], scal[1, 1:, 0, 0], result

    return jax.shard_map(
        local_run, mesh=grid,
        in_specs=(P(('x', 'k'), None, None, ('z', 'y')), P(('x', 'k'), None, None), P(('z', 'y'), None, None), P()),
        out_specs=(P(), P(), P(('x', 'k'), None, None, ('z', 'y'))), check_vma=False)
```

```python
import functools
import itertools

import jax
import jax.numpy as jnp
import numpy as np
from jax import lax
from jax.experimental import pallas as pl
from jax.experimental.pallas import tpu as pltpu
from jax.sharding import Mesh, PartitionSpec as P

LANCZOS_STEPS = 4
FULL_PREC = lax.Precision.HIGHEST
MESH_IDS = pl.DeviceIdType.MESH
scope = jax.named_scope
RING = 4
CORES = 2
PARTS = 4
STREAMS = 2
TREES = 4
BLOCKS = RING * RING
ALL_LINKS = [('x', 1), ('y', 1), ('x', -1), ('y', -1)]


def fine_mesh(mesh):
    shape = (mesh.shape['col'] // RING, RING, mesh.shape['row'] // CORES, CORES)
    return Mesh(mesh.devices.reshape(shape), ('z', 'y', 'x', 'k'))


def near(d):
    return min(d, RING - d)


def make_tree(turn):
    prefer = ALL_LINKS[turn:] + ALL_LINKS[:turn]
    load = dict.fromkeys(prefer, 0)
    tree = {}
    for offset in sorted(itertools.product(range(RING), repeat=2), key=lambda o: near(o[0]) + near(o[1])):
        options = [
            (axis, sign) for axis, d in zip('xy', offset) for sign in (-1, 1)
            if d and (-sign * d) % RING == near(d)]
        if options:
            tree[offset] = min(options, key=lambda link: (load[link], prefer.index(link)))
            load[tree[offset]] += 1
    return tree


def source_of(message):
    part, dx, dy = message
    axis, sign = LINKS[message]
    return (part, (dx + sign) % RING, dy) if axis == 'x' else (part, dx, (dy + sign) % RING)


LINKS = {(part, *offset): link for part in range(TREES) for offset, link in make_tree(part % len(ALL_LINKS)).items()}
SENDS = {}
for sent in LINKS:
    SENDS.setdefault(source_of(sent), []).append(sent)


def gather_order(release):
    free = dict.fromkeys(ALL_LINKS, 0.0)
    arrival = {}
    order = []

    def issue(now, message):
        order.append(message)
        for sent in SENDS.get(message, ()):
            link = LINKS[sent]
            free[link] = max(free[link], now) + 1.0
            arrival[sent] = free[link] + 0.6

    todo = [(now, (part, 0, 0)) for part, now in enumerate(release)]
    while len(order) < TREES * BLOCKS:
        left = [(now, message) for message, now in arrival.items() if message not in order]
        if todo and (not left or min(left)[0] > todo[0][0]):
            issue(*todo.pop(0))
        else:
            issue(*min(left))
    return order


def counts(*texts):
    return [int(c) for text in texts for c in text]


RELEASE = [0, 2.9000000000000004, 8.0, 8.0]
LAGS = counts('34456')
FINISH = [17, 25, 33, 72]
HOOKS = (7, 17, 43)
DURING_ONE = counts('113000051510220120300011340', '000000400000000000')
DURING_RING = counts('00000000000000000000000400020421')
DURING_TAIL = counts('10310200')
EARLY = sum(DURING_RING) + sum(DURING_TAIL)
HELD = gather_order(RELEASE)
INDEX = {message: i for i, message in enumerate(HELD)}
MESSAGES = [message for message in HELD if message in LINKS]
GROUP = TREES
WIDE = len(HELD) // 4
CHUNKS = [(c * WIDE, WIDE) for c in range(3)] + [(3 * WIDE + c * WIDE // 2, WIDE // 2) for c in range(2)]


def dot(lhs, rhs):
    return jnp.dot(lhs, rhs, precision=FULL_PREC, preferred_element_type=jnp.float32)


def lanczos_kernel(
        num_elems, num_z, psi_ref, left_ref, right_ref, mpo_ref, spread_out_ref, spread_in_ref, same_ref, out_ref, scal_ref,
        gath, right_full, left_own, left_turn, left_perm, w_mat, acc, mid, terms, ring, h_buf, v_buf, pack_out, pack_in,
        red_held, red_slots, alpha_sum,
        ag_send, ag_recv, sib_send, sib_recv, rs_send, rs_recv, red_send, red_recv, turn_send, turn_recv,
        env_send, env_recv, load_sem, ag_credit, rs_credit):
    phys, rows, cols = h_buf.shape[1:]
    bonds = right_full.shape[0]
    bonds_l = left_own.shape[0]
    piece = rows // TREES
    slab = rows // PARTS
    octs = rows // 8
    pairs = pack_in.shape[2]
    last_step = LANCZOS_STEPS - 1
    z, y, x, k = (lax.axis_index(name) for name in ('z', 'y', 'x', 'k'))
    other = 1 - k

    x_at, y_at = ([lax.rem(pos + d, RING) for d in range(RING)] for pos in (x, y))
    k_at = (k, other)

    def step_to(axis, sign):
        return {axis: {'x': x_at, 'y': y_at}[axis][sign % RING]}

    phases = (
        (num_z, z, lambda i: {'z': i}),
        (RING * RING * CORES, (x * CORES + k) * RING + y,
         lambda i: {'x': lax.div(i, CORES * RING), 'k': lax.rem(lax.div(i, RING), CORES), 'y': lax.rem(i, RING)}),
    )
    bases = (0, num_z)
    barrier = pltpu.get_barrier_semaphore()
    def repeat(lo, hi, fn):
        def body(i, c):
            fn(i)
            return c
        lax.fori_loop(lo, hi, body, 0)

    for count, me, device in phases:
        def enter(d, count=count, me=me, device=device):
            pl.semaphore_signal(barrier, inc=1, device_id=device(lax.rem(me + d, count)), device_id_type=MESH_IDS)
        repeat(1, count, enter)

    own_rows = pl.multiple_of(y * rows, rows)
    load_left = pltpu.make_async_copy(left_ref.at[:, pl.ds(own_rows, rows), :], left_own, load_sem.at[0])
    load_left.start()
    load_right = pltpu.make_async_copy(right_ref, right_full.at[:, pl.ds(own_rows, rows), :], load_sem.at[1])
    load_right.start()

    lane = lax.broadcasted_iota(jnp.int32, (rows, 128), 1)

    def pack(which, value):
        def body(pair):
            halves = [value(2 * pair), value(jnp.minimum(2 * pair + 1, phys - 1))]
            for target in range(RING):
                tile, half = divmod(target * rows, 128)
                first, second = (v[:, tile * 128:(tile + 1) * 128] for v in halves)
                if half == 0:
                    second = pltpu.roll(second, rows, 1)
                else:
                    first = pltpu.roll(first, rows, 1)
                pack_out[which, target, pair] = jnp.where(lane < rows, first, second)
        repeat(0, pairs, body)

    def turn_copy(which, src, dst, d, device):
        return pltpu.make_async_remote_copy(
            src_ref=pack_out.at[which, src], dst_ref=pack_in.at[which, dst],
            send_sem=turn_send.at[which, d], recv_sem=turn_recv.at[which, dst],
            device_id=device, device_id_type=MESH_IDS)

    def turn_start(which):
        for d in range(1, RING):
            peer = y_at[d]
            turn_copy(which, peer, y, d, {'y': peer}).start()
        pack_in[which, y] = pack_out[which, y]

    def turn_finish(which):
        for d in range(1, RING):
            peer = y_at[d]
            copy = turn_copy(which, peer, peer, d, {'y': peer})
            copy.wait_send()
            copy.wait_recv()

    def turned(which, pair):
        return jnp.concatenate([pack_in[which, i, pair] for i in range(RING)], axis=0)

    with scope('pack'):
        pack(0, lambda p: psi_ref[p])
    with scope('entry_barrier'):
        pl.semaphore_wait(barrier, sum(count - 1 for count, _, _ in phases))
    turn_start(0)
    h_buf[1] = jnp.zeros(h_buf.shape[1:], jnp.float32)
    v_buf[...] = jnp.zeros(v_buf.shape, jnp.float32)

    def sum_start(which, phase, value):
        count, me, device = phases[phase]
        red_held[which, phase] = value

        def send(d):
            pltpu.make_async_remote_copy(
                src_ref=red_held.at[which, phase], dst_ref=red_slots.at[which, bases[phase] + me],
                send_sem=red_send.at[which, bases[phase] + d], recv_sem=red_recv.at[which, bases[phase] + me],
                device_id=device(lax.rem(me + d, count)), device_id_type=MESH_IDS).start()
        repeat(1, count, send)
        red_slots[which, bases[phase] + me] = value

    def sum_finish(which, phase):
        count, me, device = phases[phase]

        def wait(d):
            peer = lax.rem(me + d, count)
            copy = pltpu.make_async_remote_copy(
                src_ref=red_held.at[which, phase], dst_ref=red_slots.at[which, bases[phase] + peer],
                send_sem=red_send.at[which, bases[phase] + d], recv_sem=red_recv.at[which, bases[phase] + peer],
                device_id=device(peer), device_id_type=MESH_IDS)
            copy.wait_send()
            copy.wait_recv()
        repeat(1, count, wait)
        return red_slots[which, bases[phase]:bases[phase] + count].sum(0)

    def mean_of(value):
        return jnp.broadcast_to(jnp.sum(value, axis=(0, 1), keepdims=True) * (1.0 / num_elems), (8, 128))

    def fold(values):
        lanes = values.reshape(-1, 8, cols).sum(0)
        tile = lanes[:, :128]
        for c in range(128, cols, 128):
            tile = tile + lanes[:, c:c + 128]
        return tile

    def gather_copy(message):
        index = INDEX[message]
        return pltpu.make_async_remote_copy(
            src_ref=gath.at[0, INDEX[source_of(message)]], dst_ref=gath.at[0, index],
            send_sem=ag_send.at[index], recv_sem=ag_recv.at[index],
            device_id=step_to(*LINKS[message]), device_id_type=MESH_IDS)

    def sibling_copy(index):
        span = pl.ds(index * GROUP, GROUP)
        return pltpu.make_async_remote_copy(
            src_ref=gath.at[0, span], dst_ref=gath.at[1, span],
            send_sem=sib_send.at[index], recv_sem=sib_recv.at[index],
            device_id={'k': other}, device_id_type=MESH_IDS)

    def groups_after(held, sequence):
        done = {}
        held = set(held)
        for message in sequence:
            held.add(message)
            for i in range(BLOCKS):
                group = HELD[i * GROUP:(i + 1) * GROUP]
                if message in group and held.issuperset(group):
                    done.setdefault(message, []).append(i)
        return done

    def take(message, groups):
        if message in LINKS:
            gather_copy(message).wait_recv()
        for sent in SENDS.get(message, ()):
            gather_copy(sent).start()
        for i in groups.get(message, ()):
            sibling_copy(i).start()

    def own_parts(s):
        each = TREES // PARTS
        return [(s * each + i, 0, 0) for i in range(each)]

    with scope('left'):
        load_left.wait()
    order = []
    for first, count in CHUNKS:
        order += [(dk, message) for dk in range(CORES) for message in HELD[first:first + count]]
    per_tile = 128 // piece
    lanes = lax.broadcasted_iota(jnp.int32, (rows, 128), 1)

    left_tiles = {
        (dx, dk, dy): pl.multiple_of(lax.div((x_at[dx] * CORES + k_at[dk]) * RING + y_at[dy], 2) * 128, 128)
        for dx in range(RING) for dk in range(CORES) for dy in range(RING)}

    def left_rows(l, c):
        for tile in range(left_own.shape[2] // 128):
            at = slice(tile * 128, (tile + 1) * 128)
            plain = left_own[l, :, at]
            rolled = pltpu.roll(plain, rows, 1)
            left_turn[0, :, at] = jnp.where(lax.rem(y, 2) == 0, plain, rolled)
            left_turn[1, :, at] = jnp.where(lax.rem(y, 2) == 0, rolled, plain)
        for tile in range(left_perm.shape[2] // 128):
            result = None
            for i in range(per_tile):
                dk, message = order[tile * per_tile + i]
                _, dx, dy = message
                values = left_turn[dy % 2, :, pl.ds(left_tiles[dx, dk, dy], 128)]
                if i != message[0]:
                    values = pltpu.roll(values, (i - message[0]) * piece % 128, 1)
                result = values if i == 0 else jnp.where(lanes >= i * piece, values, result)
            left_perm[l, :, tile * 128:(tile + 1) * 128] = result
        return c

    with scope('left_order'):
        lax.fori_loop(0, bonds_l, left_rows, 0)

    with scope('mpo'):
        wide = dot(dot(spread_out_ref[...], mpo_ref[...]), spread_in_ref[...])
        n_out, n_in = w_mat.shape
        same = jnp.broadcast_to(same_ref[...][None], (n_out // 8, 8, n_in)).reshape(n_out, n_in)
        w_mat[...] = wide * same

    with scope('turn_wait'):
        turn_finish(0)
    with scope('turn'):
        def unpack(pair):
            block = jnp.transpose(turned(0, pair))
            for i, p in enumerate((2 * pair, jnp.minimum(2 * pair + 1, phys - 1))):
                h_buf[0, p] = block[i * rows:(i + 1) * rows, :]
                for part in range(TREES):
                    span = slice(i * rows + part * piece, i * rows + (part + 1) * piece)
                    gath[0, INDEX[part, 0, 0], p] = block[span, :]
        repeat(0, pairs, unpack)
    own = [message for message in HELD if message not in LINKS]
    groups = groups_after((), own + MESSAGES[:EARLY])
    with scope('gather_early'):
        for message in own + MESSAGES[:EARLY]:
            take(message, groups)

    def stage_one(first, count, p, fresh):
        depth = count * piece
        rhs = jnp.concatenate(
            [gath[dk, pl.ds(first, count), p].reshape(depth, cols) for dk in range(CORES)], axis=0)
        column = pl.multiple_of(first * CORES * piece, 128)
        lhs = left_perm[:, :, pl.ds(column, CORES * depth)].reshape(bonds_l * rows, CORES * depth)
        res = dot(lhs, rhs).reshape(bonds_l, octs, 8, cols)
        acc[p] = jnp.where(fresh, 0.0, acc[p]) + res

    def at_steps(i, events):
        wide = 8
        for base in sorted({n // wide for n in events}):
            @pl.when(lax.div(i, wide) == base)
            def _(base=base):
                for n in range(base * wide, (base + 1) * wide):
                    if n in events:
                        @pl.when(i == n)
                        def _(n=n):
                            for event in events[n]:
                                event()

    half = rows // 2
    quarter = rows // 4

    def env_view(row, count, i):
        block = ring_block(0, i)
        return right_full.at[:, pl.ds(pl.multiple_of(row, 8), count), pl.ds(pl.multiple_of(block * cols, cols), cols)]

    def env_copy(kind, i, row, count, device):
        view = env_view(row, count, i)
        return pltpu.make_async_remote_copy(
            src_ref=view, dst_ref=view, send_sem=env_send.at[kind, i], recv_sem=env_recv.at[kind, i],
            device_id=device, device_id_type=MESH_IDS)

    up, down, far = y_at[1], y_at[3], y_at[2]

    def env_row(owner, core):
        return owner * rows + core * half

    def env_start(i):
        env_copy(0, i, env_row(y, k), half, {'y': up}).start()
        env_copy(1, i, env_row(y, k), half, {'y': down}).start()

    def env_pass(i):
        env_copy(0, i, env_row(down, k), half, {'y': up}).wait_recv()
        env_copy(2, i, env_row(down, k), quarter, {'y': up}).start()
        env_copy(4, i, env_row(down, k), half, {'k': other}).start()
        env_copy(1, i, env_row(up, k), half, {'y': down}).wait_recv()
        env_copy(3, i, env_row(up, k) + quarter, quarter, {'y': down}).start()
        env_copy(5, i, env_row(up, k), half, {'k': other}).start()

    def env_end(i):
        env_copy(2, i, env_row(far, k), quarter, {'y': up}).wait_recv()
        env_copy(3, i, env_row(far, k) + quarter, quarter, {'y': down}).wait_recv()
        env_copy(6, i, env_row(far, k), half, {'k': other}).start()

    def env_done(i):
        env_copy(4, i, env_row(down, other), half, {'k': other}).wait_recv()
        env_copy(5, i, env_row(up, other), half, {'k': other}).wait_recv()
        env_copy(6, i, env_row(far, other), half, {'k': other}).wait_recv()

    def env_sent(i):
        for kind, row, count in ((0, env_row(y, k), half), (1, env_row(y, k), half), (2, env_row(down, k), quarter),
                                 (3, env_row(up, k) + quarter, quarter), (4, env_row(down, k), half),
                                 (5, env_row(up, k), half), (6, env_row(far, k), half)):
            env_copy(kind, i, row, count, {'k': other}).wait_send()

    def env_ready(j, s, n):
        @pl.when((j == 0) & (s == 0))
        def _():
            with scope('env_ready'):
                @pl.when(n == 0)
                def _():
                    repeat(0, 2, env_pass)

                @pl.when(n + 2 < num_z)
                def _():
                    env_pass(n + 2)

                env_end(n)
                env_done(n)

    def way(s):
        return 1 - 2 * lax.rem(s, 2)

    def ring_side(s, n):
        return way(s) * (1 - 2 * lax.rem(n, 2))

    def ring_block(s, n):
        return lax.rem(z + num_z + ring_side(s, n) * (num_z // 2 - lax.div(n + 1, 2)), num_z)

    def ring_copy(src, s, n, h):
        return pltpu.make_async_remote_copy(
            src_ref=src, dst_ref=ring.at[s, n, h], send_sem=rs_send.at[s, n, h], recv_sem=rs_recv.at[s, n, h],
            device_id={'z': lax.rem(z + num_z + ring_side(s, n), num_z)}, device_id_type=MESH_IDS)

    def ring_wait(s, n, h):
        ring_copy(terms.at[s, n, h], s, n, h).wait_recv()

    def ring_pass(s, n, h):
        with scope('ring_pass'):
            ring_wait(s, n - 2, h)
            ring[s, n - 2, h] = ring[s, n - 2, h] + terms[s, n, h]
            ring_copy(ring.at[s, n - 2, h], s, n, h).start()

    def middle(o):
        res = dot(w_mat[...], acc[:, :, o].reshape(phys * bonds_l * 8, cols)).reshape(bonds, phys, 8, cols)
        for r in range(bonds):
            mid[:, o, :, r * cols:(r + 1) * cols] = res[r]

    def last_stage(s, n):
        lhs = mid[:, pl.ds(s * STREAMS, STREAMS)].reshape(phys * slab, bonds * cols)
        first = pl.multiple_of(ring_block(s, n) * cols, cols)
        rhs = right_full[:, :, pl.ds(first, cols)].reshape(bonds * cols, cols)
        res = dot(lhs, rhs).reshape(phys, STREAMS, 8, cols)
        for h in range(STREAMS):
            terms[s, n, h] = res[:, h]

    def new_direction(cur, alpha, beta_prev):
        nxt = 1 - cur
        a, b = alpha[0:1, 0:1], beta_prev[0:1, 0:1]
        def body(p, total):
            w = h_buf[cur, p] - a * v_buf[cur, p] - b * v_buf[nxt, p]
            v_buf[nxt, p] = w
            return total + fold(w * w)

        return lax.fori_loop(0, phys, body, jnp.zeros((8, 128), jnp.float32))

    def step(j, carry):
        alpha_part, beta_prev = carry
        cur = lax.rem(j, 2)
        nxt = 1 - cur
        more = j < last_step

        def alpha_z():
            sum_start(0, 1, sum_finish(0, 0))

        def alpha_plane():
            alpha = mean_of(sum_finish(0, 1))
            scal_ref[0, j] = alpha
            sum_start(1, 0, new_direction(cur, alpha, beta_prev))

        def beta_z():
            sum_start(1, 1, sum_finish(1, 0))

        sum_start(0, 0, alpha_part)
        queue = MESSAGES[EARLY:]
        groups = groups_after(own + MESSAGES[:EARLY], queue)
        wide_steps, all_steps = 3 * phys, 5 * phys
        events = {}
        hooks = dict(zip(HOOKS, (alpha_z, alpha_plane, beta_z)))
        for n, count in enumerate(DURING_ONE):
            at = events.setdefault(n * phys // 9, [])
            at += [functools.partial(take, message, groups) for message in queue[:count]]
            queue = queue[count:]
            if n % 9 == 0:
                first, count = CHUNKS[n // 9]
                at += [sibling_copy(i).wait_recv for i in range(first // GROUP, (first + count) // GROUP)]
            if n in hooks:
                at.append(hooks[n])

        def wide_step(i):
            with scope('events_wide'):
                at_steps(i, {n: e for n, e in events.items() if n < wide_steps})
            with scope('one_wide'):
                stage_one(lax.div(i, phys) * WIDE, WIDE, lax.rem(i, phys), i < phys)

        def half_step(i):
            with scope('events_half'):
                at_steps(i, {n - wide_steps: e for n, e in events.items() if n >= wide_steps})

            @pl.when((j == 0) & (i == phys))
            def _():
                load_right.wait()
                repeat(0, num_z, env_start)

            with scope('one_half'):
                stage_one(3 * WIDE + lax.div(i, phys) * (WIDE // 2), WIDE // 2, lax.rem(i, phys), i < 0)

        repeat(0, wide_steps, wide_step)
        repeat(0, all_steps - wide_steps, half_step)
        with scope('gather_sent'):
            for message in MESSAGES:
                gather_copy(message).wait_send()
            repeat(0, BLOCKS, lambda i: sibling_copy(i).wait_send())

        @pl.when(more)
        def _():
            for link in ALL_LINKS:
                pl.semaphore_signal(ag_credit, inc=1, device_id=step_to(*link), device_id_type=MESH_IDS)
            pl.semaphore_signal(ag_credit, inc=1, device_id={'k': other}, device_id_type=MESH_IDS)

        @pl.when(j > 0)
        def _():
            pl.semaphore_wait(rs_credit, 2)

        def scale():
            beta = jnp.sqrt(mean_of(sum_finish(1, 1)))
            scal_ref[1, j] = beta
            inv = (1.0 / beta)[0:1, 0:1]

            def normalize(p):
                v_buf[nxt, p] = v_buf[nxt, p] * inv
            repeat(0, phys, normalize)

            @pl.when(more)
            def _():
                pl.semaphore_wait(ag_credit, len(ALL_LINKS) + 1)

            @pl.when(j == last_step)
            def _():
                pack(1, lambda p: v_buf[nxt, p])
                turn_start(1)

        def finish(s):
            if s == 0:
                scale()
            with scope('ring_end'):
                for h in range(STREAMS):
                    for n in range(max(num_z - 3, 0), num_z - 1):
                        ring_wait(s, n, h)
            alpha, beta = scal_ref[0, j], scal_ref[1, j]
            a, b, inv = alpha[0:1, 0:1], beta_prev[0:1, 0:1], (1.0 / beta)[0:1, 0:1]
            span = slice(s * slab, (s + 1) * slab)

            def body(p, total):
                new = []
                for h in range(STREAMS):
                    at = slice(s * slab + 8 * h, s * slab + 8 * h + 8)
                    g_new = terms[s, num_z - 1, h, p]
                    for n in range(max(num_z - 3, 0), num_z - 1):
                        g_new = g_new + ring[s, n, h, p]
                    new.append((g_new - a * h_buf[cur, p, at, :] - b * h_buf[nxt, p, at, :]) * inv)
                h_new = jnp.concatenate(new, axis=0)
                h_buf[nxt, p, span, :] = h_new
                for i, message in enumerate(own_parts(s)):
                    gath[0, INDEX[message], p] = h_new[i * piece:(i + 1) * piece]
                return total + fold(v_buf[nxt, p, span, :] * h_new)

            total = lax.fori_loop(0, phys, body, jnp.zeros((8, 128), jnp.float32))
            alpha_sum[...] = total if s == 0 else alpha_sum[...] + total

            @pl.when(more)
            def _():
                for message in own_parts(s):
                    take(message, next_groups)

        def early(message):
            @pl.when(more)
            def _():
                take(message, next_groups)

        def happen(event):
            {'pass': ring_pass, 'finish': finish, 'early': early}[event[0]](*event[1:])

        ring_steps = PARTS * num_z
        events = {}
        for s in range(PARTS):
            for n in range(2, num_z - 1):
                at = s * num_z + n + LAGS[n - 2]
                events.setdefault(at, []).extend(('pass', s, n, h) for h in range(STREAMS))
            events.setdefault(FINISH[s] * num_z // 8, []).append(('finish', s))
        tail = [event for at in sorted(events) if at >= ring_steps for event in events.pop(at)]
        queue = MESSAGES[:EARLY]
        for at, count in enumerate(DURING_RING):
            events.setdefault(at * num_z // 8, []).extend(('early', message) for message in queue[:count])
            queue = queue[count:]
        mixed = []
        spare = list(DURING_TAIL)
        for i, event in enumerate(tail):
            mixed.append(event)
            count = len(queue) if i == len(tail) - 1 else spare.pop(0) if spare else 0
            mixed += [('early', message) for message in queue[:count]]
            queue = queue[count:]
        tail = mixed
        sequence = [event for at in sorted(events) for event in events[at]] + tail
        sequence = [
            message for kind, *what in sequence if kind != 'pass'
            for message in (own_parts(*what) if kind == 'finish' else what)]
        next_groups = groups_after((), sequence)

        def ring_step(i):
            s, n = lax.div(i, num_z), lax.rem(i, num_z)

            @pl.when(n == 0)
            def _():
                repeat(0, STREAMS, lambda o: middle(s * STREAMS + o))

            env_ready(j, s, n)
            with scope('last_stage'):
                last_stage(s, n)

            @pl.when(n < min(2, num_z - 1))
            def _():
                for h in range(STREAMS):
                    ring_copy(terms.at[s, n, h], s, n, h).start()

            with scope('events_ring'):
                at_steps(i, {at: [functools.partial(happen, event) for event in events[at]] for at in events})

        repeat(0, ring_steps, ring_step)
        with scope('tail'):
            for event in tail:
                happen(event)

        def ring_sent(i):
            s, n = lax.div(i, num_z - 1), lax.rem(i, num_z - 1)
            for h in range(STREAMS):
                ring_copy(terms.at[s, n, h], s, n, h).wait_send()
        repeat(0, PARTS * (num_z - 1), ring_sent)

        @pl.when(more)
        def _():
            for sign in (1, num_z - 1):
                pl.semaphore_signal(
                    rs_credit, inc=1, device_id={'z': lax.rem(z + sign, num_z)}, device_id_type=MESH_IDS)

        return alpha_sum[...], jnp.where(j > 0, scal_ref[1, j], 0.0)

    zero = jnp.zeros((8, 128), jnp.float32)
    _, beta_prev = lax.fori_loop(0, LANCZOS_STEPS, step, (zero, zero))
    repeat(0, num_z, env_sent)

    cur = LANCZOS_STEPS % 2
    shift = scal_ref[0, last_step][0:1, 0:1]
    b = beta_prev[0:1, 0:1]

    def end_body(p, sums):
        h, v = h_buf[cur, p], v_buf[cur, p]
        d = h - shift * v - b * v_buf[1 - cur, p]
        h_buf[1 - cur, p] = d
        return tuple(total + fold(term) for total, term in zip(sums, (v * h, d * d, d * v, v * v)))

    sums = lax.fori_loop(0, phys, end_body, (zero,) * 4)
    row = lax.broadcasted_iota(jnp.int32, (8, 128), 0)

    def squeeze(tile):
        tile = tile + pltpu.roll(tile, 4, 0)
        return tile + pltpu.roll(tile, 2, 0)

    packed = squeeze(sums[0])
    for i in range(1, 4):
        packed = jnp.where(row >= 2 * i, squeeze(sums[i]), packed)
    with scope('end_sum'):
        sum_start(0, 0, packed)
        pack(0, lambda p: h_buf[1 - cur, p])
        turn_start(0)
        sum_start(0, 1, sum_finish(0, 0))
        packed = sum_finish(0, 1)
    v_h, d_d, d_v, v_v = (mean_of(jnp.where((row >= 2 * i) & (row < 2 * i + 2), packed, 0.0)) for i in range(4))
    delta = v_h - shift
    beta = jnp.sqrt(d_d - 2.0 * delta * d_v + delta * delta * v_v)
    scal_ref[0, LANCZOS_STEPS] = v_h
    scal_ref[1, LANCZOS_STEPS] = beta
    inv = (1.0 / beta)[0:1, 0:1]
    delta = delta[0:1, 0:1]
    with scope('end_turn_wait'):
        turn_finish(1)
        turn_finish(0)
    with scope('end_turn'):
        def end_unpack(pair):
            block = jnp.transpose((turned(0, pair) - delta * turned(1, pair)) * inv)
            for i, p in enumerate((2 * pair, jnp.minimum(2 * pair + 1, phys - 1))):
                out_ref[p] = block[i * rows:(i + 1) * rows, :]
        repeat(0, pairs, end_unpack)


def solution(mesh):
    grid = fine_mesh(mesh)
    num_z = grid.shape['z']

    def local_run(psi_blk, left_blk, right_blk, mpo_pair):
        full_rows, n_s, n_u, local_cols = psi_blk.shape
        phys = n_s * n_u
        rows = full_rows // RING
        cols = local_cols * RING
        bonds_l, bonds_r = left_blk.shape[1], right_blk.shape[1]
        full_a, full_b = left_blk.shape[2], right_blk.shape[2]
        psi = psi_blk.transpose(1, 2, 3, 0).reshape(phys, local_cols, full_rows)
        left = left_blk.transpose(1, 0, 2)
        right = right_blk.transpose(1, 0, 2)
        mpo = mpo_pair.reshape(bonds_l, bonds_r, phys, phys).transpose(1, 3, 2, 0)
        mpo = mpo.reshape(bonds_r * phys, phys * bonds_l)
        eye = np.eye(8, dtype=np.float32)
        one = np.ones((1, 8), np.float32)
        spread_out = np.kron(np.eye(bonds_r * phys, dtype=np.float32), one.T)
        spread_in = np.kron(np.eye(phys * bonds_l, dtype=np.float32), one)
        same = np.tile(eye, (1, phys * bonds_l))
        red = num_z + RING * RING * CORES
        pairs = (phys + 1) // 2
        f32 = jnp.float32
        out, scal = pl.pallas_call(
            functools.partial(lanczos_kernel, float(psi_blk.size * grid.size), num_z),
            out_shape=(
                jax.ShapeDtypeStruct((phys, local_cols, full_rows), f32),
                jax.ShapeDtypeStruct((2, LANCZOS_STEPS + 1, 8, 128), f32),
            ),
            in_specs=[
                pl.BlockSpec(memory_space=pltpu.VMEM),
                pl.BlockSpec(memory_space=pl.ANY),
                pl.BlockSpec(memory_space=pl.ANY),
            ] + [pl.BlockSpec(memory_space=pltpu.VMEM)] * 4,
            out_specs=(pl.BlockSpec(memory_space=pltpu.VMEM), pl.BlockSpec(memory_space=pltpu.VMEM)),
            scratch_shapes=[
                pltpu.VMEM((CORES, len(HELD), phys, rows // TREES, cols), f32),
                pltpu.VMEM((bonds_r, cols, full_b), f32),
                pltpu.VMEM((bonds_l, rows, full_a), f32),
                pltpu.VMEM((2, rows, full_a), f32),
                pltpu.VMEM((bonds_l, rows, full_a), f32),
                pltpu.VMEM((bonds_r * phys * 8, phys * bonds_l * 8), f32),
                pltpu.VMEM((phys, bonds_l, rows // 8, 8, cols), f32),
                pltpu.VMEM((phys, rows // 8, 8, bonds_r * cols), f32),
                pltpu.VMEM((PARTS, num_z, STREAMS, phys, 8, cols), f32),
                pltpu.VMEM((PARTS, num_z - 1, STREAMS, phys, 8, cols), f32),
                pltpu.VMEM((2, phys, rows, cols), f32),
                pltpu.VMEM((2, phys, rows, cols), f32),
                pltpu.VMEM((2, RING, pairs, rows, 128), f32),
                pltpu.VMEM((2, RING, pairs, rows, 128), f32),
                pltpu.VMEM((2, 2, 8, 128), f32),
                pltpu.VMEM((2, red, 8, 128), f32),
                pltpu.VMEM((8, 128), f32),
                pltpu.SemaphoreType.DMA((len(HELD),)),
                pltpu.SemaphoreType.DMA((len(HELD),)),
                pltpu.SemaphoreType.DMA((BLOCKS,)),
                pltpu.SemaphoreType.DMA((BLOCKS,)),
                pltpu.SemaphoreType.DMA((PARTS, num_z - 1, STREAMS)),
                pltpu.SemaphoreType.DMA((PARTS, num_z - 1, STREAMS)),
                pltpu.SemaphoreType.DMA((2, red)),
                pltpu.SemaphoreType.DMA((2, red)),
                pltpu.SemaphoreType.DMA((2, RING)),
                pltpu.SemaphoreType.DMA((2, RING)),
                pltpu.SemaphoreType.DMA((7, num_z)),
                pltpu.SemaphoreType.DMA((7, num_z)),
                pltpu.SemaphoreType.DMA((2,)),
                pltpu.SemaphoreType.REGULAR,
                pltpu.SemaphoreType.REGULAR,
            ],
            compiler_params=pltpu.CompilerParams(
                collective_id=0, has_side_effects=True, vmem_limit_bytes=67043328),
        )(psi, left, right, mpo, spread_out, spread_in, same)
        result = out.reshape(n_s, n_u, local_cols, full_rows).transpose(3, 0, 1, 2)
        return scal[0, 1:, 0, 0], scal[1, 1:, 0, 0], result

    return jax.shard_map(
        local_run, mesh=grid,
        in_specs=(P(('x', 'k'), None, None, ('z', 'y')), P(('x', 'k'), None, None), P(('z', 'y'), None, None), P()),
        out_specs=(P(), P(), P(('x', 'k'), None, None, ('z', 'y'))), check_vma=False)
```

```python
import functools
import itertools

import jax
import jax.numpy as jnp
import numpy as np
from jax import lax
from jax.experimental import pallas as pl
from jax.experimental.pallas import tpu as pltpu
from jax.sharding import Mesh, PartitionSpec as P

LANCZOS_STEPS = 4
FULL_PREC = lax.Precision.HIGHEST
MESH_IDS = pl.DeviceIdType.MESH
scope = jax.named_scope
SUB = 8
LANES = 128
TILE = (SUB, LANES)
RING = 4
CORES = 2
PARTS = 4
STREAMS = 2
TREES = 4
BLOCKS = RING * RING
ALL_LINKS = [('x', 1), ('y', 1), ('x', -1), ('y', -1)]


def fine_mesh(mesh):
    shape = (mesh.shape['col'] // RING, RING, mesh.shape['row'] // CORES, CORES)
    return Mesh(mesh.devices.reshape(shape), ('z', 'y', 'x', 'k'))


def near(d):
    return min(d, RING - d)


def make_tree(turn):
    prefer = ALL_LINKS[turn:] + ALL_LINKS[:turn]
    load = dict.fromkeys(prefer, 0)
    tree = {}
    for offset in sorted(itertools.product(range(RING), repeat=2), key=lambda o: near(o[0]) + near(o[1])):
        options = [
            (axis, sign) for axis, d in zip('xy', offset) for sign in (-1, 1)
            if d and (-sign * d) % RING == near(d)]
        if options:
            tree[offset] = min(options, key=lambda link: (load[link], prefer.index(link)))
            load[tree[offset]] += 1
    return tree


def source_of(message):
    part, dx, dy = message
    axis, sign = LINKS[message]
    return (part, (dx + sign) % RING, dy) if axis == 'x' else (part, dx, (dy + sign) % RING)


LINKS = {(part, *offset): link for part in range(TREES) for offset, link in make_tree(part % len(ALL_LINKS)).items()}
SENDS = {}
for sent in LINKS:
    SENDS.setdefault(source_of(sent), []).append(sent)


def gather_order(release):
    free = dict.fromkeys(ALL_LINKS, 0.0)
    arrival = {}
    order = []

    def issue(now, message):
        order.append(message)
        for sent in SENDS.get(message, ()):
            link = LINKS[sent]
            free[link] = max(free[link], now) + 1.0
            arrival[sent] = free[link] + 0.6

    todo = [(now, (part, 0, 0)) for part, now in enumerate(release)]
    while len(order) < TREES * BLOCKS:
        left = [(now, message) for message, now in arrival.items() if message not in order]
        if todo and (not left or min(left)[0] > todo[0][0]):
            issue(*todo.pop(0))
        else:
            issue(*min(left))
    return order


def counts(*texts):
    return [int(c) for text in texts for c in text]


RELEASE = [0, 3.9, 8.0, 10.0]
LAGS = counts('22344')
FINISH = [9, 14, 18, 32]
HOOKS = (7, 15, 27)
DURING_ONE = counts('000400102000130623103010210', '210200')
DURING_RING = counts('0000000000040407')
DURING_TAIL = counts('20020150')
EARLY = sum(DURING_RING) + sum(DURING_TAIL)
ENV_PIECES = 4
ENV_STRIDE = 2
ENV_STEPS = (1, 8, 14, 18, 23)
CHUNK_STEPS = (0, 9, 18, 27, 30)
SPAN = 4
HELD = gather_order(RELEASE)
INDEX = {message: i for i, message in enumerate(HELD)}
MESSAGES = [message for message in HELD if message in LINKS]
GROUP = TREES
WIDE = len(HELD) // 4
CHUNKS = [(c * WIDE, WIDE) for c in range(3)] + [(3 * WIDE + c * WIDE // 2, WIDE // 2) for c in range(2)]


def dot(lhs, rhs):
    return jnp.dot(lhs, rhs, precision=FULL_PREC, preferred_element_type=jnp.float32)


def lanczos_kernel(
        num_elems, num_z, psi_ref, left_ref, right_ref, mpo_ref, spread_out_ref, spread_in_ref, same_ref, out_ref, scal_ref,
        gath, right_full, left_own, left_turn, left_perm, w_mat, acc, mid, terms, ring, h_buf, v_buf, pack_out, pack_in,
        red_held, red_slots, alpha_sum,
        ag_send, ag_recv, sib_send, sib_recv, rs_send, rs_recv, red_send, red_recv, turn_send, turn_recv,
        env_send, env_recv, load_sem, ag_credit, rs_credit):
    phys, rows, cols = h_buf.shape[1:]
    bonds = right_full.shape[0]
    bonds_l = left_own.shape[0]
    piece = rows // TREES
    slab = rows // PARTS
    octs = rows // 8
    pairs = pack_in.shape[2]
    last_step = LANCZOS_STEPS - 1
    z, y, x, k = (lax.axis_index(name) for name in ('z', 'y', 'x', 'k'))
    other = 1 - k

    x_at, y_at = ([lax.rem(pos + d, RING) for d in range(RING)] for pos in (x, y))
    k_at = (k, other)

    def step_to(axis, sign):
        return {axis: {'x': x_at, 'y': y_at}[axis][sign % RING]}

    phases = (
        (num_z, z, lambda i: {'z': i}),
        (RING * RING * CORES, (x * CORES + k) * RING + y,
         lambda i: {'x': lax.div(i, CORES * RING), 'k': lax.rem(lax.div(i, RING), CORES), 'y': lax.rem(i, RING)}),
    )
    bases = (0, num_z)
    barrier = pltpu.get_barrier_semaphore()
    def repeat(lo, hi, fn):
        def body(i, c):
            fn(i)
            return c
        lax.fori_loop(lo, hi, body, 0)

    for count, me, device in phases:
        def enter(d, count=count, me=me, device=device):
            pl.semaphore_signal(barrier, inc=1, device_id=device(lax.rem(me + d, count)), device_id_type=MESH_IDS)
        repeat(1, count, enter)

    own_rows = pl.multiple_of(y * rows, rows)
    load_left = pltpu.make_async_copy(left_ref.at[:, pl.ds(own_rows, rows), :], left_own, load_sem.at[0])
    load_left.start()
    load_right = pltpu.make_async_copy(right_ref, right_full.at[:, pl.ds(y * RING, RING)], load_sem.at[1])
    load_right.start()

    lane = lax.broadcasted_iota(jnp.int32, (rows, LANES), 1)

    def pack(which, value):
        def body(pair):
            halves = [value(2 * pair), value(jnp.minimum(2 * pair + 1, phys - 1))]
            for target in range(RING):
                tile, half = divmod(target * rows, LANES)
                first, second = (v[:, tile * LANES:(tile + 1) * LANES] for v in halves)
                if half == 0:
                    second = pltpu.roll(second, rows, 1)
                else:
                    first = pltpu.roll(first, rows, 1)
                pack_out[which, target, pair] = jnp.where(lane < rows, first, second)
        repeat(0, pairs, body)

    def turn_copy(which, src, dst, d, device):
        return pltpu.make_async_remote_copy(
            src_ref=pack_out.at[which, src], dst_ref=pack_in.at[which, dst],
            send_sem=turn_send.at[which, d], recv_sem=turn_recv.at[which, dst],
            device_id=device, device_id_type=MESH_IDS)

    def turn_start(which):
        for d in range(1, RING):
            peer = y_at[d]
            turn_copy(which, peer, y, d, {'y': peer}).start()
        pack_in[which, y] = pack_out[which, y]

    def turn_finish(which):
        for d in range(1, RING):
            peer = y_at[d]
            copy = turn_copy(which, peer, peer, d, {'y': peer})
            copy.wait_send()
            copy.wait_recv()

    def turned(which, pair):
        return jnp.concatenate([pack_in[which, i, pair] for i in range(RING)], axis=0)

    with scope('pack'):
        pack(0, lambda p: psi_ref[p])
    with scope('entry_barrier'):
        pl.semaphore_wait(barrier, sum(count - 1 for count, _, _ in phases))
    turn_start(0)
    h_buf[1] = jnp.zeros(h_buf.shape[1:], jnp.float32)
    v_buf[...] = jnp.zeros(v_buf.shape, jnp.float32)

    def sum_start(which, phase, value):
        count, me, device = phases[phase]
        red_held[which, phase] = value

        def send(d):
            pltpu.make_async_remote_copy(
                src_ref=red_held.at[which, phase], dst_ref=red_slots.at[which, bases[phase] + me],
                send_sem=red_send.at[which, bases[phase] + d], recv_sem=red_recv.at[which, bases[phase] + me],
                device_id=device(lax.rem(me + d, count)), device_id_type=MESH_IDS).start()
        repeat(1, count, send)
        red_slots[which, bases[phase] + me] = value

    def sum_finish(which, phase):
        count, me, device = phases[phase]

        def wait(d):
            peer = lax.rem(me + d, count)
            copy = pltpu.make_async_remote_copy(
                src_ref=red_held.at[which, phase], dst_ref=red_slots.at[which, bases[phase] + peer],
                send_sem=red_send.at[which, bases[phase] + d], recv_sem=red_recv.at[which, bases[phase] + peer],
                device_id=device(peer), device_id_type=MESH_IDS)
            copy.wait_send()
            copy.wait_recv()
        repeat(1, count, wait)
        return red_slots[which, bases[phase]:bases[phase] + count].sum(0)

    def mean_of(value):
        return jnp.broadcast_to(jnp.sum(value, axis=(0, 1), keepdims=True) * (1.0 / num_elems), TILE)

    def only(tile):
        return tile[:1, :1]

    def fold(values):
        lanes = values.reshape(-1, 8, cols).sum(0)
        tile = lanes[:, :LANES]
        for c in range(LANES, cols, LANES):
            tile = tile + lanes[:, c:c + LANES]
        return tile

    def gather_copy(message):
        index = INDEX[message]
        return pltpu.make_async_remote_copy(
            src_ref=gath.at[0, INDEX[source_of(message)]], dst_ref=gath.at[0, index],
            send_sem=ag_send.at[index], recv_sem=ag_recv.at[index],
            device_id=step_to(*LINKS[message]), device_id_type=MESH_IDS)

    def sibling_copy(index):
        span = pl.ds(index * GROUP, GROUP)
        return pltpu.make_async_remote_copy(
            src_ref=gath.at[0, span], dst_ref=gath.at[1, span],
            send_sem=sib_send.at[index], recv_sem=sib_recv.at[index],
            device_id={'k': other}, device_id_type=MESH_IDS)

    def groups_after(held, sequence):
        done = {}
        held = set(held)
        for message in sequence:
            held.add(message)
            for i in range(BLOCKS):
                group = HELD[i * GROUP:(i + 1) * GROUP]
                if message in group and held.issuperset(group):
                    done.setdefault(message, []).append(i)
        return done

    def take(message, groups):
        if message in LINKS:
            gather_copy(message).wait_recv()
        for sent in SENDS.get(message, ()):
            gather_copy(sent).start()
        for i in groups.get(message, ()):
            sibling_copy(i).start()

    def own_parts(s):
        each = TREES // PARTS
        return [(s * each + i, 0, 0) for i in range(each)]

    with scope('turn_wait'):
        turn_finish(0)
    with scope('turn'):
        def unpack(pair):
            block = jnp.transpose(turned(0, pair))
            for i, p in enumerate((2 * pair, jnp.minimum(2 * pair + 1, phys - 1))):
                h_buf[0, p] = block[i * rows:(i + 1) * rows, :]
                for part in range(TREES):
                    span = slice(i * rows + part * piece, i * rows + (part + 1) * piece)
                    gath[0, INDEX[part, 0, 0], p] = block[span, :]
        repeat(0, pairs, unpack)
    own = [message for message in HELD if message not in LINKS]
    groups = groups_after((), own + MESSAGES[:EARLY])
    for message in own:
        take(message, groups)

    with scope('left'):
        load_left.wait()
    order = []
    for first, count in CHUNKS:
        order += [(dk, message) for dk in range(CORES) for message in HELD[first:first + count]]
    per_tile = LANES // piece
    lanes = lax.broadcasted_iota(jnp.int32, (rows, LANES), 1)

    left_tiles = {
        (dx, dk, dy): pl.multiple_of(lax.div((x_at[dx] * CORES + k_at[dk]) * RING + y_at[dy], 2) * LANES, LANES)
        for dx in range(RING) for dk in range(CORES) for dy in range(RING)}

    def left_rows(l, c):
        for tile in range(left_own.shape[2] // LANES):
            at = slice(tile * LANES, (tile + 1) * LANES)
            plain = left_own[l, :, at]
            rolled = pltpu.roll(plain, rows, 1)
            left_turn[0, :, at] = jnp.where(lax.rem(y, 2) == 0, plain, rolled)
            left_turn[1, :, at] = jnp.where(lax.rem(y, 2) == 0, rolled, plain)
        for tile in range(left_perm.shape[2] // LANES):
            result = None
            for i in range(per_tile):
                dk, message = order[tile * per_tile + i]
                _, dx, dy = message
                values = left_turn[dy % 2, :, pl.ds(left_tiles[dx, dk, dy], LANES)]
                if i != message[0]:
                    values = pltpu.roll(values, (i - message[0]) * piece % LANES, 1)
                result = values if i == 0 else jnp.where(lanes >= i * piece, values, result)
            left_perm[l, :, tile * LANES:(tile + 1) * LANES] = result
        return c

    with scope('left_order'):
        lax.fori_loop(0, bonds_l, left_rows, 0)

    with scope('mpo'):
        rows_out = lax.dot_general(
            spread_out_ref[...], mpo_ref[...], (((1,), (1,)), ((), ())), precision=FULL_PREC,
            preferred_element_type=jnp.float32)
        wide = dot(rows_out, spread_in_ref[...])
        n_out, n_in = w_mat.shape
        same = jnp.broadcast_to(same_ref[...][None], (n_out // 8, 8, n_in)).reshape(n_out, n_in)
        w_mat[...] = wide * same

    with scope('gather_early'):
        for message in MESSAGES[:EARLY]:
            take(message, groups)

    def stage_one(first, count, p, fresh):
        depth = count * piece
        rhs = jnp.concatenate(
            [gath[dk, pl.ds(first, count), p].reshape(depth, cols) for dk in range(CORES)], axis=0)
        column = pl.multiple_of(first * CORES * piece, LANES)
        lhs = left_perm[:, :, pl.ds(column, CORES * depth)].reshape(bonds_l * rows, CORES * depth)
        res = dot(lhs, rhs).reshape(bonds_l, octs, 8, cols)
        acc[p] = jnp.where(fresh, 0.0, acc[p]) + res

    def at_steps(i, events):
        steps = sorted(events)

        def run(steps):
            if len(steps) > 1:
                middle = len(steps) // 2
                lax.cond(i < steps[middle], lambda: run(steps[:middle]), lambda: run(steps[middle:]))
            else:
                for step in steps:
                    @pl.when(i == step)
                    def _():
                        for event in events[step]:
                            event()

        run(steps)

    up, down, far = y_at[1], y_at[3], y_at[2]
    strip = right_full.shape[-1] // ENV_PIECES

    def env_copy(kind, c, block, device, count=1, core=None):
        span = pl.ds(c * strip, strip)
        row = k if core is None else core
        view = right_full.at[:, pl.ds(block, count), pl.ds(row, 1), :, span]
        return pltpu.make_async_remote_copy(
            src_ref=view, dst_ref=view, send_sem=env_send.at[kind, c], recv_sem=env_recv.at[kind, c],
            device_id=device, device_id_type=MESH_IDS)

    def block_of(owner, d):
        return owner * RING + x_at[d]

    TAKEN = (0, 1)

    def env_start(c):
        for d in TAKEN:
            env_copy(d, c, block_of(y, d), {'y': up}).start()
            env_copy(2 + d, c, block_of(y, d), {'y': down}).start()

    def env_pass_x(c, i, owner):
        env_copy(6 + i, c, block_of(owner, 0), {'x': x_at[1]}).start()
        env_copy(9 + i, c, block_of(owner, 1), {'x': x_at[3]}).start()

    def env_pass(c):
        for d in TAKEN:
            env_copy(d, c, block_of(down, d), {'y': up}).wait_recv()
            env_copy(2 + d, c, block_of(up, d), {'y': down}).wait_recv()
        env_copy(4, c, block_of(down, 0), {'y': up}).start()
        env_copy(5, c, block_of(up, 1), {'y': down}).start()
        env_pass_x(c, 0, down)
        env_pass_x(c, 1, up)

    def env_far(c):
        env_copy(4, c, block_of(far, 0), {'y': up}).wait_recv()
        env_copy(5, c, block_of(far, 1), {'y': down}).wait_recv()
        env_pass_x(c, 2, far)

    def env_share(c):
        for i, owner in enumerate((down, up, far)):
            env_copy(6 + i, c, block_of(owner, 3), {'x': x_at[1]}).wait_recv()
            env_copy(9 + i, c, block_of(owner, 2), {'x': x_at[3]}).wait_recv()
            env_copy(12 + i, c, owner * RING, {'k': other}, RING).start()

    def env_done(c):
        for i, owner in enumerate((down, up, far)):
            env_copy(12 + i, c, owner * RING, {'k': other}, RING, other).wait_recv()

    def env_sent(c):
        for kind in range(12):
            env_copy(kind, c, 0, {'k': other}).wait_send()
        for i in range(3):
            env_copy(12 + i, c, 0, {'k': other}, RING).wait_send()

    def way(s):
        return 1 - 2 * lax.rem(s, 2)

    def ring_side(s, n):
        return way(s) * (1 - 2 * lax.rem(n, 2))

    def ring_block(s, n):
        return lax.rem(z + num_z + ring_side(s, n) * (num_z // 2 - lax.div(n + 1, 2)), num_z)

    def ring_copy(src, s, n, h):
        return pltpu.make_async_remote_copy(
            src_ref=src, dst_ref=ring.at[s, n, h], send_sem=rs_send.at[s, n, h], recv_sem=rs_recv.at[s, n, h],
            device_id={'z': lax.rem(z + num_z + ring_side(s, n), num_z)}, device_id_type=MESH_IDS)

    def ring_wait(s, n, h):
        ring_copy(terms.at[s, n, h], s, n, h).wait_recv()

    def ring_pass(s, n, h):
        with scope('ring_pass'):
            ring_wait(s, n - 2, h)
            ring[s, n - 2, h] = ring[s, n - 2, h] + terms[s, n, h]
            ring_copy(ring.at[s, n - 2, h], s, n, h).start()

    def middle(o):
        res = dot(w_mat[...], acc[:, :, o].reshape(phys * bonds_l * 8, cols)).reshape(bonds, phys, 8, cols)
        for r in range(bonds):
            mid[:, o, :, r * cols:(r + 1) * cols] = res[r]

    def last_stage(s, which):
        lhs = mid[:, pl.ds(s * STREAMS, STREAMS)].reshape(phys * slab, bonds * cols)
        for n in which:
            first = pl.multiple_of(ring_block(s, n) * cols, cols)
            rhs = right_full[:, :, :, :, pl.ds(first, cols)].reshape(bonds * cols, cols)
            res = dot(lhs, rhs).reshape(phys, STREAMS, 8, cols)
            for h in range(STREAMS):
                terms[s, n, h] = res[:, h]

    def new_direction(cur, alpha, beta_prev):
        nxt = 1 - cur
        a, b = only(alpha), only(beta_prev)
        def body(p, total):
            w = h_buf[cur, p] - a * v_buf[cur, p] - b * v_buf[nxt, p]
            v_buf[nxt, p] = w
            return total + fold(w * w)

        return lax.fori_loop(0, phys, body, jnp.zeros(TILE, jnp.float32))

    def step(j, carry):
        alpha_part, beta_prev = carry
        cur = lax.rem(j, 2)
        nxt = 1 - cur
        more = j < last_step

        def alpha_z():
            sum_start(0, 1, sum_finish(0, 0))

        def alpha_plane():
            alpha = mean_of(sum_finish(0, 1))
            scal_ref[0, j] = alpha
            sum_start(1, 0, new_direction(cur, alpha, beta_prev))

        def beta_z():
            sum_start(1, 1, sum_finish(1, 0))

        def in_first(event, *what):
            @pl.when(j == 0)
            def _():
                event(*what)

        sum_start(0, 0, alpha_part)
        queue = MESSAGES[EARLY:]
        groups = groups_after(own + MESSAGES[:EARLY], queue)
        wide_steps = 3 * phys
        each = 3 if phys % 3 == 0 else 1
        half_steps = 2 * phys // each
        events = {}
        hooks = dict(zip(HOOKS, (alpha_z, alpha_plane, beta_z)))
        for n, count in enumerate(DURING_ONE):
            at = n * phys // 9 if n < 27 else wide_steps + (n - 27) * half_steps // 6
            at = events.setdefault(at, [])
            at += [functools.partial(take, message, groups) for message in queue[:count]]
            queue = queue[count:]
            if n in CHUNK_STEPS:
                first, count = CHUNKS[CHUNK_STEPS.index(n)]
                at += [sibling_copy(i).wait_recv for i in range(first // GROUP, (first + count) // GROUP)]
            if n in hooks:
                at.append(hooks[n])
            for event in (load_right.wait,) * (n == ENV_STEPS[0]):
                at.append(functools.partial(in_first, event))
            for first_step, event in zip(ENV_STEPS, (env_start, env_pass, env_far, env_share, env_done)):
                if 0 <= n - first_step < ENV_PIECES * ENV_STRIDE and (n - first_step) % ENV_STRIDE == 0:
                    at.append(functools.partial(in_first, event, (n - first_step) // ENV_STRIDE))

        def wide_step(i):
            with scope('events_wide'):
                at_steps(i, {n: e for n, e in events.items() if n < wide_steps})
            with scope('one_wide'):
                stage_one(lax.div(i, phys) * WIDE, WIDE, lax.rem(i, phys), i < phys)

        def half_step(i):
            with scope('events_half'):
                at_steps(i, {n - wide_steps: e for n, e in events.items() if n >= wide_steps})

            with scope('one_half'):
                chunk, p = lax.div(i * each, phys), lax.rem(i * each, phys)
                for q in range(each):
                    stage_one(3 * WIDE + chunk * (WIDE // 2), WIDE // 2, p + q, i < 0)

        repeat(0, wide_steps, wide_step)
        repeat(0, half_steps, half_step)
        with scope('gather_sent'):
            for message in MESSAGES:
                gather_copy(message).wait_send()
            repeat(0, BLOCKS, lambda i: sibling_copy(i).wait_send())

        @pl.when(more)
        def _():
            for link in ALL_LINKS:
                pl.semaphore_signal(ag_credit, inc=1, device_id=step_to(*link), device_id_type=MESH_IDS)
            pl.semaphore_signal(ag_credit, inc=1, device_id={'k': other}, device_id_type=MESH_IDS)

        @pl.when(j > 0)
        def _():
            pl.semaphore_wait(rs_credit, 2)

        def scale():
            beta = jnp.sqrt(mean_of(sum_finish(1, 1)))
            scal_ref[1, j] = beta
            inv = only(1.0 / beta)

            def normalize(p):
                v_buf[nxt, p] = v_buf[nxt, p] * inv
            repeat(0, phys, normalize)

            @pl.when(more)
            def _():
                pl.semaphore_wait(ag_credit, len(ALL_LINKS) + 1)

            @pl.when(j == last_step)
            def _():
                pack(1, lambda p: v_buf[nxt, p])
                turn_start(1)

        def finish(s):
            if s == 0:
                scale()
            with scope('ring_end'):
                for h in range(STREAMS):
                    for n in range(max(num_z - 3, 0), num_z - 1):
                        ring_wait(s, n, h)
            alpha, beta = scal_ref[0, j], scal_ref[1, j]
            a, b, inv = only(alpha), only(beta_prev), only(1.0 / beta)
            span = slice(s * slab, (s + 1) * slab)

            def body(p, total):
                new = []
                for h in range(STREAMS):
                    at = slice(s * slab + 8 * h, s * slab + 8 * h + 8)
                    g_new = terms[s, num_z - 1, h, p]
                    for n in range(max(num_z - 3, 0), num_z - 1):
                        g_new = g_new + ring[s, n, h, p]
                    new.append((g_new - a * h_buf[cur, p, at, :] - b * h_buf[nxt, p, at, :]) * inv)
                h_new = jnp.concatenate(new, axis=0)
                h_buf[nxt, p, span, :] = h_new
                for i, message in enumerate(own_parts(s)):
                    gath[0, INDEX[message], p] = h_new[i * piece:(i + 1) * piece]
                return total + fold(v_buf[nxt, p, span, :] * h_new)

            total = lax.fori_loop(0, phys, body, jnp.zeros(TILE, jnp.float32))
            alpha_sum[...] = total if s == 0 else alpha_sum[...] + total

            @pl.when(more)
            def _():
                for message in own_parts(s):
                    take(message, next_groups)

        def early(message):
            @pl.when(more)
            def _():
                take(message, next_groups)

        def happen(event):
            {'pass': ring_pass, 'finish': finish, 'early': early}[event[0]](*event[1:])

        pairs_z = num_z // 2
        ring_steps = PARTS * pairs_z
        events = {}
        for s in range(PARTS):
            for n in range(2, num_z - 1):
                at = s * pairs_z + n // 2 + LAGS[n - 2]
                events.setdefault(at, []).extend(('pass', s, n, h) for h in range(STREAMS))
            events.setdefault(FINISH[s] * pairs_z // SPAN, []).append(('finish', s))
        tail = [event for at in sorted(events) if at >= ring_steps for event in events.pop(at)]
        queue = MESSAGES[:EARLY]
        for at, count in enumerate(DURING_RING):
            events.setdefault(at * pairs_z // SPAN, []).extend(('early', message) for message in queue[:count])
            queue = queue[count:]
        mixed = []
        spare = list(DURING_TAIL)
        for i, event in enumerate(tail):
            mixed.append(event)
            count = len(queue) if i == len(tail) - 1 else spare.pop(0) if spare else 0
            mixed += [('early', message) for message in queue[:count]]
            queue = queue[count:]
        tail = mixed
        sequence = [event for at in sorted(events) for event in events[at]] + tail
        sequence = [
            message for kind, *what in sequence if kind != 'pass'
            for message in (own_parts(*what) if kind == 'finish' else what)]
        next_groups = groups_after((), sequence)

        def ring_step(i):
            s, t = lax.div(i, pairs_z), lax.rem(i, pairs_z)

            @pl.when(t == 0)
            def _():
                with scope('middle'):
                    for o in range(STREAMS):
                        middle(s * STREAMS + o)

            with scope('last_stage'):
                last_stage(s, (2 * t, 2 * t + 1))

            @pl.when(t == 0)
            def _():
                for n in range(min(2, num_z - 1)):
                    for h in range(STREAMS):
                        ring_copy(terms.at[s, n, h], s, n, h).start()

            with scope('events_ring'):
                at_steps(i, {at: [functools.partial(happen, event) for event in events[at]] for at in events})

        repeat(0, ring_steps, ring_step)
        with scope('tail'):
            for event in tail:
                happen(event)

        def ring_sent(i):
            s, n = lax.div(i, num_z - 1), lax.rem(i, num_z - 1)
            for h in range(STREAMS):
                ring_copy(terms.at[s, n, h], s, n, h).wait_send()
        repeat(0, PARTS * (num_z - 1), ring_sent)

        @pl.when(more)
        def _():
            for sign in (1, num_z - 1):
                pl.semaphore_signal(
                    rs_credit, inc=1, device_id={'z': lax.rem(z + sign, num_z)}, device_id_type=MESH_IDS)

        return alpha_sum[...], jnp.where(j > 0, scal_ref[1, j], 0.0)

    zero = jnp.zeros(TILE, jnp.float32)
    _, beta_prev = lax.fori_loop(0, LANCZOS_STEPS, step, (zero, zero))
    repeat(0, ENV_PIECES, env_sent)

    cur = LANCZOS_STEPS % 2
    shift = only(scal_ref[0, last_step])
    b = only(beta_prev)

    def end_body(p, sums):
        h, v = h_buf[cur, p], v_buf[cur, p]
        d = h - shift * v - b * v_buf[1 - cur, p]
        h_buf[1 - cur, p] = d
        return tuple(total + fold(term) for total, term in zip(sums, (v * h, d * d, d * v, v * v)))

    sums = lax.fori_loop(0, phys, end_body, (zero,) * 4)
    row = lax.broadcasted_iota(jnp.int32, TILE, 0)

    def squeeze(tile):
        tile = tile + pltpu.roll(tile, 4, 0)
        return tile + pltpu.roll(tile, 2, 0)

    packed = squeeze(sums[0])
    for i in range(1, 4):
        packed = jnp.where(row >= 2 * i, squeeze(sums[i]), packed)
    with scope('end_sum'):
        sum_start(0, 0, packed)
        pack(0, lambda p: h_buf[1 - cur, p])
        turn_start(0)
        sum_start(0, 1, sum_finish(0, 0))
        packed = sum_finish(0, 1)
    v_h, d_d, d_v, v_v = (mean_of(jnp.where((row >= 2 * i) & (row < 2 * i + 2), packed, 0.0)) for i in range(4))
    delta = v_h - shift
    beta = jnp.sqrt(d_d - 2.0 * delta * d_v + delta * delta * v_v)
    scal_ref[0, LANCZOS_STEPS] = v_h
    scal_ref[1, LANCZOS_STEPS] = beta
    inv = only(1.0 / beta)
    delta = only(delta)
    with scope('end_turn_wait'):
        turn_finish(1)
        turn_finish(0)
    with scope('end_turn'):
        def end_unpack(pair):
            block = jnp.transpose((turned(0, pair) - delta * turned(1, pair)) * inv)
            for i, p in enumerate((2 * pair, jnp.minimum(2 * pair + 1, phys - 1))):
                out_ref[p] = block[i * rows:(i + 1) * rows, :]
        repeat(0, pairs, end_unpack)


def solution(mesh):
    grid = fine_mesh(mesh)
    num_z = grid.shape['z']

    def local_run(psi_blk, left_blk, right_blk, mpo_pair):
        full_rows, n_s, n_u, local_cols = psi_blk.shape
        phys = n_s * n_u
        rows = full_rows // RING
        cols = local_cols * RING
        bonds_l, bonds_r = left_blk.shape[1], right_blk.shape[1]
        full_a, full_b = left_blk.shape[2], right_blk.shape[2]
        psi = psi_blk.transpose(1, 2, 3, 0).reshape(phys, local_cols, full_rows)
        left = left_blk.transpose(1, 0, 2)
        right = right_blk.transpose(1, 0, 2).reshape(bonds_r, RING, CORES, 8, full_b)
        mpo = mpo_pair.transpose(0, 2, 3, 4, 5, 1).reshape(bonds_l * phys, phys * bonds_r)
        eye = np.eye(8, dtype=np.float32)
        one = np.ones((1, 8), np.float32)
        order_out = np.arange(phys * bonds_r).reshape(phys, bonds_r).T.ravel()
        order_in = np.arange(bonds_l * phys).reshape(bonds_l, phys).T.ravel()
        spread_out = np.kron(np.eye(order_out.size, dtype=np.float32)[order_out], one.T)
        spread_in = np.kron(np.eye(order_in.size, dtype=np.float32)[:, order_in], one)
        same = np.tile(eye, (1, phys * bonds_l))
        red = num_z + RING * RING * CORES
        pairs = (phys + 1) // 2
        f32 = jnp.float32
        out, scal = pl.pallas_call(
            functools.partial(lanczos_kernel, float(psi_blk.size * grid.size), num_z),
            out_shape=(
                jax.ShapeDtypeStruct((phys, local_cols, full_rows), f32),
                jax.ShapeDtypeStruct((2, LANCZOS_STEPS + 1) + TILE, f32),
            ),
            in_specs=[
                pl.BlockSpec(memory_space=pltpu.VMEM),
                pl.BlockSpec(memory_space=pl.ANY),
                pl.BlockSpec(memory_space=pl.ANY),
            ] + [pl.BlockSpec(memory_space=pltpu.VMEM)] * 4,
            out_specs=(pl.BlockSpec(memory_space=pltpu.VMEM), pl.BlockSpec(memory_space=pltpu.VMEM)),
            scratch_shapes=[
                pltpu.VMEM((CORES, len(HELD), phys, rows // TREES, cols), f32),
                pltpu.VMEM((bonds_r, BLOCKS, CORES, 8, full_b), f32),
                pltpu.VMEM((bonds_l, rows, full_a), f32),
                pltpu.VMEM((2, rows, full_a), f32),
                pltpu.VMEM((bonds_l, rows, full_a), f32),
                pltpu.VMEM((bonds_r * phys * 8, phys * bonds_l * 8), f32),
                pltpu.VMEM((phys, bonds_l, rows // 8, 8, cols), f32),
                pltpu.VMEM((phys, rows // 8, 8, bonds_r * cols), f32),
                pltpu.VMEM((PARTS, num_z, STREAMS, phys, 8, cols), f32),
                pltpu.VMEM((PARTS, num_z - 1, STREAMS, phys, 8, cols), f32),
                pltpu.VMEM((2, phys, rows, cols), f32),
                pltpu.VMEM((2, phys, rows, cols), f32),
                pltpu.VMEM((2, RING, pairs, rows, LANES), f32),
                pltpu.VMEM((2, RING, pairs, rows, LANES), f32),
                pltpu.VMEM((2, 2) + TILE, f32),
                pltpu.VMEM((2, red) + TILE, f32),
                pltpu.VMEM(TILE, f32),
                pltpu.SemaphoreType.DMA((len(HELD),)),
                pltpu.SemaphoreType.DMA((len(HELD),)),
                pltpu.SemaphoreType.DMA((BLOCKS,)),
                pltpu.SemaphoreType.DMA((BLOCKS,)),
                pltpu.SemaphoreType.DMA((PARTS, num_z - 1, STREAMS)),
                pltpu.SemaphoreType.DMA((PARTS, num_z - 1, STREAMS)),
                pltpu.SemaphoreType.DMA((2, red)),
                pltpu.SemaphoreType.DMA((2, red)),
                pltpu.SemaphoreType.DMA((2, RING)),
                pltpu.SemaphoreType.DMA((2, RING)),
                pltpu.SemaphoreType.DMA((15, ENV_PIECES)),
                pltpu.SemaphoreType.DMA((15, ENV_PIECES)),
                pltpu.SemaphoreType.DMA((2,)),
                pltpu.SemaphoreType.REGULAR,
                pltpu.SemaphoreType.REGULAR,
            ],
            compiler_params=pltpu.CompilerParams(
                collective_id=0, has_side_effects=True, vmem_limit_bytes=67043328),
        )(psi, left, right, mpo, spread_out, spread_in, same)
        result = out.reshape(n_s, n_u, local_cols, full_rows).transpose(3, 0, 1, 2)
        return scal[0, 1:, 0, 0], scal[1, 1:, 0, 0], result

    return jax.shard_map(
        local_run, mesh=grid,
        in_specs=(P(('x', 'k'), None, None, ('z', 'y')), P(('x', 'k'), None, None), P(('z', 'y'), None, None), P()),
        out_specs=(P(), P(), P(('x', 'k'), None, None, ('z', 'y'))), check_vma=False)
```

```python
import functools
import itertools

import jax
import jax.numpy as jnp
import numpy as np
from jax import lax
from jax.experimental import pallas as pl
from jax.experimental.pallas import tpu as pltpu
from jax.sharding import Mesh, PartitionSpec as P

LANCZOS_STEPS = 4
FULL_PREC = lax.Precision.HIGHEST
MESH_IDS = pl.DeviceIdType.MESH
scope = jax.named_scope
SUB = 8
LANES = 128
TILE = (SUB, LANES)
RING = 4
CORES = 2
PARTS = 4
STREAMS = 2
TREES = 4
BLOCKS = RING * RING
ALL_LINKS = [('x', 1), ('y', 1), ('x', -1), ('y', -1)]


def fine_mesh(mesh):
    shape = (mesh.shape['col'] // RING, RING, mesh.shape['row'] // CORES, CORES)
    return Mesh(mesh.devices.reshape(shape), ('z', 'y', 'x', 'k'))


def near(d):
    return min(d, RING - d)


def make_tree(turn):
    prefer = ALL_LINKS[turn:] + ALL_LINKS[:turn]
    load = dict.fromkeys(prefer, 0)
    tree = {}
    for offset in sorted(itertools.product(range(RING), repeat=2), key=lambda o: near(o[0]) + near(o[1])):
        options = [
            (axis, sign) for axis, d in zip('xy', offset) for sign in (-1, 1)
            if d and (-sign * d) % RING == near(d)]
        if options:
            tree[offset] = min(options, key=lambda link: (load[link], prefer.index(link)))
            load[tree[offset]] += 1
    return tree


def source_of(message):
    part, dx, dy = message
    axis, sign = LINKS[message]
    return (part, (dx + sign) % RING, dy) if axis == 'x' else (part, dx, (dy + sign) % RING)


LINKS = {(part, *offset): link for part in range(TREES) for offset, link in make_tree(part % len(ALL_LINKS)).items()}
SENDS = {}
for sent in LINKS:
    SENDS.setdefault(source_of(sent), []).append(sent)


def gather_order(release):
    free = dict.fromkeys(ALL_LINKS, 0.0)
    arrival = {}
    order = []

    def issue(now, message):
        order.append(message)
        for sent in SENDS.get(message, ()):
            link = LINKS[sent]
            free[link] = max(free[link], now) + 1.0
            arrival[sent] = free[link] + 0.6

    todo = [(now, (part, 0, 0)) for part, now in enumerate(release)]
    while len(order) < TREES * BLOCKS:
        left = [(now, message) for message, now in arrival.items() if message not in order]
        if todo and (not left or min(left)[0] > todo[0][0]):
            issue(*todo.pop(0))
        else:
            issue(*min(left))
    return order


def counts(*texts):
    return [int(c) for text in texts for c in text]


RELEASE = [0, 2.9, 3.5, 5.5]
PAIR_ORDER = counts('0101202101323332')
LAGS = (counts('11021'), counts('16253'), counts('14130'), counts('02445'))
FINISH = [11, 15, 28, 29]
HOOKS = (1, 11, 16)
DURING_ONE = counts('113202510123420221111120300', '011200')
DURING_RING = counts('0000000000000311')
DURING_TAIL = counts('07002100')
EARLY = sum(DURING_RING) + sum(DURING_TAIL)
ENV_PIECES = 4
ENV_STRIDE = 3
ENV_STEPS = (0, 6, 14, 15, 22)
CHUNK_STEPS = (0, 9, 18, 27, 30)
SPAN = 4
HELD = gather_order(RELEASE)
INDEX = {message: i for i, message in enumerate(HELD)}
MESSAGES = [message for message in HELD if message in LINKS]
GROUP = TREES
WIDE = len(HELD) // 4
CHUNKS = [(c * WIDE, WIDE) for c in range(3)] + [(3 * WIDE + c * WIDE // 2, WIDE // 2) for c in range(2)]


def dot(lhs, rhs):
    return jnp.dot(lhs, rhs, precision=FULL_PREC, preferred_element_type=jnp.float32)


def lanczos_kernel(
        num_elems, num_z, psi_ref, left_ref, right_ref, mpo_ref, spread_out_ref, spread_in_ref, same_ref, out_ref, scal_ref,
        gath, right_full, left_own, left_turn, left_perm, w_mat, acc, mid, terms, ring, h_buf, v_buf, pack_out, pack_in,
        red_held, red_slots, alpha_sum,
        ag_send, ag_recv, sib_send, sib_recv, rs_send, rs_recv, red_send, red_recv, turn_send, turn_recv,
        env_send, env_recv, load_sem, ag_credit, rs_credit):
    phys, rows, cols = h_buf.shape[1:]
    bonds = right_full.shape[0]
    bonds_l = left_own.shape[0]
    piece = rows // TREES
    slab = rows // PARTS
    octs = rows // 8
    pairs = pack_in.shape[2]
    last_step = LANCZOS_STEPS - 1
    z, y, x, k = (lax.axis_index(name) for name in ('z', 'y', 'x', 'k'))
    other = 1 - k

    x_at, y_at = ([lax.rem(pos + d, RING) for d in range(RING)] for pos in (x, y))
    k_at = (k, other)

    def step_to(axis, sign):
        return {axis: {'x': x_at, 'y': y_at}[axis][sign % RING]}

    phases = (
        (num_z, z, lambda i: {'z': i}),
        (RING * RING * CORES, (x * CORES + k) * RING + y,
         lambda i: {'x': lax.div(i, CORES * RING), 'k': lax.rem(lax.div(i, RING), CORES), 'y': lax.rem(i, RING)}),
    )
    bases = (0, num_z)
    barrier = pltpu.get_barrier_semaphore()
    def repeat(lo, hi, fn):
        def body(i, c):
            fn(i)
            return c
        lax.fori_loop(lo, hi, body, 0)

    for count, me, device in phases:
        def enter(d, count=count, me=me, device=device):
            pl.semaphore_signal(barrier, inc=1, device_id=device(lax.rem(me + d, count)), device_id_type=MESH_IDS)
        repeat(1, count, enter)

    own_rows = pl.multiple_of(y * rows, rows)
    load_left = pltpu.make_async_copy(left_ref.at[:, pl.ds(own_rows, rows), :], left_own, load_sem.at[0])
    load_left.start()
    load_right = pltpu.make_async_copy(right_ref, right_full.at[:, pl.ds(y * RING, RING)], load_sem.at[1])
    load_right.start()

    lane = lax.broadcasted_iota(jnp.int32, (rows, LANES), 1)

    def pack(which, value):
        def body(pair):
            halves = [value(2 * pair), value(jnp.minimum(2 * pair + 1, phys - 1))]
            for target in range(RING):
                tile, half = divmod(target * rows, LANES)
                first, second = (v[:, tile * LANES:(tile + 1) * LANES] for v in halves)
                if half == 0:
                    second = pltpu.roll(second, rows, 1)
                else:
                    first = pltpu.roll(first, rows, 1)
                pack_out[which, target, pair] = jnp.where(lane < rows, first, second)
        repeat(0, pairs, body)

    def turn_copy(which, src, dst, d, device):
        return pltpu.make_async_remote_copy(
            src_ref=pack_out.at[which, src], dst_ref=pack_in.at[which, dst],
            send_sem=turn_send.at[which, d], recv_sem=turn_recv.at[which, dst],
            device_id=device, device_id_type=MESH_IDS)

    def turn_start(which):
        for d in range(1, RING):
            peer = y_at[d]
            turn_copy(which, peer, y, d, {'y': peer}).start()
        pack_in[which, y] = pack_out[which, y]

    def turn_finish(which):
        for d in range(1, RING):
            peer = y_at[d]
            copy = turn_copy(which, peer, peer, d, {'y': peer})
            copy.wait_send()
            copy.wait_recv()

    def turned(which, pair):
        return jnp.concatenate([pack_in[which, i, pair] for i in range(RING)], axis=0)

    with scope('pack'):
        pack(0, lambda p: psi_ref[p])
    with scope('entry_barrier'):
        pl.semaphore_wait(barrier, sum(count - 1 for count, _, _ in phases))
    turn_start(0)
    h_buf[1] = jnp.zeros(h_buf.shape[1:], jnp.float32)
    v_buf[...] = jnp.zeros(v_buf.shape, jnp.float32)

    def sum_start(which, phase, value):
        count, me, device = phases[phase]
        red_held[which, phase] = value

        def send(d):
            pltpu.make_async_remote_copy(
                src_ref=red_held.at[which, phase], dst_ref=red_slots.at[which, bases[phase] + me],
                send_sem=red_send.at[which, bases[phase] + d], recv_sem=red_recv.at[which, bases[phase] + me],
                device_id=device(lax.rem(me + d, count)), device_id_type=MESH_IDS).start()
        repeat(1, count, send)
        red_slots[which, bases[phase] + me] = value

    def sum_finish(which, phase):
        count, me, device = phases[phase]

        def wait(d):
            peer = lax.rem(me + d, count)
            copy = pltpu.make_async_remote_copy(
                src_ref=red_held.at[which, phase], dst_ref=red_slots.at[which, bases[phase] + peer],
                send_sem=red_send.at[which, bases[phase] + d], recv_sem=red_recv.at[which, bases[phase] + peer],
                device_id=device(peer), device_id_type=MESH_IDS)
            copy.wait_send()
            copy.wait_recv()
        repeat(1, count, wait)
        return red_slots[which, bases[phase]:bases[phase] + count].sum(0)

    def mean_of(value):
        return jnp.broadcast_to(jnp.sum(value, axis=(0, 1), keepdims=True) * (1.0 / num_elems), TILE)

    def only(tile):
        return tile[:1, :1]

    def fold(values):
        lanes = values.reshape(-1, 8, cols).sum(0)
        tile = lanes[:, :LANES]
        for c in range(LANES, cols, LANES):
            tile = tile + lanes[:, c:c + LANES]
        return tile

    def gather_copy(message):
        index = INDEX[message]
        return pltpu.make_async_remote_copy(
            src_ref=gath.at[0, INDEX[source_of(message)]], dst_ref=gath.at[0, index],
            send_sem=ag_send.at[index], recv_sem=ag_recv.at[index],
            device_id=step_to(*LINKS[message]), device_id_type=MESH_IDS)

    def sibling_copy(index):
        span = pl.ds(index * GROUP, GROUP)
        return pltpu.make_async_remote_copy(
            src_ref=gath.at[0, span], dst_ref=gath.at[1, span],
            send_sem=sib_send.at[index], recv_sem=sib_recv.at[index],
            device_id={'k': other}, device_id_type=MESH_IDS)

    def groups_after(held, sequence):
        done = {}
        held = set(held)
        for message in sequence:
            held.add(message)
            for i in range(BLOCKS):
                group = HELD[i * GROUP:(i + 1) * GROUP]
                if message in group and held.issuperset(group):
                    done.setdefault(message, []).append(i)
        return done

    def take(message, groups):
        if message in LINKS:
            gather_copy(message).wait_recv()
        for sent in SENDS.get(message, ()):
            gather_copy(sent).start()
        for i in groups.get(message, ()):
            sibling_copy(i).start()

    def own_parts(s):
        each = TREES // PARTS
        return [(s * each + i, 0, 0) for i in range(each)]

    with scope('turn_wait'):
        turn_finish(0)
    with scope('turn'):
        def unpack(pair):
            block = jnp.transpose(turned(0, pair))
            for i, p in enumerate((2 * pair, jnp.minimum(2 * pair + 1, phys - 1))):
                h_buf[0, p] = block[i * rows:(i + 1) * rows, :]
                for part in range(TREES):
                    span = slice(i * rows + part * piece, i * rows + (part + 1) * piece)
                    gath[0, INDEX[part, 0, 0], p] = block[span, :]
        repeat(0, pairs, unpack)
    own = [message for message in HELD if message not in LINKS]
    groups = groups_after((), own + MESSAGES[:EARLY])
    for message in own:
        take(message, groups)

    with scope('left'):
        load_left.wait()
    order = []
    for first, count in CHUNKS:
        order += [(dk, message) for dk in range(CORES) for message in HELD[first:first + count]]
    per_tile = LANES // piece
    lanes = lax.broadcasted_iota(jnp.int32, (rows, LANES), 1)

    left_tiles = {
        (dx, dk, dy): pl.multiple_of(lax.div((x_at[dx] * CORES + k_at[dk]) * RING + y_at[dy], 2) * LANES, LANES)
        for dx in range(RING) for dk in range(CORES) for dy in range(RING)}

    def left_rows(l, c):
        for tile in range(left_own.shape[2] // LANES):
            at = slice(tile * LANES, (tile + 1) * LANES)
            plain = left_own[l, :, at]
            rolled = pltpu.roll(plain, rows, 1)
            left_turn[0, :, at] = jnp.where(lax.rem(y, 2) == 0, plain, rolled)
            left_turn[1, :, at] = jnp.where(lax.rem(y, 2) == 0, rolled, plain)
        for tile in range(left_perm.shape[2] // LANES):
            result = None
            for i in range(per_tile):
                dk, message = order[tile * per_tile + i]
                _, dx, dy = message
                values = left_turn[dy % 2, :, pl.ds(left_tiles[dx, dk, dy], LANES)]
                if i != message[0]:
                    values = pltpu.roll(values, (i - message[0]) * piece % LANES, 1)
                result = values if i == 0 else jnp.where(lanes >= i * piece, values, result)
            left_perm[l, :, tile * LANES:(tile + 1) * LANES] = result
        return c

    with scope('left_order'):
        lax.fori_loop(0, bonds_l, left_rows, 0)

    with scope('mpo'):
        rows_out = lax.dot_general(
            spread_out_ref[...], mpo_ref[...], (((1,), (1,)), ((), ())), precision=FULL_PREC,
            preferred_element_type=jnp.float32)
        wide = dot(rows_out, spread_in_ref[...])
        n_out, n_in = w_mat.shape
        same = jnp.broadcast_to(same_ref[...][None], (n_out // 8, 8, n_in)).reshape(n_out, n_in)
        w_mat[...] = wide * same

    with scope('gather_early'):
        for message in MESSAGES[:EARLY]:
            take(message, groups)

    def stage_one(first, count, p, fresh):
        depth = count * piece
        rhs = jnp.concatenate(
            [gath[dk, pl.ds(first, count), p].reshape(depth, cols) for dk in range(CORES)], axis=0)
        column = pl.multiple_of(first * CORES * piece, LANES)
        lhs = left_perm[:, :, pl.ds(column, CORES * depth)].reshape(bonds_l * rows, CORES * depth)
        res = dot(lhs, rhs).reshape(bonds_l, octs, 8, cols)
        acc[p] = jnp.where(fresh, 0.0, acc[p]) + res

    def at_steps(i, events):
        steps = sorted(events)

        def run(steps):
            if len(steps) > 1:
                middle = len(steps) // 2
                lax.cond(i < steps[middle], lambda: run(steps[:middle]), lambda: run(steps[middle:]))
            else:
                for step in steps:
                    @pl.when(i == step)
                    def _():
                        for event in events[step]:
                            event()

        run(steps)

    up, down, far = y_at[1], y_at[3], y_at[2]
    strip = right_full.shape[-1] // ENV_PIECES

    def env_copy(kind, c, block, device, count=1, core=None):
        span = pl.ds(c * strip, strip)
        row = k if core is None else core
        view = right_full.at[:, pl.ds(block, count), pl.ds(row, 1), :, span]
        return pltpu.make_async_remote_copy(
            src_ref=view, dst_ref=view, send_sem=env_send.at[kind, c], recv_sem=env_recv.at[kind, c],
            device_id=device, device_id_type=MESH_IDS)

    def block_of(owner, d):
        return owner * RING + x_at[d]

    TAKEN = (0, 1)

    def env_start(c):
        for d in TAKEN:
            env_copy(d, c, block_of(y, d), {'y': up}).start()
            env_copy(2 + d, c, block_of(y, d), {'y': down}).start()

    def env_pass_x(c, i, owner):
        env_copy(6 + i, c, block_of(owner, 0), {'x': x_at[1]}).start()
        env_copy(9 + i, c, block_of(owner, 1), {'x': x_at[3]}).start()

    def env_pass(c):
        for d in TAKEN:
            env_copy(d, c, block_of(down, d), {'y': up}).wait_recv()
            env_copy(2 + d, c, block_of(up, d), {'y': down}).wait_recv()
        env_copy(4, c, block_of(down, 0), {'y': up}).start()
        env_copy(5, c, block_of(up, 1), {'y': down}).start()
        env_pass_x(c, 0, down)
        env_pass_x(c, 1, up)

    def env_far(c):
        env_copy(4, c, block_of(far, 0), {'y': up}).wait_recv()
        env_copy(5, c, block_of(far, 1), {'y': down}).wait_recv()
        env_pass_x(c, 2, far)

    def env_share(c):
        for i, owner in enumerate((down, up, far)):
            env_copy(6 + i, c, block_of(owner, 3), {'x': x_at[1]}).wait_recv()
            env_copy(9 + i, c, block_of(owner, 2), {'x': x_at[3]}).wait_recv()
            env_copy(12 + i, c, owner * RING, {'k': other}, RING).start()

    def env_done(c):
        for i, owner in enumerate((down, up, far)):
            env_copy(12 + i, c, owner * RING, {'k': other}, RING, other).wait_recv()

    def env_sent(c):
        for kind in range(12):
            env_copy(kind, c, 0, {'k': other}).wait_send()
        for i in range(3):
            env_copy(12 + i, c, 0, {'k': other}, RING).wait_send()

    def way(s):
        return 1 - 2 * lax.rem(s, 2)

    def ring_side(s, n):
        return way(s) * (1 - 2 * lax.rem(n, 2))

    def ring_block(s, n):
        return lax.rem(z + num_z + ring_side(s, n) * (num_z // 2 - lax.div(n + 1, 2)), num_z)

    def ring_copy(src, s, n, h):
        return pltpu.make_async_remote_copy(
            src_ref=src, dst_ref=ring.at[s, n, h], send_sem=rs_send.at[s, n, h], recv_sem=rs_recv.at[s, n, h],
            device_id={'z': lax.rem(z + num_z + ring_side(s, n), num_z)}, device_id_type=MESH_IDS)

    def ring_wait(s, n, h):
        ring_copy(terms.at[s, n, h], s, n, h).wait_recv()

    def ring_pass(s, n, h):
        with scope('ring_pass'):
            ring_wait(s, n - 2, h)
            ring[s, n - 2, h] = ring[s, n - 2, h] + terms[s, n, h]
            ring_copy(ring.at[s, n - 2, h], s, n, h).start()

    def middle(o):
        res = dot(w_mat[...], acc[:, :, o].reshape(phys * bonds_l * 8, cols)).reshape(bonds, phys, 8, cols)
        for r in range(bonds):
            mid[:, o, :, r * cols:(r + 1) * cols] = res[r]

    def last_stage(s, which):
        lhs = mid[:, pl.ds(s * STREAMS, STREAMS)].reshape(phys * slab, bonds * cols)
        for n in which:
            first = pl.multiple_of(ring_block(s, n) * cols, cols)
            rhs = right_full[:, :, :, :, pl.ds(first, cols)].reshape(bonds * cols, cols)
            res = dot(lhs, rhs).reshape(phys, STREAMS, 8, cols)
            for h in range(STREAMS):
                terms[s, n, h] = res[:, h]

    def new_direction(cur, alpha, beta_prev):
        nxt = 1 - cur
        a, b = only(alpha), only(beta_prev)
        def body(p, total):
            w = h_buf[cur, p] - a * v_buf[cur, p] - b * v_buf[nxt, p]
            v_buf[nxt, p] = w
            return total + fold(w * w)

        return lax.fori_loop(0, phys, body, jnp.zeros(TILE, jnp.float32))

    def step(j, carry):
        alpha_part, beta_prev = carry
        cur = lax.rem(j, 2)
        nxt = 1 - cur
        more = j < last_step

        def alpha_z():
            sum_start(0, 1, sum_finish(0, 0))

        def alpha_plane():
            alpha = mean_of(sum_finish(0, 1))
            scal_ref[0, j] = alpha
            sum_start(1, 0, new_direction(cur, alpha, beta_prev))

        def beta_z():
            sum_start(1, 1, sum_finish(1, 0))

        def in_first(event, *what):
            @pl.when(j == 0)
            def _():
                event(*what)

        sum_start(0, 0, alpha_part)
        queue = MESSAGES[EARLY:]
        groups = groups_after(own + MESSAGES[:EARLY], queue)
        wide_steps = 3 * phys
        each = 3 if phys % 3 == 0 else 1
        half_steps = 2 * phys // each
        events = {}
        hooks = dict(zip(HOOKS, (alpha_z, alpha_plane, beta_z)))
        for n, count in enumerate(DURING_ONE):
            at = n * phys // 9 if n < 27 else wide_steps + (n - 27) * half_steps // 6
            at = events.setdefault(at, [])
            at += [functools.partial(take, message, groups) for message in queue[:count]]
            queue = queue[count:]
            for event in (load_right.wait,) * (n == ENV_STEPS[0]):
                at.append(functools.partial(in_first, event))
            for first_step, event in zip(ENV_STEPS, (env_start, env_pass, env_far, env_share, env_done)):
                if 0 <= n - first_step < ENV_PIECES * ENV_STRIDE and (n - first_step) % ENV_STRIDE == 0:
                    at.append(functools.partial(in_first, event, (n - first_step) // ENV_STRIDE))
            if n in CHUNK_STEPS:
                first, count = CHUNKS[CHUNK_STEPS.index(n)]
                at += [sibling_copy(i).wait_recv for i in range(first // GROUP, (first + count) // GROUP)]
            if n in hooks:
                at.append(hooks[n])

        def wide_step(i):
            with scope('events_wide'):
                at_steps(i, {n: e for n, e in events.items() if n < wide_steps})
            with scope('one_wide'):
                stage_one(lax.div(i, phys) * WIDE, WIDE, lax.rem(i, phys), i < phys)

        def half_step(i):
            with scope('events_half'):
                at_steps(i, {n - wide_steps: e for n, e in events.items() if n >= wide_steps})

            with scope('one_half'):
                chunk, p = lax.div(i * each, phys), lax.rem(i * each, phys)
                for q in range(each):
                    stage_one(3 * WIDE + chunk * (WIDE // 2), WIDE // 2, p + q, i < 0)

        repeat(0, wide_steps, wide_step)
        repeat(0, half_steps, half_step)
        with scope('gather_sent'):
            for message in MESSAGES:
                gather_copy(message).wait_send()
            repeat(0, BLOCKS, lambda i: sibling_copy(i).wait_send())

        @pl.when(more)
        def _():
            for link in ALL_LINKS:
                pl.semaphore_signal(ag_credit, inc=1, device_id=step_to(*link), device_id_type=MESH_IDS)
            pl.semaphore_signal(ag_credit, inc=1, device_id={'k': other}, device_id_type=MESH_IDS)

        @pl.when(j > 0)
        def _():
            pl.semaphore_wait(rs_credit, 2)

        def scale():
            beta = jnp.sqrt(mean_of(sum_finish(1, 1)))
            scal_ref[1, j] = beta
            inv = only(1.0 / beta)

            def normalize(p):
                v_buf[nxt, p] = v_buf[nxt, p] * inv
            repeat(0, phys, normalize)

            @pl.when(more)
            def _():
                pl.semaphore_wait(ag_credit, len(ALL_LINKS) + 1)

            @pl.when(j == last_step)
            def _():
                pack(1, lambda p: v_buf[nxt, p])
                turn_start(1)

        def finish(s):
            if s == 0:
                scale()
            with scope('ring_end'):
                for h in range(STREAMS):
                    for n in range(max(num_z - 3, 0), num_z - 1):
                        ring_wait(s, n, h)
            alpha, beta = scal_ref[0, j], scal_ref[1, j]
            a, b, inv = only(alpha), only(beta_prev), only(1.0 / beta)
            span = slice(s * slab, (s + 1) * slab)

            def body(p, total):
                new = []
                for h in range(STREAMS):
                    at = slice(s * slab + 8 * h, s * slab + 8 * h + 8)
                    g_new = terms[s, num_z - 1, h, p]
                    for n in range(max(num_z - 3, 0), num_z - 1):
                        g_new = g_new + ring[s, n, h, p]
                    new.append((g_new - a * h_buf[cur, p, at, :] - b * h_buf[nxt, p, at, :]) * inv)
                h_new = jnp.concatenate(new, axis=0)
                h_buf[nxt, p, span, :] = h_new
                for i, message in enumerate(own_parts(s)):
                    gath[0, INDEX[message], p] = h_new[i * piece:(i + 1) * piece]
                return total + fold(v_buf[nxt, p, span, :] * h_new)

            total = lax.fori_loop(0, phys, body, jnp.zeros(TILE, jnp.float32))
            alpha_sum[...] = total if s == 0 else alpha_sum[...] + total

            @pl.when(more)
            def _():
                for message in own_parts(s):
                    take(message, next_groups)

        def early(message):
            @pl.when(more)
            def _():
                take(message, next_groups)

        def happen(event):
            {'pass': ring_pass, 'finish': finish, 'early': early}[event[0]](*event[1:])

        pairs_z = num_z // 2
        ring_steps = PARTS * pairs_z
        pairs_at = []
        for s in PAIR_ORDER:
            if sum(s == other_s for other_s, _ in pairs_at) < pairs_z:
                pairs_at.append((s, sum(s == other_s for other_s, _ in pairs_at)))
        slots = {pair: i for i, pair in enumerate(pairs_at)}
        events = {}
        for s in range(PARTS):
            for n in range(2, num_z - 1):
                at = slots[s, n // 2] + LAGS[s][n - 2]
                events.setdefault(at, []).extend(('pass', s, n, h) for h in range(STREAMS))
            events.setdefault(FINISH[s] * pairs_z // SPAN, []).append(('finish', s))
        tail = [event for at in sorted(events) if at >= ring_steps for event in events.pop(at)]
        queue = MESSAGES[:EARLY]
        for at, count in enumerate(DURING_RING):
            events.setdefault(at * pairs_z // SPAN, []).extend(('early', message) for message in queue[:count])
            queue = queue[count:]
        mixed = []
        spare = list(DURING_TAIL)
        for i, event in enumerate(tail):
            mixed.append(event)
            count = len(queue) if i == len(tail) - 1 else spare.pop(0) if spare else 0
            mixed += [('early', message) for message in queue[:count]]
            queue = queue[count:]
        tail = mixed
        sequence = [event for at in sorted(events) for event in events[at]] + tail
        sequence = [
            message for kind, *what in sequence if kind != 'pass'
            for message in (own_parts(*what) if kind == 'finish' else what)]
        next_groups = groups_after((), sequence)

        def ring_step(i):
            s, t = pairs_at[0]
            for n, pair in enumerate(pairs_at):
                s, t = jnp.where(i == n, pair[0], s), jnp.where(i == n, pair[1], t)

            @pl.when(t == 0)
            def _():
                with scope('middle'):
                    for o in range(STREAMS):
                        middle(s * STREAMS + o)

            with scope('last_stage'):
                last_stage(s, (2 * t, 2 * t + 1))

            @pl.when(t == 0)
            def _():
                for n in range(min(2, num_z - 1)):
                    for h in range(STREAMS):
                        ring_copy(terms.at[s, n, h], s, n, h).start()

            with scope('events_ring'):
                at_steps(i, {at: [functools.partial(happen, event) for event in events[at]] for at in events})

        repeat(0, ring_steps, ring_step)
        with scope('tail'):
            for event in tail:
                happen(event)

        def ring_sent(i):
            s, n = lax.div(i, num_z - 1), lax.rem(i, num_z - 1)
            for h in range(STREAMS):
                ring_copy(terms.at[s, n, h], s, n, h).wait_send()
        repeat(0, PARTS * (num_z - 1), ring_sent)

        @pl.when(more)
        def _():
            for sign in (1, num_z - 1):
                pl.semaphore_signal(
                    rs_credit, inc=1, device_id={'z': lax.rem(z + sign, num_z)}, device_id_type=MESH_IDS)

        return alpha_sum[...], jnp.where(j > 0, scal_ref[1, j], 0.0)

    zero = jnp.zeros(TILE, jnp.float32)
    _, beta_prev = lax.fori_loop(0, LANCZOS_STEPS, step, (zero, zero))
    repeat(0, ENV_PIECES, env_sent)

    cur = LANCZOS_STEPS % 2
    shift = only(scal_ref[0, last_step])
    b = only(beta_prev)

    def end_body(p, sums):
        h, v = h_buf[cur, p], v_buf[cur, p]
        d = h - shift * v - b * v_buf[1 - cur, p]
        h_buf[1 - cur, p] = d
        return tuple(total + fold(term) for total, term in zip(sums, (v * h, d * d, d * v, v * v)))

    sums = lax.fori_loop(0, phys, end_body, (zero,) * 4)
    row = lax.broadcasted_iota(jnp.int32, TILE, 0)

    def squeeze(tile):
        tile = tile + pltpu.roll(tile, 4, 0)
        return tile + pltpu.roll(tile, 2, 0)

    packed = squeeze(sums[0])
    for i in range(1, 4):
        packed = jnp.where(row >= 2 * i, squeeze(sums[i]), packed)
    with scope('end_sum'):
        sum_start(0, 0, packed)
        pack(0, lambda p: h_buf[1 - cur, p])
        turn_start(0)
        sum_start(0, 1, sum_finish(0, 0))
        packed = sum_finish(0, 1)
    v_h, d_d, d_v, v_v = (mean_of(jnp.where((row >= 2 * i) & (row < 2 * i + 2), packed, 0.0)) for i in range(4))
    delta = v_h - shift
    beta = jnp.sqrt(d_d - 2.0 * delta * d_v + delta * delta * v_v)
    scal_ref[0, LANCZOS_STEPS] = v_h
    scal_ref[1, LANCZOS_STEPS] = beta
    inv = only(1.0 / beta)
    delta = only(delta)
    with scope('end_turn_wait'):
        turn_finish(1)
        turn_finish(0)
    with scope('end_turn'):
        def end_unpack(pair):
            block = jnp.transpose((turned(0, pair) - delta * turned(1, pair)) * inv)
            for i, p in enumerate((2 * pair, jnp.minimum(2 * pair + 1, phys - 1))):
                out_ref[p] = block[i * rows:(i + 1) * rows, :]
        repeat(0, pairs, end_unpack)


def solution(mesh):
    grid = fine_mesh(mesh)
    num_z = grid.shape['z']

    def local_run(psi_blk, left_blk, right_blk, mpo_pair):
        full_rows, n_s, n_u, local_cols = psi_blk.shape
        phys = n_s * n_u
        rows = full_rows // RING
        cols = local_cols * RING
        bonds_l, bonds_r = left_blk.shape[1], right_blk.shape[1]
        full_a, full_b = left_blk.shape[2], right_blk.shape[2]
        psi = psi_blk.transpose(1, 2, 3, 0).reshape(phys, local_cols, full_rows)
        left = left_blk.transpose(1, 0, 2)
        right = right_blk.transpose(1, 0, 2).reshape(bonds_r, RING, CORES, 8, full_b)
        mpo = mpo_pair.transpose(0, 2, 3, 4, 5, 1).reshape(bonds_l * phys, phys * bonds_r)
        eye = np.eye(8, dtype=np.float32)
        one = np.ones((1, 8), np.float32)
        order_out = np.arange(phys * bonds_r).reshape(phys, bonds_r).T.ravel()
        order_in = np.arange(bonds_l * phys).reshape(bonds_l, phys).T.ravel()
        spread_out = np.kron(np.eye(order_out.size, dtype=np.float32)[order_out], one.T)
        spread_in = np.kron(np.eye(order_in.size, dtype=np.float32)[:, order_in], one)
        same = np.tile(eye, (1, phys * bonds_l))
        red = num_z + RING * RING * CORES
        pairs = (phys + 1) // 2
        f32 = jnp.float32
        out, scal = pl.pallas_call(
            functools.partial(lanczos_kernel, float(psi_blk.size * grid.size), num_z),
            out_shape=(
                jax.ShapeDtypeStruct((phys, local_cols, full_rows), f32),
                jax.ShapeDtypeStruct((2, LANCZOS_STEPS + 1) + TILE, f32),
            ),
            in_specs=[
                pl.BlockSpec(memory_space=pltpu.VMEM),
                pl.BlockSpec(memory_space=pl.ANY),
                pl.BlockSpec(memory_space=pl.ANY),
            ] + [pl.BlockSpec(memory_space=pltpu.VMEM)] * 4,
            out_specs=(pl.BlockSpec(memory_space=pltpu.VMEM), pl.BlockSpec(memory_space=pltpu.VMEM)),
            scratch_shapes=[
                pltpu.VMEM((CORES, len(HELD), phys, rows // TREES, cols), f32),
                pltpu.VMEM((bonds_r, BLOCKS, CORES, 8, full_b), f32),
                pltpu.VMEM((bonds_l, rows, full_a), f32),
                pltpu.VMEM((2, rows, full_a), f32),
                pltpu.VMEM((bonds_l, rows, full_a), f32),
                pltpu.VMEM((bonds_r * phys * 8, phys * bonds_l * 8), f32),
                pltpu.VMEM((phys, bonds_l, rows // 8, 8, cols), f32),
                pltpu.VMEM((phys, rows // 8, 8, bonds_r * cols), f32),
                pltpu.VMEM((PARTS, num_z, STREAMS, phys, 8, cols), f32),
                pltpu.VMEM((PARTS, num_z - 1, STREAMS, phys, 8, cols), f32),
                pltpu.VMEM((2, phys, rows, cols), f32),
                pltpu.VMEM((2, phys, rows, cols), f32),
                pltpu.VMEM((2, RING, pairs, rows, LANES), f32),
                pltpu.VMEM((2, RING, pairs, rows, LANES), f32),
                pltpu.VMEM((2, 2) + TILE, f32),
                pltpu.VMEM((2, red) + TILE, f32),
                pltpu.VMEM(TILE, f32),
                pltpu.SemaphoreType.DMA((len(HELD),)),
                pltpu.SemaphoreType.DMA((len(HELD),)),
                pltpu.SemaphoreType.DMA((BLOCKS,)),
                pltpu.SemaphoreType.DMA((BLOCKS,)),
                pltpu.SemaphoreType.DMA((PARTS, num_z - 1, STREAMS)),
                pltpu.SemaphoreType.DMA((PARTS, num_z - 1, STREAMS)),
                pltpu.SemaphoreType.DMA((2, red)),
                pltpu.SemaphoreType.DMA((2, red)),
                pltpu.SemaphoreType.DMA((2, RING)),
                pltpu.SemaphoreType.DMA((2, RING)),
                pltpu.SemaphoreType.DMA((15, ENV_PIECES)),
                pltpu.SemaphoreType.DMA((15, ENV_PIECES)),
                pltpu.SemaphoreType.DMA((2,)),
                pltpu.SemaphoreType.REGULAR,
                pltpu.SemaphoreType.REGULAR,
            ],
            compiler_params=pltpu.CompilerParams(
                collective_id=0, has_side_effects=True, vmem_limit_bytes=67043328),
        )(psi, left, right, mpo, spread_out, spread_in, same)
        result = out.reshape(n_s, n_u, local_cols, full_rows).transpose(3, 0, 1, 2)
        return scal[0, 1:, 0, 0], scal[1, 1:, 0, 0], result

    return jax.shard_map(
        local_run, mesh=grid,
        in_specs=(P(('x', 'k'), None, None, ('z', 'y')), P(('x', 'k'), None, None), P(('z', 'y'), None, None), P()),
        out_specs=(P(), P(), P(('x', 'k'), None, None, ('z', 'y'))), check_vma=False)
```

```python
import functools
import itertools

import jax
import jax.numpy as jnp
import numpy as np
from jax import lax
from jax.experimental import pallas as pl
from jax.experimental.pallas import tpu as pltpu
from jax.sharding import Mesh, PartitionSpec as P

LANCZOS_STEPS = 4
FULL_PREC = lax.Precision.HIGHEST
MESH_IDS = pl.DeviceIdType.MESH
scope = jax.named_scope
SUB = 8
LANES = 128
TILE = (SUB, LANES)
RING = 4
CORES = 2
PARTS = 4
STREAMS = 2
TREES = 4
BLOCKS = RING * RING
ALL_LINKS = [('x', 1), ('y', 1), ('x', -1), ('y', -1)]


def fine_mesh(mesh):
    shape = (mesh.shape['col'] // RING, RING, mesh.shape['row'] // CORES, CORES)
    return Mesh(mesh.devices.reshape(shape), ('z', 'y', 'x', 'k'))


def near(d):
    return min(d, RING - d)


def make_tree(turn):
    prefer = ALL_LINKS[turn:] + ALL_LINKS[:turn]
    load = dict.fromkeys(prefer, 0)
    tree = {}
    for offset in sorted(itertools.product(range(RING), repeat=2), key=lambda o: near(o[0]) + near(o[1])):
        options = [
            (axis, sign) for axis, d in zip('xy', offset) for sign in (-1, 1)
            if d and (-sign * d) % RING == near(d)]
        if options:
            tree[offset] = min(options, key=lambda link: (load[link], prefer.index(link)))
            load[tree[offset]] += 1
    return tree


def source_of(message):
    part, dx, dy = message
    axis, sign = LINKS[message]
    return (part, (dx + sign) % RING, dy) if axis == 'x' else (part, dx, (dy + sign) % RING)


LINKS = {(part, *offset): link for part in range(TREES) for offset, link in make_tree(part % len(ALL_LINKS)).items()}
SENDS = {}
for sent in LINKS:
    SENDS.setdefault(source_of(sent), []).append(sent)


def gather_order(release):
    free = dict.fromkeys(ALL_LINKS, 0.0)
    arrival = {}
    order = []

    def issue(now, message):
        order.append(message)
        for sent in SENDS.get(message, ()):
            link = LINKS[sent]
            free[link] = max(free[link], now) + 1.0
            arrival[sent] = free[link] + 0.6

    todo = [(now, (part, 0, 0)) for part, now in enumerate(release)]
    while len(order) < TREES * BLOCKS:
        left = [(now, message) for message, now in arrival.items() if message not in order]
        if todo and (not left or min(left)[0] > todo[0][0]):
            issue(*todo.pop(0))
        else:
            issue(*min(left))
    return order


def counts(*texts):
    return [int(c, 36) for text in texts for c in text]


RELEASE = [0, 2.9, 4.5, 8.0]
PAIR_ORDER = counts('0101220013132323')
LAGS = (counts('11011'), counts('35040'), counts('39276'), counts('17387'))
FINISH = [9, 17, 23, 24]
HOOKS = (7, 15, 30)
DURING_ONE = counts('500020104111105222303030100', '301300')
DURING_RING = counts('0000000000000400')
DURING_TAIL = counts('000102004010301')
EARLY = sum(DURING_RING) + sum(DURING_TAIL)
ENV_STEPS = (counts('g515i4mp'), counts('sa2btbvw'), counts('wh8kwrww'), counts('wkbnwtxw'), counts('xontywyx'))
ENV_PIECES = len(ENV_STEPS[0])
ENV_LEAD = 2
CHUNK_STEPS = (0, 9, 18, 27, 30)
SPAN = 4
HELD = gather_order(RELEASE)
INDEX = {message: i for i, message in enumerate(HELD)}
MESSAGES = [message for message in HELD if message in LINKS]
GROUP = TREES
WIDE = len(HELD) // 4
CHUNKS = [(c * WIDE, WIDE) for c in range(3)] + [(3 * WIDE + c * WIDE // 2, WIDE // 2) for c in range(2)]


def dot(lhs, rhs):
    return jnp.dot(lhs, rhs, precision=FULL_PREC, preferred_element_type=jnp.float32)


def lanczos_kernel(
        num_elems, num_z, psi_ref, left_ref, right_ref, mpo_ref, spread_out_ref, spread_in_ref, same_ref, out_ref, scal_ref,
        gath, right_full, left_own, left_turn, left_perm, w_mat, acc, mid, terms, ring, h_buf, v_buf, pack_out, pack_in,
        red_held, red_slots, alpha_sum,
        ag_send, ag_recv, sib_send, sib_recv, rs_send, rs_recv, red_send, red_recv, turn_send, turn_recv,
        env_send, env_recv, load_sem, ag_credit, rs_credit):
    phys, rows, cols = h_buf.shape[1:]
    bonds = right_full.shape[0]
    bonds_l = left_own.shape[0]
    piece = rows // TREES
    slab = rows // PARTS
    octs = rows // 8
    pairs = pack_in.shape[2]
    last_step = LANCZOS_STEPS - 1
    z, y, x, k = (lax.axis_index(name) for name in ('z', 'y', 'x', 'k'))
    other = 1 - k

    x_at, y_at = ([lax.rem(pos + d, RING) for d in range(RING)] for pos in (x, y))
    k_at = (k, other)

    def step_to(axis, sign):
        return {axis: {'x': x_at, 'y': y_at}[axis][sign % RING]}

    phases = (
        (num_z, z, lambda i: {'z': i}),
        (RING * RING * CORES, (x * CORES + k) * RING + y,
         lambda i: {'x': lax.div(i, CORES * RING), 'k': lax.rem(lax.div(i, RING), CORES), 'y': lax.rem(i, RING)}),
    )
    bases = (0, num_z)
    barrier = pltpu.get_barrier_semaphore()
    def repeat(lo, hi, fn):
        def body(i, c):
            fn(i)
            return c
        lax.fori_loop(lo, hi, body, 0)

    for count, me, device in phases:
        def enter(d, count=count, me=me, device=device):
            pl.semaphore_signal(barrier, inc=1, device_id=device(lax.rem(me + d, count)), device_id_type=MESH_IDS)
        repeat(1, count, enter)

    own_rows = pl.multiple_of(y * rows, rows)
    load_left = pltpu.make_async_copy(left_ref.at[:, pl.ds(own_rows, rows), :], left_own, load_sem.at[0])
    load_left.start()
    load_right = pltpu.make_async_copy(right_ref, right_full.at[:, pl.ds(y * RING, RING)], load_sem.at[1])
    load_right.start()

    lane = lax.broadcasted_iota(jnp.int32, (rows, LANES), 1)

    def pack(which, value):
        def body(pair):
            halves = [value(2 * pair), value(jnp.minimum(2 * pair + 1, phys - 1))]
            for target in range(RING):
                tile, half = divmod(target * rows, LANES)
                first, second = (v[:, tile * LANES:(tile + 1) * LANES] for v in halves)
                if half == 0:
                    second = pltpu.roll(second, rows, 1)
                else:
                    first = pltpu.roll(first, rows, 1)
                pack_out[which, target, pair] = jnp.where(lane < rows, first, second)
        repeat(0, pairs, body)

    def turn_copy(which, src, dst, d, device):
        return pltpu.make_async_remote_copy(
            src_ref=pack_out.at[which, src], dst_ref=pack_in.at[which, dst],
            send_sem=turn_send.at[which, d], recv_sem=turn_recv.at[which, dst],
            device_id=device, device_id_type=MESH_IDS)

    def turn_start(which):
        for d in range(1, RING):
            peer = y_at[d]
            turn_copy(which, peer, y, d, {'y': peer}).start()
        pack_in[which, y] = pack_out[which, y]

    def turn_finish(which):
        for d in range(1, RING):
            peer = y_at[d]
            copy = turn_copy(which, peer, peer, d, {'y': peer})
            copy.wait_send()
            copy.wait_recv()

    def turned(which, pair):
        return jnp.concatenate([pack_in[which, i, pair] for i in range(RING)], axis=0)

    with scope('pack'):
        pack(0, lambda p: psi_ref[p])
    with scope('entry_barrier'):
        pl.semaphore_wait(barrier, sum(count - 1 for count, _, _ in phases))
    turn_start(0)

    up, down, far = y_at[1], y_at[3], y_at[2]
    strip = right_full.shape[-1] // ENV_PIECES

    def env_copy(kind, c, block, device, count=1, core=None):
        span = pl.ds(c * strip, strip)
        row = k if core is None else core
        view = right_full.at[:, pl.ds(block, count), pl.ds(row, 1), :, span]
        return pltpu.make_async_remote_copy(
            src_ref=view, dst_ref=view, send_sem=env_send.at[kind, c], recv_sem=env_recv.at[kind, c],
            device_id=device, device_id_type=MESH_IDS)

    def block_of(owner, d):
        return owner * RING + x_at[d]

    TAKEN = (0, 1)

    def env_start(c):
        for d in TAKEN:
            env_copy(d, c, block_of(y, d), {'y': up}).start()
            env_copy(2 + d, c, block_of(y, d), {'y': down}).start()

    def env_pass_x(c, i, owner):
        env_copy(6 + i, c, block_of(owner, 0), {'x': x_at[1]}).start()
        env_copy(9 + i, c, block_of(owner, 1), {'x': x_at[3]}).start()

    def env_pass(c):
        for d in TAKEN:
            env_copy(d, c, block_of(down, d), {'y': up}).wait_recv()
            env_copy(2 + d, c, block_of(up, d), {'y': down}).wait_recv()
        env_copy(4, c, block_of(down, 0), {'y': up}).start()
        env_copy(5, c, block_of(up, 1), {'y': down}).start()
        env_pass_x(c, 0, down)
        env_pass_x(c, 1, up)

    def env_far(c):
        env_copy(4, c, block_of(far, 0), {'y': up}).wait_recv()
        env_copy(5, c, block_of(far, 1), {'y': down}).wait_recv()
        env_pass_x(c, 2, far)

    def env_share(c):
        for i, owner in enumerate((down, up, far)):
            env_copy(6 + i, c, block_of(owner, 3), {'x': x_at[1]}).wait_recv()
            env_copy(9 + i, c, block_of(owner, 2), {'x': x_at[3]}).wait_recv()
            env_copy(12 + i, c, owner * RING, {'k': other}, RING).start()

    def env_done(c):
        for i, owner in enumerate((down, up, far)):
            env_copy(12 + i, c, owner * RING, {'k': other}, RING, other).wait_recv()

    env_events = (env_start, env_pass, env_far, env_share, env_done)

    def env_before(step):
        for c in range(ENV_PIECES):
            if ENV_STEPS[0][c] == step:
                env_start(c)

    def env_sent(c):
        for kind in range(12):
            env_copy(kind, c, 0, {'k': other}).wait_send()
        for i in range(3):
            env_copy(12 + i, c, 0, {'k': other}, RING).wait_send()

    load_right.wait()
    env_before(0)
    h_buf[1] = jnp.zeros(h_buf.shape[1:], jnp.float32)
    v_buf[...] = jnp.zeros(v_buf.shape, jnp.float32)

    def sum_start(which, phase, value):
        count, me, device = phases[phase]
        red_held[which, phase] = value

        def send(d):
            pltpu.make_async_remote_copy(
                src_ref=red_held.at[which, phase], dst_ref=red_slots.at[which, bases[phase] + me],
                send_sem=red_send.at[which, bases[phase] + d], recv_sem=red_recv.at[which, bases[phase] + me],
                device_id=device(lax.rem(me + d, count)), device_id_type=MESH_IDS).start()
        repeat(1, count, send)
        red_slots[which, bases[phase] + me] = value

    def sum_finish(which, phase):
        count, me, device = phases[phase]

        def wait(d):
            peer = lax.rem(me + d, count)
            copy = pltpu.make_async_remote_copy(
                src_ref=red_held.at[which, phase], dst_ref=red_slots.at[which, bases[phase] + peer],
                send_sem=red_send.at[which, bases[phase] + d], recv_sem=red_recv.at[which, bases[phase] + peer],
                device_id=device(peer), device_id_type=MESH_IDS)
            copy.wait_send()
            copy.wait_recv()
        repeat(1, count, wait)
        return red_slots[which, bases[phase]:bases[phase] + count].sum(0)

    def mean_of(value):
        return jnp.broadcast_to(jnp.sum(value, axis=(0, 1), keepdims=True) * (1.0 / num_elems), TILE)

    def only(tile):
        return tile[:1, :1]

    def fold(values):
        lanes = values.reshape(-1, 8, cols).sum(0)
        tile = lanes[:, :LANES]
        for c in range(LANES, cols, LANES):
            tile = tile + lanes[:, c:c + LANES]
        return tile

    def gather_copy(message):
        index = INDEX[message]
        return pltpu.make_async_remote_copy(
            src_ref=gath.at[0, INDEX[source_of(message)]], dst_ref=gath.at[0, index],
            send_sem=ag_send.at[index], recv_sem=ag_recv.at[index],
            device_id=step_to(*LINKS[message]), device_id_type=MESH_IDS)

    def sibling_copy(index):
        span = pl.ds(index * GROUP, GROUP)
        return pltpu.make_async_remote_copy(
            src_ref=gath.at[0, span], dst_ref=gath.at[1, span],
            send_sem=sib_send.at[index], recv_sem=sib_recv.at[index],
            device_id={'k': other}, device_id_type=MESH_IDS)

    def groups_after(held, sequence):
        done = {}
        held = set(held)
        for message in sequence:
            held.add(message)
            for i in range(BLOCKS):
                group = HELD[i * GROUP:(i + 1) * GROUP]
                if message in group and held.issuperset(group):
                    done.setdefault(message, []).append(i)
        return done

    def take(message, groups):
        if message in LINKS:
            gather_copy(message).wait_recv()
        for sent in SENDS.get(message, ()):
            gather_copy(sent).start()
        for i in groups.get(message, ()):
            sibling_copy(i).start()

    def own_parts(s):
        each = TREES // PARTS
        return [(s * each + i, 0, 0) for i in range(each)]

    with scope('turn_wait'):
        turn_finish(0)
    with scope('turn'):
        def unpack(pair):
            block = jnp.transpose(turned(0, pair))
            for i, p in enumerate((2 * pair, jnp.minimum(2 * pair + 1, phys - 1))):
                h_buf[0, p] = block[i * rows:(i + 1) * rows, :]
                for part in range(TREES):
                    span = slice(i * rows + part * piece, i * rows + (part + 1) * piece)
                    gath[0, INDEX[part, 0, 0], p] = block[span, :]
        repeat(0, pairs, unpack)
    own = [message for message in HELD if message not in LINKS]
    groups = groups_after((), own + MESSAGES[:EARLY])
    for message in own:
        take(message, groups)

    with scope('left'):
        load_left.wait()
    order = []
    for first, count in CHUNKS:
        order += [(dk, message) for dk in range(CORES) for message in HELD[first:first + count]]
    per_tile = LANES // piece
    lanes = lax.broadcasted_iota(jnp.int32, (rows, LANES), 1)

    left_tiles = {
        (dx, dk, dy): pl.multiple_of(lax.div((x_at[dx] * CORES + k_at[dk]) * RING + y_at[dy], 2) * LANES, LANES)
        for dx in range(RING) for dk in range(CORES) for dy in range(RING)}

    def left_rows(l, c):
        for tile in range(left_own.shape[2] // LANES):
            at = slice(tile * LANES, (tile + 1) * LANES)
            plain = left_own[l, :, at]
            rolled = pltpu.roll(plain, rows, 1)
            left_turn[0, :, at] = jnp.where(lax.rem(y, 2) == 0, plain, rolled)
            left_turn[1, :, at] = jnp.where(lax.rem(y, 2) == 0, rolled, plain)
        for tile in range(left_perm.shape[2] // LANES):
            result = None
            for i in range(per_tile):
                dk, message = order[tile * per_tile + i]
                _, dx, dy = message
                values = left_turn[dy % 2, :, pl.ds(left_tiles[dx, dk, dy], LANES)]
                if i != message[0]:
                    values = pltpu.roll(values, (i - message[0]) * piece % LANES, 1)
                result = values if i == 0 else jnp.where(lanes >= i * piece, values, result)
            left_perm[l, :, tile * LANES:(tile + 1) * LANES] = result
        return c

    with scope('left_order'):
        lax.fori_loop(0, bonds_l, left_rows, 0)

    with scope('mpo'):
        rows_out = lax.dot_general(
            spread_out_ref[...], mpo_ref[...], (((1,), (1,)), ((), ())), precision=FULL_PREC,
            preferred_element_type=jnp.float32)
        wide = dot(rows_out, spread_in_ref[...])
        n_out, n_in = w_mat.shape
        same = jnp.broadcast_to(same_ref[...][None], (n_out // 8, 8, n_in)).reshape(n_out, n_in)
        w_mat[...] = wide * same

    env_before(1)
    with scope('gather_early'):
        for message in MESSAGES[:EARLY]:
            take(message, groups)

    def stage_one(first, count, p, fresh):
        depth = count * piece
        rhs = jnp.concatenate(
            [gath[dk, pl.ds(first, count), p].reshape(depth, cols) for dk in range(CORES)], axis=0)
        column = pl.multiple_of(first * CORES * piece, LANES)
        lhs = left_perm[:, :, pl.ds(column, CORES * depth)].reshape(bonds_l * rows, CORES * depth)
        res = dot(lhs, rhs).reshape(bonds_l, octs, 8, cols)
        acc[p] = jnp.where(fresh, 0.0, acc[p]) + res

    def at_steps(i, events):
        steps = sorted(events)

        def run(steps):
            if len(steps) > 1:
                middle = len(steps) // 2
                lax.cond(i < steps[middle], lambda: run(steps[:middle]), lambda: run(steps[middle:]))
            else:
                for step in steps:
                    @pl.when(i == step)
                    def _():
                        for event in events[step]:
                            event()

        run(steps)

    def way(s):
        return 1 - 2 * lax.rem(s, 2)

    def ring_side(s, n):
        return way(s) * (1 - 2 * lax.rem(n, 2))

    def ring_block(s, n):
        return lax.rem(z + num_z + ring_side(s, n) * (num_z // 2 - lax.div(n + 1, 2)), num_z)

    def ring_copy(src, s, n, h):
        return pltpu.make_async_remote_copy(
            src_ref=src, dst_ref=ring.at[s, n, h], send_sem=rs_send.at[s, n, h], recv_sem=rs_recv.at[s, n, h],
            device_id={'z': lax.rem(z + num_z + ring_side(s, n), num_z)}, device_id_type=MESH_IDS)

    def ring_wait(s, n, h):
        ring_copy(terms.at[s, n, h], s, n, h).wait_recv()

    def ring_pass(s, n, h):
        with scope('ring_pass'):
            ring_wait(s, n - 2, h)
            ring[s, n - 2, h] = ring[s, n - 2, h] + terms[s, n, h]
            ring_copy(ring.at[s, n - 2, h], s, n, h).start()

    def middle(o):
        res = dot(w_mat[...], acc[:, :, o].reshape(phys * bonds_l * 8, cols)).reshape(bonds, phys, 8, cols)
        for r in range(bonds):
            mid[:, o, :, r * cols:(r + 1) * cols] = res[r]

    def last_stage(s, which):
        lhs = mid[:, pl.ds(s * STREAMS, STREAMS)].reshape(phys * slab, bonds * cols)
        for n in which:
            first = pl.multiple_of(ring_block(s, n) * cols, cols)
            rhs = right_full[:, :, :, :, pl.ds(first, cols)].reshape(bonds * cols, cols)
            res = dot(lhs, rhs).reshape(phys, STREAMS, 8, cols)
            for h in range(STREAMS):
                terms[s, n, h] = res[:, h]

    def new_direction(cur, alpha, beta_prev):
        nxt = 1 - cur
        a, b = only(alpha), only(beta_prev)
        def body(p, total):
            w = h_buf[cur, p] - a * v_buf[cur, p] - b * v_buf[nxt, p]
            v_buf[nxt, p] = w
            return total + fold(w * w)

        return lax.fori_loop(0, phys, body, jnp.zeros(TILE, jnp.float32))

    def step(j, carry):
        alpha_part, beta_prev = carry
        cur = lax.rem(j, 2)
        nxt = 1 - cur
        more = j < last_step

        def alpha_z():
            sum_start(0, 1, sum_finish(0, 0))

        def alpha_plane():
            alpha = mean_of(sum_finish(0, 1))
            scal_ref[0, j] = alpha
            sum_start(1, 0, new_direction(cur, alpha, beta_prev))

        def beta_z():
            sum_start(1, 1, sum_finish(1, 0))

        def in_first(event, *what):
            @pl.when(j == 0)
            def _():
                event(*what)

        sum_start(0, 0, alpha_part)
        queue = MESSAGES[EARLY:]
        groups = groups_after(own + MESSAGES[:EARLY], queue)
        wide_steps = 3 * phys
        each = 3 if phys % 3 == 0 else 1
        half_steps = 2 * phys // each
        events = {}
        hooks = dict(zip(HOOKS, (alpha_z, alpha_plane, beta_z)))
        for n, count in enumerate(DURING_ONE):
            at = n * phys // 9 if n < 27 else wide_steps + (n - 27) * half_steps // 6
            at = events.setdefault(at, [])
            at += [functools.partial(take, message, groups) for message in queue[:count]]
            queue = queue[count:]
            for event, steps in zip(env_events, ENV_STEPS):
                at += [functools.partial(in_first, event, c) for c in range(ENV_PIECES) if steps[c] == n + ENV_LEAD]
            if n in CHUNK_STEPS:
                first, count = CHUNKS[CHUNK_STEPS.index(n)]
                at += [sibling_copy(i).wait_recv for i in range(first // GROUP, (first + count) // GROUP)]
            if n in hooks:
                at.append(hooks[n])

        def wide_step(i):
            with scope('events_wide'):
                at_steps(i, {n: e for n, e in events.items() if n < wide_steps})
            with scope('one_wide'):
                stage_one(lax.div(i, phys) * WIDE, WIDE, lax.rem(i, phys), i < phys)

        def half_step(i):
            with scope('events_half'):
                at_steps(i, {n - wide_steps: e for n, e in events.items() if n >= wide_steps})

            with scope('one_half'):
                chunk, p = lax.div(i * each, phys), lax.rem(i * each, phys)
                for q in range(each):
                    stage_one(3 * WIDE + chunk * (WIDE // 2), WIDE // 2, p + q, i < 0)

        repeat(0, wide_steps, wide_step)
        repeat(0, half_steps, half_step)
        with scope('gather_sent'):
            for message in MESSAGES:
                gather_copy(message).wait_send()
            repeat(0, BLOCKS, lambda i: sibling_copy(i).wait_send())

        @pl.when(more)
        def _():
            for link in ALL_LINKS:
                pl.semaphore_signal(ag_credit, inc=1, device_id=step_to(*link), device_id_type=MESH_IDS)
            pl.semaphore_signal(ag_credit, inc=1, device_id={'k': other}, device_id_type=MESH_IDS)

        @pl.when(j > 0)
        def _():
            pl.semaphore_wait(rs_credit, 2)

        def scale():
            beta = jnp.sqrt(mean_of(sum_finish(1, 1)))
            scal_ref[1, j] = beta
            inv = only(1.0 / beta)

            def normalize(p):
                v_buf[nxt, p] = v_buf[nxt, p] * inv
            repeat(0, phys, normalize)

            @pl.when(more)
            def _():
                pl.semaphore_wait(ag_credit, len(ALL_LINKS) + 1)

            @pl.when(j == last_step)
            def _():
                pack(1, lambda p: v_buf[nxt, p])
                turn_start(1)

        def finish(s):
            if s == 0:
                scale()
            with scope('ring_end'):
                for h in range(STREAMS):
                    for n in range(max(num_z - 3, 0), num_z - 1):
                        ring_wait(s, n, h)
            alpha, beta = scal_ref[0, j], scal_ref[1, j]
            a, b, inv = only(alpha), only(beta_prev), only(1.0 / beta)
            span = slice(s * slab, (s + 1) * slab)

            def body(p, total):
                new = []
                for h in range(STREAMS):
                    at = slice(s * slab + 8 * h, s * slab + 8 * h + 8)
                    g_new = terms[s, num_z - 1, h, p]
                    for n in range(max(num_z - 3, 0), num_z - 1):
                        g_new = g_new + ring[s, n, h, p]
                    new.append((g_new - a * h_buf[cur, p, at, :] - b * h_buf[nxt, p, at, :]) * inv)
                h_new = jnp.concatenate(new, axis=0)
                h_buf[nxt, p, span, :] = h_new
                for i, message in enumerate(own_parts(s)):
                    gath[0, INDEX[message], p] = h_new[i * piece:(i + 1) * piece]
                return total + fold(v_buf[nxt, p, span, :] * h_new)

            total = lax.fori_loop(0, phys, body, jnp.zeros(TILE, jnp.float32))
            alpha_sum[...] = total if s == 0 else alpha_sum[...] + total

            @pl.when(more)
            def _():
                for message in own_parts(s):
                    take(message, next_groups)

        def early(message):
            @pl.when(more)
            def _():
                take(message, next_groups)

        def happen(event):
            {'pass': ring_pass, 'finish': finish, 'early': early}[event[0]](*event[1:])

        pairs_z = num_z // 2
        ring_steps = PARTS * pairs_z
        pairs_at = []
        for s in PAIR_ORDER:
            if sum(s == other_s for other_s, _ in pairs_at) < pairs_z:
                pairs_at.append((s, sum(s == other_s for other_s, _ in pairs_at)))
        slots = {pair: i for i, pair in enumerate(pairs_at)}
        events = {}
        for s in range(PARTS):
            for n in range(2, num_z - 1):
                at = slots[s, n // 2] + LAGS[s][n - 2]
                events.setdefault(at, []).extend(('pass', s, n, h) for h in range(STREAMS))
            events.setdefault(FINISH[s] * pairs_z // SPAN, []).append(('finish', s))
        tail = [event for at in sorted(events) if at >= ring_steps for event in events.pop(at)]
        queue = MESSAGES[:EARLY]
        for at, count in enumerate(DURING_RING):
            events.setdefault(at * pairs_z // SPAN, []).extend(('early', message) for message in queue[:count])
            queue = queue[count:]
        mixed = []
        spare = list(DURING_TAIL)
        for i, event in enumerate(tail):
            mixed.append(event)
            count = len(queue) if i == len(tail) - 1 else spare.pop(0) if spare else 0
            mixed += [('early', message) for message in queue[:count]]
            queue = queue[count:]
        tail = mixed
        sequence = [event for at in sorted(events) for event in events[at]] + tail
        sequence = [
            message for kind, *what in sequence if kind != 'pass'
            for message in (own_parts(*what) if kind == 'finish' else what)]
        next_groups = groups_after((), sequence)

        def ring_step(i):
            s, t = pairs_at[0]
            for n, pair in enumerate(pairs_at):
                s, t = jnp.where(i == n, pair[0], s), jnp.where(i == n, pair[1], t)

            @pl.when(t == 0)
            def _():
                with scope('middle'):
                    for o in range(STREAMS):
                        middle(s * STREAMS + o)

            with scope('last_stage'):
                last_stage(s, (2 * t, 2 * t + 1))

            @pl.when(t == 0)
            def _():
                for n in range(min(2, num_z - 1)):
                    for h in range(STREAMS):
                        ring_copy(terms.at[s, n, h], s, n, h).start()

            with scope('events_ring'):
                at_steps(i, {at: [functools.partial(happen, event) for event in events[at]] for at in events})

        repeat(0, ring_steps, ring_step)
        with scope('tail'):
            for event in tail:
                happen(event)

        def ring_sent(i):
            s, n = lax.div(i, num_z - 1), lax.rem(i, num_z - 1)
            for h in range(STREAMS):
                ring_copy(terms.at[s, n, h], s, n, h).wait_send()
        repeat(0, PARTS * (num_z - 1), ring_sent)

        @pl.when(more)
        def _():
            for sign in (1, num_z - 1):
                pl.semaphore_signal(
                    rs_credit, inc=1, device_id={'z': lax.rem(z + sign, num_z)}, device_id_type=MESH_IDS)

        return alpha_sum[...], jnp.where(j > 0, scal_ref[1, j], 0.0)

    zero = jnp.zeros(TILE, jnp.float32)
    _, beta_prev = lax.fori_loop(0, LANCZOS_STEPS, step, (zero, zero))
    repeat(0, ENV_PIECES, env_sent)

    cur = LANCZOS_STEPS % 2
    shift = only(scal_ref[0, last_step])
    b = only(beta_prev)

    def end_body(p, sums):
        h, v = h_buf[cur, p], v_buf[cur, p]
        d = h - shift * v - b * v_buf[1 - cur, p]
        h_buf[1 - cur, p] = d
        return tuple(total + fold(term) for total, term in zip(sums, (v * h, d * d, d * v, v * v)))

    sums = lax.fori_loop(0, phys, end_body, (zero,) * 4)
    row = lax.broadcasted_iota(jnp.int32, TILE, 0)

    def squeeze(tile):
        tile = tile + pltpu.roll(tile, 4, 0)
        return tile + pltpu.roll(tile, 2, 0)

    packed = squeeze(sums[0])
    for i in range(1, 4):
        packed = jnp.where(row >= 2 * i, squeeze(sums[i]), packed)
    with scope('end_sum'):
        sum_start(0, 0, packed)
        pack(0, lambda p: h_buf[1 - cur, p])
        turn_start(0)
        sum_start(0, 1, sum_finish(0, 0))
        packed = sum_finish(0, 1)
    v_h, d_d, d_v, v_v = (mean_of(jnp.where((row >= 2 * i) & (row < 2 * i + 2), packed, 0.0)) for i in range(4))
    delta = v_h - shift
    beta = jnp.sqrt(d_d - 2.0 * delta * d_v + delta * delta * v_v)
    scal_ref[0, LANCZOS_STEPS] = v_h
    scal_ref[1, LANCZOS_STEPS] = beta
    inv = only(1.0 / beta)
    delta = only(delta)
    with scope('end_turn_wait'):
        turn_finish(1)
        turn_finish(0)
    with scope('end_turn'):
        def end_unpack(pair):
            block = jnp.transpose((turned(0, pair) - delta * turned(1, pair)) * inv)
            for i, p in enumerate((2 * pair, jnp.minimum(2 * pair + 1, phys - 1))):
                out_ref[p] = block[i * rows:(i + 1) * rows, :]
        repeat(0, pairs, end_unpack)


def solution(mesh):
    grid = fine_mesh(mesh)
    num_z = grid.shape['z']

    def local_run(psi_blk, left_blk, right_blk, mpo_pair):
        full_rows, n_s, n_u, local_cols = psi_blk.shape
        phys = n_s * n_u
        rows = full_rows // RING
        cols = local_cols * RING
        bonds_l, bonds_r = left_blk.shape[1], right_blk.shape[1]
        full_a, full_b = left_blk.shape[2], right_blk.shape[2]
        psi = psi_blk.transpose(1, 2, 3, 0).reshape(phys, local_cols, full_rows)
        left = left_blk.transpose(1, 0, 2)
        right = right_blk.transpose(1, 0, 2).reshape(bonds_r, RING, CORES, 8, full_b)
        mpo = mpo_pair.transpose(0, 2, 3, 4, 5, 1).reshape(bonds_l * phys, phys * bonds_r)
        eye = np.eye(8, dtype=np.float32)
        one = np.ones((1, 8), np.float32)
        order_out = np.arange(phys * bonds_r).reshape(phys, bonds_r).T.ravel()
        order_in = np.arange(bonds_l * phys).reshape(bonds_l, phys).T.ravel()
        spread_out = np.kron(np.eye(order_out.size, dtype=np.float32)[order_out], one.T)
        spread_in = np.kron(np.eye(order_in.size, dtype=np.float32)[:, order_in], one)
        same = np.tile(eye, (1, phys * bonds_l))
        red = num_z + RING * RING * CORES
        pairs = (phys + 1) // 2
        f32 = jnp.float32
        out, scal = pl.pallas_call(
            functools.partial(lanczos_kernel, float(psi_blk.size * grid.size), num_z),
            out_shape=(
                jax.ShapeDtypeStruct((phys, local_cols, full_rows), f32),
                jax.ShapeDtypeStruct((2, LANCZOS_STEPS + 1) + TILE, f32),
            ),
            in_specs=[
                pl.BlockSpec(memory_space=pltpu.VMEM),
                pl.BlockSpec(memory_space=pl.ANY),
                pl.BlockSpec(memory_space=pl.ANY),
            ] + [pl.BlockSpec(memory_space=pltpu.VMEM)] * 4,
            out_specs=(pl.BlockSpec(memory_space=pltpu.VMEM), pl.BlockSpec(memory_space=pltpu.VMEM)),
            scratch_shapes=[
                pltpu.VMEM((CORES, len(HELD), phys, rows // TREES, cols), f32),
                pltpu.VMEM((bonds_r, BLOCKS, CORES, 8, full_b), f32),
                pltpu.VMEM((bonds_l, rows, full_a), f32),
                pltpu.VMEM((2, rows, full_a), f32),
                pltpu.VMEM((bonds_l, rows, full_a), f32),
                pltpu.VMEM((bonds_r * phys * 8, phys * bonds_l * 8), f32),
                pltpu.VMEM((phys, bonds_l, rows // 8, 8, cols), f32),
                pltpu.VMEM((phys, rows // 8, 8, bonds_r * cols), f32),
                pltpu.VMEM((PARTS, num_z, STREAMS, phys, 8, cols), f32),
                pltpu.VMEM((PARTS, num_z - 1, STREAMS, phys, 8, cols), f32),
                pltpu.VMEM((2, phys, rows, cols), f32),
                pltpu.VMEM((2, phys, rows, cols), f32),
                pltpu.VMEM((2, RING, pairs, rows, LANES), f32),
                pltpu.VMEM((2, RING, pairs, rows, LANES), f32),
                pltpu.VMEM((2, 2) + TILE, f32),
                pltpu.VMEM((2, red) + TILE, f32),
                pltpu.VMEM(TILE, f32),
                pltpu.SemaphoreType.DMA((len(HELD),)),
                pltpu.SemaphoreType.DMA((len(HELD),)),
                pltpu.SemaphoreType.DMA((BLOCKS,)),
                pltpu.SemaphoreType.DMA((BLOCKS,)),
                pltpu.SemaphoreType.DMA((PARTS, num_z - 1, STREAMS)),
                pltpu.SemaphoreType.DMA((PARTS, num_z - 1, STREAMS)),
                pltpu.SemaphoreType.DMA((2, red)),
                pltpu.SemaphoreType.DMA((2, red)),
                pltpu.SemaphoreType.DMA((2, RING)),
                pltpu.SemaphoreType.DMA((2, RING)),
                pltpu.SemaphoreType.DMA((15, ENV_PIECES)),
                pltpu.SemaphoreType.DMA((15, ENV_PIECES)),
                pltpu.SemaphoreType.DMA((2,)),
                pltpu.SemaphoreType.REGULAR,
                pltpu.SemaphoreType.REGULAR,
            ],
            compiler_params=pltpu.CompilerParams(
                collective_id=0, has_side_effects=True, vmem_limit_bytes=67043328),
        )(psi, left, right, mpo, spread_out, spread_in, same)
        result = out.reshape(n_s, n_u, local_cols, full_rows).transpose(3, 0, 1, 2)
        return scal[0, 1:, 0, 0], scal[1, 1:, 0, 0], result

    return jax.shard_map(
        local_run, mesh=grid,
        in_specs=(P(('x', 'k'), None, None, ('z', 'y')), P(('x', 'k'), None, None), P(('z', 'y'), None, None), P()),
        out_specs=(P(), P(), P(('x', 'k'), None, None, ('z', 'y'))), check_vma=False)
```

```python
import functools
import itertools

import jax
import jax.numpy as jnp
import numpy as np
from jax import lax
from jax.experimental import pallas as pl
from jax.experimental.pallas import tpu as pltpu
from jax.sharding import Mesh, PartitionSpec as P

LANCZOS_STEPS = 4
FULL_PREC = lax.Precision.HIGHEST
MESH_IDS = pl.DeviceIdType.MESH
scope = jax.named_scope
SUB = 8
LANES = 128
TILE = (SUB, LANES)
RING = 4
CORES = 2
PARTS = 4
STREAMS = 2
TREES = 8
BLOCKS = RING * RING
ALL_LINKS = [('x', 1), ('y', 1), ('x', -1), ('y', -1)]


def fine_mesh(mesh):
    shape = (mesh.shape['col'] // RING, RING, mesh.shape['row'] // CORES, CORES)
    return Mesh(mesh.devices.reshape(shape), ('z', 'y', 'x', 'k'))


def near(d):
    return min(d, RING - d)


def make_tree(turn):
    prefer = ALL_LINKS[turn:] + ALL_LINKS[:turn]
    load = dict.fromkeys(prefer, 0)
    tree = {}
    for offset in sorted(itertools.product(range(RING), repeat=2), key=lambda o: near(o[0]) + near(o[1])):
        options = [
            (axis, sign) for axis, d in zip('xy', offset) for sign in (-1, 1)
            if d and (-sign * d) % RING == near(d)]
        if options:
            tree[offset] = min(options, key=lambda link: (load[link], prefer.index(link)))
            load[tree[offset]] += 1
    return tree


def source_of(message):
    part, dx, dy = message
    axis, sign = LINKS[message]
    return (part, (dx + sign) % RING, dy) if axis == 'x' else (part, dx, (dy + sign) % RING)


LINKS = {(part, *offset): link for part in range(TREES) for offset, link in make_tree(part % len(ALL_LINKS)).items()}
SENDS = {}
for sent in LINKS:
    SENDS.setdefault(source_of(sent), []).append(sent)


def gather_order(release):
    free = dict.fromkeys(ALL_LINKS, 0.0)
    arrival = {}
    order = []

    def issue(now, message):
        order.append(message)
        for sent in SENDS.get(message, ()):
            link = LINKS[sent]
            free[link] = max(free[link], now) + 1.0
            arrival[sent] = free[link] + 0.6

    todo = [(now, (part, 0, 0)) for part, now in enumerate(release)]
    while len(order) < TREES * BLOCKS:
        left = [(now, message) for message, now in arrival.items() if message not in order]
        if todo and (not left or min(left)[0] > todo[0][0]):
            issue(*todo.pop(0))
        else:
            issue(*min(left))
    return order


def counts(*texts):
    return [int(c, 36) for text in texts for c in text]


RELEASE = [0, 0, 0, 0, 8.0, 8.0, 8.0, 8.0]
PAIR_ORDER = counts('0101200112332233')
LAGS = (counts('11023'), counts('14233'), counts('32455'), counts('22255'))
FINISH = [11, 14, 21, 22]
HOOKS = (6, 15, 30)
DURING_ONE = counts('311703122404652560300724111', '542200')
DURING_RING = counts('0000000000000400')
DURING_TAIL = counts('13500529211120')
EARLY = sum(DURING_RING) + sum(DURING_TAIL)
ENV_STEPS = (counts('7d2ji2op'), counts('hjarnatv'), counts('mpgtqhuw'), counts('nqkurlvw'), counts('qxqwwywy'))
ENV_PIECES = len(ENV_STEPS[0])
ENV_LEAD = 2
CHUNK_STEPS = (0, 9, 18, 27, 30)
SPAN = 4
HELD = gather_order(RELEASE)
INDEX = {message: i for i, message in enumerate(HELD)}
MESSAGES = [message for message in HELD if message in LINKS]
GROUP = TREES
WIDE = len(HELD) // 4
CHUNKS = [(c * WIDE, WIDE) for c in range(3)] + [(3 * WIDE + c * WIDE // 2, WIDE // 2) for c in range(2)]


def dot(lhs, rhs):
    return jnp.dot(lhs, rhs, precision=FULL_PREC, preferred_element_type=jnp.float32)


def lanczos_kernel(
        num_elems, num_z, psi_ref, left_ref, right_ref, mpo_ref, spread_out_ref, spread_in_ref, same_ref, out_ref, scal_ref,
        gath, right_full, left_own, left_turn, left_perm, w_mat, acc, mid, terms, ring, h_buf, v_buf, pack_out, pack_in,
        red_held, red_slots, alpha_sum,
        ag_send, ag_recv, sib_send, sib_recv, rs_send, rs_recv, red_send, red_recv, turn_send, turn_recv,
        env_send, env_recv, load_sem, ag_credit, rs_credit):
    phys, rows, cols = h_buf.shape[1:]
    bonds = right_full.shape[0]
    bonds_l = left_own.shape[0]
    piece = rows // TREES
    slab = rows // PARTS
    octs = rows // 8
    pairs = pack_in.shape[2]
    last_step = LANCZOS_STEPS - 1
    z, y, x, k = (lax.axis_index(name) for name in ('z', 'y', 'x', 'k'))
    other = 1 - k

    x_at, y_at = ([lax.rem(pos + d, RING) for d in range(RING)] for pos in (x, y))
    k_at = (k, other)

    def step_to(axis, sign):
        return {axis: {'x': x_at, 'y': y_at}[axis][sign % RING]}

    phases = (
        (num_z, z, lambda i: {'z': i}),
        (RING * RING * CORES, (x * CORES + k) * RING + y,
         lambda i: {'x': lax.div(i, CORES * RING), 'k': lax.rem(lax.div(i, RING), CORES), 'y': lax.rem(i, RING)}),
    )
    bases = (0, num_z)
    barrier = pltpu.get_barrier_semaphore()
    def repeat(lo, hi, fn):
        def body(i, c):
            fn(i)
            return c
        lax.fori_loop(lo, hi, body, 0)

    for count, me, device in phases:
        def enter(d, count=count, me=me, device=device):
            pl.semaphore_signal(barrier, inc=1, device_id=device(lax.rem(me + d, count)), device_id_type=MESH_IDS)
        repeat(1, count, enter)

    own_rows = pl.multiple_of(y * rows, rows)
    load_left = pltpu.make_async_copy(left_ref.at[:, pl.ds(own_rows, rows), :], left_own, load_sem.at[0])
    load_left.start()
    load_right = pltpu.make_async_copy(right_ref, right_full.at[:, pl.ds(y * RING, RING)], load_sem.at[1])
    load_right.start()

    lane = lax.broadcasted_iota(jnp.int32, (rows, LANES), 1)

    def pack(which, value):
        def body(pair):
            halves = [value(2 * pair), value(jnp.minimum(2 * pair + 1, phys - 1))]
            for target in range(RING):
                tile, half = divmod(target * rows, LANES)
                first, second = (v[:, tile * LANES:(tile + 1) * LANES] for v in halves)
                if half == 0:
                    second = pltpu.roll(second, rows, 1)
                else:
                    first = pltpu.roll(first, rows, 1)
                pack_out[which, target, pair] = jnp.where(lane < rows, first, second)
        repeat(0, pairs, body)

    def turn_copy(which, src, dst, d, device):
        return pltpu.make_async_remote_copy(
            src_ref=pack_out.at[which, src], dst_ref=pack_in.at[which, dst],
            send_sem=turn_send.at[which, d], recv_sem=turn_recv.at[which, dst],
            device_id=device, device_id_type=MESH_IDS)

    def turn_start(which):
        for d in range(1, RING):
            peer = y_at[d]
            turn_copy(which, peer, y, d, {'y': peer}).start()
        pack_in[which, y] = pack_out[which, y]

    def turn_finish(which):
        for d in range(1, RING):
            peer = y_at[d]
            copy = turn_copy(which, peer, peer, d, {'y': peer})
            copy.wait_send()
            copy.wait_recv()

    def turned(which, pair):
        return jnp.concatenate([pack_in[which, i, pair] for i in range(RING)], axis=0)

    with scope('pack'):
        pack(0, lambda p: psi_ref[p])
    with scope('entry_barrier'):
        pl.semaphore_wait(barrier, sum(count - 1 for count, _, _ in phases))
    turn_start(0)

    up, down, far = y_at[1], y_at[3], y_at[2]
    strip = right_full.shape[-1] // ENV_PIECES

    def env_copy(kind, c, block, device, count=1, core=None):
        span = pl.ds(c * strip, strip)
        row = k if core is None else core
        view = right_full.at[:, pl.ds(block, count), pl.ds(row, 1), :, span]
        return pltpu.make_async_remote_copy(
            src_ref=view, dst_ref=view, send_sem=env_send.at[kind, c], recv_sem=env_recv.at[kind, c],
            device_id=device, device_id_type=MESH_IDS)

    def block_of(owner, d):
        return owner * RING + x_at[d]

    TAKEN = (0, 1)

    def env_start(c):
        for d in TAKEN:
            env_copy(d, c, block_of(y, d), {'y': up}).start()
            env_copy(2 + d, c, block_of(y, d), {'y': down}).start()

    def env_pass_x(c, i, owner):
        env_copy(6 + i, c, block_of(owner, 0), {'x': x_at[1]}).start()
        env_copy(9 + i, c, block_of(owner, 1), {'x': x_at[3]}).start()

    def env_pass(c):
        for d in TAKEN:
            env_copy(d, c, block_of(down, d), {'y': up}).wait_recv()
            env_copy(2 + d, c, block_of(up, d), {'y': down}).wait_recv()
        env_copy(4, c, block_of(down, 0), {'y': up}).start()
        env_copy(5, c, block_of(up, 1), {'y': down}).start()
        env_pass_x(c, 0, down)
        env_pass_x(c, 1, up)

    def env_far(c):
        env_copy(4, c, block_of(far, 0), {'y': up}).wait_recv()
        env_copy(5, c, block_of(far, 1), {'y': down}).wait_recv()
        env_pass_x(c, 2, far)

    def env_share(c):
        for i, owner in enumerate((down, up, far)):
            env_copy(6 + i, c, block_of(owner, 3), {'x': x_at[1]}).wait_recv()
            env_copy(9 + i, c, block_of(owner, 2), {'x': x_at[3]}).wait_recv()
            env_copy(12 + i, c, owner * RING, {'k': other}, RING).start()

    def env_done(c):
        for i, owner in enumerate((down, up, far)):
            env_copy(12 + i, c, owner * RING, {'k': other}, RING, other).wait_recv()

    env_events = (env_start, env_pass, env_far, env_share, env_done)

    def env_before(step):
        for c in range(ENV_PIECES):
            if ENV_STEPS[0][c] == step:
                env_start(c)

    def env_sent(c):
        for kind in range(12):
            env_copy(kind, c, 0, {'k': other}).wait_send()
        for i in range(3):
            env_copy(12 + i, c, 0, {'k': other}, RING).wait_send()

    load_right.wait()
    env_before(0)
    h_buf[1] = jnp.zeros(h_buf.shape[1:], jnp.float32)
    v_buf[...] = jnp.zeros(v_buf.shape, jnp.float32)

    def sum_start(which, phase, value):
        count, me, device = phases[phase]
        red_held[which, phase] = value

        def send(d):
            pltpu.make_async_remote_copy(
                src_ref=red_held.at[which, phase], dst_ref=red_slots.at[which, bases[phase] + me],
                send_sem=red_send.at[which, bases[phase] + d], recv_sem=red_recv.at[which, bases[phase] + me],
                device_id=device(lax.rem(me + d, count)), device_id_type=MESH_IDS).start()
        repeat(1, count, send)
        red_slots[which, bases[phase] + me] = value

    def sum_finish(which, phase):
        count, me, device = phases[phase]

        def wait(d):
            peer = lax.rem(me + d, count)
            copy = pltpu.make_async_remote_copy(
                src_ref=red_held.at[which, phase], dst_ref=red_slots.at[which, bases[phase] + peer],
                send_sem=red_send.at[which, bases[phase] + d], recv_sem=red_recv.at[which, bases[phase] + peer],
                device_id=device(peer), device_id_type=MESH_IDS)
            copy.wait_send()
            copy.wait_recv()
        repeat(1, count, wait)
        return red_slots[which, bases[phase]:bases[phase] + count].sum(0)

    def mean_of(value):
        return jnp.broadcast_to(jnp.sum(value, axis=(0, 1), keepdims=True) * (1.0 / num_elems), TILE)

    def only(tile):
        return tile[:1, :1]

    def fold(values):
        lanes = values.reshape(-1, 8, cols).sum(0)
        tile = lanes[:, :LANES]
        for c in range(LANES, cols, LANES):
            tile = tile + lanes[:, c:c + LANES]
        return tile

    def gather_copy(message):
        index = INDEX[message]
        return pltpu.make_async_remote_copy(
            src_ref=gath.at[0, INDEX[source_of(message)]], dst_ref=gath.at[0, index],
            send_sem=ag_send.at[MESSAGES.index(message)], recv_sem=ag_recv.at[MESSAGES.index(message)],
            device_id=step_to(*LINKS[message]), device_id_type=MESH_IDS)

    def gather_sent(index):
        pltpu.make_async_remote_copy(
            src_ref=gath.at[0, index], dst_ref=gath.at[0, index], send_sem=ag_send.at[index], recv_sem=ag_recv.at[index],
            device_id=step_to(*ALL_LINKS[0]), device_id_type=MESH_IDS).wait_send()

    def sibling_copy(index):
        span = pl.ds(index * GROUP, GROUP)
        return pltpu.make_async_remote_copy(
            src_ref=gath.at[0, span], dst_ref=gath.at[1, span],
            send_sem=sib_send.at[index], recv_sem=sib_recv.at[index],
            device_id={'k': other}, device_id_type=MESH_IDS)

    def groups_after(held, sequence):
        done = {}
        held = set(held)
        for message in sequence:
            held.add(message)
            for i in range(BLOCKS):
                group = HELD[i * GROUP:(i + 1) * GROUP]
                if message in group and held.issuperset(group):
                    done.setdefault(message, []).append(i)
        return done

    def take(message, groups):
        if message in LINKS:
            gather_copy(message).wait_recv()
        for sent in SENDS.get(message, ()):
            gather_copy(sent).start()
        for i in groups.get(message, ()):
            sibling_copy(i).start()

    def own_parts(s):
        each = TREES // PARTS
        return [(s * each + i, 0, 0) for i in range(each)]

    with scope('turn_wait'):
        turn_finish(0)
    with scope('turn'):
        def unpack(pair):
            block = jnp.transpose(turned(0, pair))
            for i, p in enumerate((2 * pair, jnp.minimum(2 * pair + 1, phys - 1))):
                h_buf[0, p] = block[i * rows:(i + 1) * rows, :]
                for part in range(TREES):
                    span = slice(i * rows + part * piece, i * rows + (part + 1) * piece)
                    gath[0, INDEX[part, 0, 0], p] = block[span, :]
        repeat(0, pairs, unpack)
    own = [message for message in HELD if message not in LINKS]
    groups = groups_after((), own + MESSAGES[:EARLY])
    for message in own:
        take(message, groups)

    with scope('left'):
        load_left.wait()
    order = []
    for first, count in CHUNKS:
        order += [(dk, message) for dk in range(CORES) for message in HELD[first:first + count]]
    per_tile = LANES // piece
    lanes = lax.broadcasted_iota(jnp.int32, (rows, LANES), 1)

    left_tiles = {
        (dx, dk, dy): pl.multiple_of(lax.div((x_at[dx] * CORES + k_at[dk]) * RING + y_at[dy], 2) * LANES, LANES)
        for dx in range(RING) for dk in range(CORES) for dy in range(RING)}

    def left_rows(l, c):
        for tile in range(left_own.shape[2] // LANES):
            at = slice(tile * LANES, (tile + 1) * LANES)
            plain = left_own[l, :, at]
            rolled = pltpu.roll(plain, rows, 1)
            left_turn[0, :, at] = jnp.where(lax.rem(y, 2) == 0, plain, rolled)
            left_turn[1, :, at] = jnp.where(lax.rem(y, 2) == 0, rolled, plain)
        for tile in range(left_perm.shape[2] // LANES):
            result = None
            for i in range(per_tile):
                dk, message = order[tile * per_tile + i]
                _, dx, dy = message
                values = left_turn[dy % 2, :, pl.ds(left_tiles[dx, dk, dy], LANES)]
                if i != message[0]:
                    values = pltpu.roll(values, (i - message[0]) * piece % LANES, 1)
                result = values if i == 0 else jnp.where(lanes >= i * piece, values, result)
            left_perm[l, :, tile * LANES:(tile + 1) * LANES] = result
        return c

    with scope('left_order'):
        lax.fori_loop(0, bonds_l, left_rows, 0)

    with scope('mpo'):
        rows_out = lax.dot_general(
            spread_out_ref[...], mpo_ref[...], (((1,), (1,)), ((), ())), precision=FULL_PREC,
            preferred_element_type=jnp.float32)
        wide = dot(rows_out, spread_in_ref[...])
        n_out, n_in = w_mat.shape
        same = jnp.broadcast_to(same_ref[...][None], (n_out // 8, 8, n_in)).reshape(n_out, n_in)
        w_mat[...] = wide * same

    env_before(1)
    with scope('gather_early'):
        for message in MESSAGES[:EARLY]:
            take(message, groups)

    def stage_one(first, count, p, fresh):
        depth = count * piece
        rhs = jnp.concatenate(
            [gath[dk, pl.ds(first, count), p].reshape(depth, cols) for dk in range(CORES)], axis=0)
        column = pl.multiple_of(first * CORES * piece, LANES)
        lhs = left_perm[:, :, pl.ds(column, CORES * depth)].reshape(bonds_l * rows, CORES * depth)
        res = dot(lhs, rhs).reshape(bonds_l, octs, 8, cols)
        acc[p] = jnp.where(fresh, 0.0, acc[p]) + res

    def at_steps(i, events):
        steps = sorted(events)

        def run(steps):
            if len(steps) > 1:
                middle = len(steps) // 2
                lax.cond(i < steps[middle], lambda: run(steps[:middle]), lambda: run(steps[middle:]))
            else:
                for step in steps:
                    @pl.when(i == step)
                    def _():
                        for event in events[step]:
                            event()

        run(steps)

    def way(s):
        return 1 - 2 * lax.rem(s, 2)

    def ring_side(s, n):
        return way(s) * (1 - 2 * lax.rem(n, 2))

    def ring_block(s, n):
        return lax.rem(z + num_z + ring_side(s, n) * (num_z // 2 - lax.div(n + 1, 2)), num_z)

    def ring_copy(src, s, n, h):
        return pltpu.make_async_remote_copy(
            src_ref=src, dst_ref=ring.at[s, n, h], send_sem=rs_send.at[s, n, h], recv_sem=rs_recv.at[s, n, h],
            device_id={'z': lax.rem(z + num_z + ring_side(s, n), num_z)}, device_id_type=MESH_IDS)

    def ring_wait(s, n, h):
        ring_copy(terms.at[s, n, h], s, n, h).wait_recv()

    def ring_pass(s, n, h):
        with scope('ring_pass'):
            ring_wait(s, n - 2, h)
            ring[s, n - 2, h] = ring[s, n - 2, h] + terms[s, n, h]
            ring_copy(ring.at[s, n - 2, h], s, n, h).start()

    def middle(o):
        res = dot(w_mat[...], acc[:, :, o].reshape(phys * bonds_l * 8, cols)).reshape(bonds, phys, 8, cols)
        for r in range(bonds):
            mid[:, o, :, r * cols:(r + 1) * cols] = res[r]

    def last_stage(s, which):
        lhs = mid[:, pl.ds(s * STREAMS, STREAMS)].reshape(phys * slab, bonds * cols)
        for n in which:
            first = pl.multiple_of(ring_block(s, n) * cols, cols)
            rhs = right_full[:, :, :, :, pl.ds(first, cols)].reshape(bonds * cols, cols)
            res = dot(lhs, rhs).reshape(phys, STREAMS, 8, cols)
            for h in range(STREAMS):
                terms[s, n, h] = res[:, h]

    def new_direction(cur, alpha, beta_prev):
        nxt = 1 - cur
        a, b = only(alpha), only(beta_prev)
        def body(p, total):
            w = h_buf[cur, p] - a * v_buf[cur, p] - b * v_buf[nxt, p]
            v_buf[nxt, p] = w
            return total + fold(w * w)

        return lax.fori_loop(0, phys, body, jnp.zeros(TILE, jnp.float32))

    def step(j, carry):
        alpha_part, beta_prev = carry
        cur = lax.rem(j, 2)
        nxt = 1 - cur
        more = j < last_step

        def alpha_z():
            sum_start(0, 1, sum_finish(0, 0))

        def alpha_plane():
            alpha = mean_of(sum_finish(0, 1))
            scal_ref[0, j] = alpha
            sum_start(1, 0, new_direction(cur, alpha, beta_prev))

        def beta_z():
            sum_start(1, 1, sum_finish(1, 0))

        def in_first(event, *what):
            @pl.when(j == 0)
            def _():
                event(*what)

        sum_start(0, 0, alpha_part)
        queue = MESSAGES[EARLY:]
        groups = groups_after(own + MESSAGES[:EARLY], queue)
        wide_steps = 3 * phys
        each = 3 if phys % 3 == 0 else 1
        half_steps = 2 * phys // each
        events = {}
        hooks = dict(zip(HOOKS, (alpha_z, alpha_plane, beta_z)))
        for n, count in enumerate(DURING_ONE):
            at = n * phys // 9 if n < 27 else wide_steps + (n - 27) * half_steps // 6
            at = events.setdefault(at, [])
            at += [functools.partial(take, message, groups) for message in queue[:count]]
            queue = queue[count:]
            for event, steps in zip(env_events, ENV_STEPS):
                at += [functools.partial(in_first, event, c) for c in range(ENV_PIECES) if steps[c] == n + ENV_LEAD]
            if n in CHUNK_STEPS:
                first, count = CHUNKS[CHUNK_STEPS.index(n)]
                at += [sibling_copy(i).wait_recv for i in range(first // GROUP, (first + count) // GROUP)]
            if n in hooks:
                at.append(hooks[n])

        def wide_step(i):
            with scope('events_wide'):
                at_steps(i, {n: e for n, e in events.items() if n < wide_steps})
            with scope('one_wide'):
                stage_one(lax.div(i, phys) * WIDE, WIDE, lax.rem(i, phys), i < phys)

        def half_step(i):
            with scope('events_half'):
                at_steps(i, {n - wide_steps: e for n, e in events.items() if n >= wide_steps})

            with scope('one_half'):
                chunk, p = lax.div(i * each, phys), lax.rem(i * each, phys)
                for q in range(each):
                    stage_one(3 * WIDE + chunk * (WIDE // 2), WIDE // 2, p + q, i < 0)

        repeat(0, wide_steps, wide_step)
        repeat(0, half_steps, half_step)
        with scope('gather_sent'):
            repeat(0, len(MESSAGES), gather_sent)
            repeat(0, BLOCKS, lambda i: sibling_copy(i).wait_send())

        @pl.when(more)
        def _():
            for link in ALL_LINKS:
                pl.semaphore_signal(ag_credit, inc=1, device_id=step_to(*link), device_id_type=MESH_IDS)
            pl.semaphore_signal(ag_credit, inc=1, device_id={'k': other}, device_id_type=MESH_IDS)

        @pl.when(j > 0)
        def _():
            pl.semaphore_wait(rs_credit, 2)

        def scale():
            beta = jnp.sqrt(mean_of(sum_finish(1, 1)))
            scal_ref[1, j] = beta
            inv = only(1.0 / beta)

            def normalize(p):
                v_buf[nxt, p] = v_buf[nxt, p] * inv
            repeat(0, phys, normalize)

            @pl.when(more)
            def _():
                pl.semaphore_wait(ag_credit, len(ALL_LINKS) + 1)

            @pl.when(j == last_step)
            def _():
                pack(1, lambda p: v_buf[nxt, p])
                turn_start(1)

        def finish(s):
            if s == 0:
                scale()
            with scope('ring_end'):
                for h in range(STREAMS):
                    for n in range(max(num_z - 3, 0), num_z - 1):
                        ring_wait(s, n, h)
            alpha, beta = scal_ref[0, j], scal_ref[1, j]
            a, b, inv = only(alpha), only(beta_prev), only(1.0 / beta)
            span = slice(s * slab, (s + 1) * slab)

            def body(p, total):
                new = []
                for h in range(STREAMS):
                    at = slice(s * slab + 8 * h, s * slab + 8 * h + 8)
                    g_new = terms[s, num_z - 1, h, p]
                    for n in range(max(num_z - 3, 0), num_z - 1):
                        g_new = g_new + ring[s, n, h, p]
                    new.append((g_new - a * h_buf[cur, p, at, :] - b * h_buf[nxt, p, at, :]) * inv)
                h_new = jnp.concatenate(new, axis=0)
                h_buf[nxt, p, span, :] = h_new
                for i, message in enumerate(own_parts(s)):
                    gath[0, INDEX[message], p] = h_new[i * piece:(i + 1) * piece]
                return total + fold(v_buf[nxt, p, span, :] * h_new)

            total = lax.fori_loop(0, phys, body, jnp.zeros(TILE, jnp.float32))
            alpha_sum[...] = total if s == 0 else alpha_sum[...] + total

            @pl.when(more)
            def _():
                for message in own_parts(s):
                    take(message, next_groups)

        def early(message):
            @pl.when(more)
            def _():
                take(message, next_groups)

        def happen(event):
            {'pass': ring_pass, 'finish': finish, 'early': early}[event[0]](*event[1:])

        pairs_z = num_z // 2
        ring_steps = PARTS * pairs_z
        pairs_at = []
        for s in PAIR_ORDER:
            if sum(s == other_s for other_s, _ in pairs_at) < pairs_z:
                pairs_at.append((s, sum(s == other_s for other_s, _ in pairs_at)))
        slots = {pair: i for i, pair in enumerate(pairs_at)}
        events = {}
        for s in range(PARTS):
            for n in range(2, num_z - 1):
                at = slots[s, n // 2] + LAGS[s][n - 2]
                events.setdefault(at, []).extend(('pass', s, n, h) for h in range(STREAMS))
            events.setdefault(FINISH[s] * pairs_z // SPAN, []).append(('finish', s))
        tail = [event for at in sorted(events) if at >= ring_steps for event in events.pop(at)]
        queue = MESSAGES[:EARLY]
        for at, count in enumerate(DURING_RING):
            events.setdefault(at * pairs_z // SPAN, []).extend(('early', message) for message in queue[:count])
            queue = queue[count:]
        mixed = []
        spare = list(DURING_TAIL)
        for i, event in enumerate(tail):
            mixed.append(event)
            count = len(queue) if i == len(tail) - 1 else spare.pop(0) if spare else 0
            mixed += [('early', message) for message in queue[:count]]
            queue = queue[count:]
        tail = mixed
        sequence = [event for at in sorted(events) for event in events[at]] + tail
        sequence = [
            message for kind, *what in sequence if kind != 'pass'
            for message in (own_parts(*what) if kind == 'finish' else what)]
        next_groups = groups_after((), sequence)

        def ring_step(i):
            s, t = pairs_at[0]
            for n, pair in enumerate(pairs_at):
                s, t = jnp.where(i == n, pair[0], s), jnp.where(i == n, pair[1], t)

            @pl.when(t == 0)
            def _():
                with scope('middle'):
                    for o in range(STREAMS):
                        middle(s * STREAMS + o)

            with scope('last_stage'):
                last_stage(s, (2 * t, 2 * t + 1))

            @pl.when(t == 0)
            def _():
                for n in range(min(2, num_z - 1)):
                    for h in range(STREAMS):
                        ring_copy(terms.at[s, n, h], s, n, h).start()

            with scope('events_ring'):
                at_steps(i, {at: [functools.partial(happen, event) for event in events[at]] for at in events})

        repeat(0, ring_steps, ring_step)
        with scope('tail'):
            for event in tail:
                happen(event)

        def ring_sent(i):
            s, n = lax.div(i, num_z - 1), lax.rem(i, num_z - 1)
            for h in range(STREAMS):
                ring_copy(terms.at[s, n, h], s, n, h).wait_send()
        repeat(0, PARTS * (num_z - 1), ring_sent)

        @pl.when(more)
        def _():
            for sign in (1, num_z - 1):
                pl.semaphore_signal(
                    rs_credit, inc=1, device_id={'z': lax.rem(z + sign, num_z)}, device_id_type=MESH_IDS)

        return alpha_sum[...], jnp.where(j > 0, scal_ref[1, j], 0.0)

    zero = jnp.zeros(TILE, jnp.float32)
    _, beta_prev = lax.fori_loop(0, LANCZOS_STEPS, step, (zero, zero))
    repeat(0, ENV_PIECES, env_sent)

    cur = LANCZOS_STEPS % 2
    shift = only(scal_ref[0, last_step])
    b = only(beta_prev)

    def end_body(p, sums):
        h, v = h_buf[cur, p], v_buf[cur, p]
        d = h - shift * v - b * v_buf[1 - cur, p]
        h_buf[1 - cur, p] = d
        return tuple(total + fold(term) for total, term in zip(sums, (v * h, d * d, d * v, v * v)))

    sums = lax.fori_loop(0, phys, end_body, (zero,) * 4)
    row = lax.broadcasted_iota(jnp.int32, TILE, 0)

    def squeeze(tile):
        tile = tile + pltpu.roll(tile, 4, 0)
        return tile + pltpu.roll(tile, 2, 0)

    packed = squeeze(sums[0])
    for i in range(1, 4):
        packed = jnp.where(row >= 2 * i, squeeze(sums[i]), packed)
    with scope('end_sum'):
        sum_start(0, 0, packed)
        pack(0, lambda p: h_buf[1 - cur, p])
        turn_start(0)
        sum_start(0, 1, sum_finish(0, 0))
        packed = sum_finish(0, 1)
    v_h, d_d, d_v, v_v = (mean_of(jnp.where((row >= 2 * i) & (row < 2 * i + 2), packed, 0.0)) for i in range(4))
    delta = v_h - shift
    beta = jnp.sqrt(d_d - 2.0 * delta * d_v + delta * delta * v_v)
    scal_ref[0, LANCZOS_STEPS] = v_h
    scal_ref[1, LANCZOS_STEPS] = beta
    inv = only(1.0 / beta)
    delta = only(delta)
    with scope('end_turn_wait'):
        turn_finish(1)
        turn_finish(0)
    with scope('end_turn'):
        def end_unpack(pair):
            block = jnp.transpose((turned(0, pair) - delta * turned(1, pair)) * inv)
            for i, p in enumerate((2 * pair, jnp.minimum(2 * pair + 1, phys - 1))):
                out_ref[p] = block[i * rows:(i + 1) * rows, :]
        repeat(0, pairs, end_unpack)


def solution(mesh):
    grid = fine_mesh(mesh)
    num_z = grid.shape['z']

    def local_run(psi_blk, left_blk, right_blk, mpo_pair):
        full_rows, n_s, n_u, local_cols = psi_blk.shape
        phys = n_s * n_u
        rows = full_rows // RING
        cols = local_cols * RING
        bonds_l, bonds_r = left_blk.shape[1], right_blk.shape[1]
        full_a, full_b = left_blk.shape[2], right_blk.shape[2]
        psi = psi_blk.transpose(1, 2, 3, 0).reshape(phys, local_cols, full_rows)
        left = left_blk.transpose(1, 0, 2)
        right = right_blk.transpose(1, 0, 2).reshape(bonds_r, RING, CORES, 8, full_b)
        mpo = mpo_pair.transpose(0, 2, 3, 4, 5, 1).reshape(bonds_l * phys, phys * bonds_r)
        eye = np.eye(8, dtype=np.float32)
        one = np.ones((1, 8), np.float32)
        order_out = np.arange(phys * bonds_r).reshape(phys, bonds_r).T.ravel()
        order_in = np.arange(bonds_l * phys).reshape(bonds_l, phys).T.ravel()
        spread_out = np.kron(np.eye(order_out.size, dtype=np.float32)[order_out], one.T)
        spread_in = np.kron(np.eye(order_in.size, dtype=np.float32)[:, order_in], one)
        same = np.tile(eye, (1, phys * bonds_l))
        red = num_z + RING * RING * CORES
        pairs = (phys + 1) // 2
        f32 = jnp.float32
        out, scal = pl.pallas_call(
            functools.partial(lanczos_kernel, float(psi_blk.size * grid.size), num_z),
            out_shape=(
                jax.ShapeDtypeStruct((phys, local_cols, full_rows), f32),
                jax.ShapeDtypeStruct((2, LANCZOS_STEPS + 1) + TILE, f32),
            ),
            in_specs=[
                pl.BlockSpec(memory_space=pltpu.VMEM),
                pl.BlockSpec(memory_space=pl.ANY),
                pl.BlockSpec(memory_space=pl.ANY),
            ] + [pl.BlockSpec(memory_space=pltpu.VMEM)] * 4,
            out_specs=(pl.BlockSpec(memory_space=pltpu.VMEM), pl.BlockSpec(memory_space=pltpu.VMEM)),
            scratch_shapes=[
                pltpu.VMEM((CORES, len(HELD), phys, rows // TREES, cols), f32),
                pltpu.VMEM((bonds_r, BLOCKS, CORES, 8, full_b), f32),
                pltpu.VMEM((bonds_l, rows, full_a), f32),
                pltpu.VMEM((2, rows, full_a), f32),
                pltpu.VMEM((bonds_l, rows, full_a), f32),
                pltpu.VMEM((bonds_r * phys * 8, phys * bonds_l * 8), f32),
                pltpu.VMEM((phys, bonds_l, rows // 8, 8, cols), f32),
                pltpu.VMEM((phys, rows // 8, 8, bonds_r * cols), f32),
                pltpu.VMEM((PARTS, num_z, STREAMS, phys, 8, cols), f32),
                pltpu.VMEM((PARTS, num_z - 1, STREAMS, phys, 8, cols), f32),
                pltpu.VMEM((2, phys, rows, cols), f32),
                pltpu.VMEM((2, phys, rows, cols), f32),
                pltpu.VMEM((2, RING, pairs, rows, LANES), f32),
                pltpu.VMEM((2, RING, pairs, rows, LANES), f32),
                pltpu.VMEM((2, 2) + TILE, f32),
                pltpu.VMEM((2, red) + TILE, f32),
                pltpu.VMEM(TILE, f32),
                pltpu.SemaphoreType.DMA((len(MESSAGES),)),
                pltpu.SemaphoreType.DMA((len(MESSAGES),)),
                pltpu.SemaphoreType.DMA((BLOCKS,)),
                pltpu.SemaphoreType.DMA((BLOCKS,)),
                pltpu.SemaphoreType.DMA((PARTS, num_z - 1, STREAMS)),
                pltpu.SemaphoreType.DMA((PARTS, num_z - 1, STREAMS)),
                pltpu.SemaphoreType.DMA((2, red)),
                pltpu.SemaphoreType.DMA((2, red)),
                pltpu.SemaphoreType.DMA((2, RING)),
                pltpu.SemaphoreType.DMA((2, RING)),
                pltpu.SemaphoreType.DMA((15, ENV_PIECES)),
                pltpu.SemaphoreType.DMA((15, ENV_PIECES)),
                pltpu.SemaphoreType.DMA((2,)),
                pltpu.SemaphoreType.REGULAR,
                pltpu.SemaphoreType.REGULAR,
            ],
            compiler_params=pltpu.CompilerParams(
                collective_id=0, has_side_effects=True, vmem_limit_bytes=67043328),
        )(psi, left, right, mpo, spread_out, spread_in, same)
        result = out.reshape(n_s, n_u, local_cols, full_rows).transpose(3, 0, 1, 2)
        return scal[0, 1:, 0, 0], scal[1, 1:, 0, 0], result

    return jax.shard_map(
        local_run, mesh=grid,
        in_specs=(P(('x', 'k'), None, None, ('z', 'y')), P(('x', 'k'), None, None), P(('z', 'y'), None, None), P()),
        out_specs=(P(), P(), P(('x', 'k'), None, None, ('z', 'y'))), check_vma=False)
```

```python
import functools
import itertools

import jax
import jax.numpy as jnp
import numpy as np
from jax import lax
from jax.experimental import pallas as pl
from jax.experimental.pallas import tpu as pltpu
from jax.sharding import Mesh, PartitionSpec as P

LANCZOS_STEPS = 4
FULL_PREC = lax.Precision.HIGHEST
MESH_IDS = pl.DeviceIdType.MESH
scope = jax.named_scope
SUB = 8
LANES = 128
TILE = (SUB, LANES)
RING = 4
CORES = 2
PARTS = 4
STREAMS = 2
TREES = 4
BLOCKS = RING * RING
ALL_LINKS = [('x', 1), ('y', 1), ('x', -1), ('y', -1)]


def fine_mesh(mesh):
    shape = (mesh.shape['col'] // RING, RING, mesh.shape['row'] // CORES, CORES)
    return Mesh(mesh.devices.reshape(shape), ('z', 'y', 'x', 'k'))


def near(d):
    return min(d, RING - d)


def make_tree(turn):
    prefer = ALL_LINKS[turn:] + ALL_LINKS[:turn]
    load = dict.fromkeys(prefer, 0)
    tree = {}
    for offset in sorted(itertools.product(range(RING), repeat=2), key=lambda o: near(o[0]) + near(o[1])):
        options = [
            (axis, sign) for axis, d in zip('xy', offset) for sign in (-1, 1)
            if d and (-sign * d) % RING == near(d)]
        if options:
            tree[offset] = min(options, key=lambda link: (load[link], prefer.index(link)))
            load[tree[offset]] += 1
    return tree


def source_of(message):
    part, dx, dy = message
    axis, sign = LINKS[message]
    return (part, (dx + sign) % RING, dy) if axis == 'x' else (part, dx, (dy + sign) % RING)


LINKS = {(part, *offset): link for part in range(TREES) for offset, link in make_tree(part % len(ALL_LINKS)).items()}
SENDS = {}
for sent in LINKS:
    SENDS.setdefault(source_of(sent), []).append(sent)


def gather_order(release):
    free = dict.fromkeys(ALL_LINKS, 0.0)
    arrival = {}
    order = []

    def issue(now, message):
        order.append(message)
        for sent in SENDS.get(message, ()):
            link = LINKS[sent]
            free[link] = max(free[link], now) + 1.0
            arrival[sent] = free[link] + 0.6

    todo = [(now, (part, 0, 0)) for part, now in enumerate(release)]
    while len(order) < TREES * BLOCKS:
        left = [(now, message) for message, now in arrival.items() if message not in order]
        if todo and (not left or min(left)[0] > todo[0][0]):
            issue(*todo.pop(0))
        else:
            issue(*min(left))
    return order


def counts(*texts):
    return [int(c, 36) for text in texts for c in text]


RELEASE = [0, 2.9, 4.5, 8.0]
PAIR_ORDER = counts('0101220013132323')
LAGS = (counts('11011'), counts('35040'), counts('39276'), counts('17387'))
FINISH = [9, 17, 23, 24]
HOOKS = (7, 15, 30)
DURING_ONE = counts('500020104111105222303030100', '301300')
DURING_RING = counts('0000000000000400')
DURING_TAIL = counts('000102004010301')
EARLY = sum(DURING_RING) + sum(DURING_TAIL)
ENV_STEPS = (counts('g515i4mp'), counts('sa2btbvw'), counts('wh8kwrww'), counts('wkbnwtxw'), counts('xontywyx'))
ENV_PIECES = len(ENV_STEPS[0])
ENV_LEAD = 2
CHUNK_STEPS = (0, 9, 18, 27, 30)
SPAN = 4
HELD = gather_order(RELEASE)
INDEX = {message: i for i, message in enumerate(HELD)}
MESSAGES = [message for message in HELD if message in LINKS]
GROUP = TREES
WIDE = len(HELD) // 4
CHUNKS = [(c * WIDE, WIDE) for c in range(3)] + [(3 * WIDE + c * WIDE // 2, WIDE // 2) for c in range(2)]


def dot(lhs, rhs):
    return jnp.dot(lhs, rhs, precision=FULL_PREC, preferred_element_type=jnp.float32)


def lanczos_kernel(
        num_elems, num_z, psi_ref, left_ref, right_ref, mpo_ref, spread_out_ref, spread_in_ref, same_ref, out_ref, scal_ref,
        gath, right_full, left_own, left_turn, left_perm, w_mat, acc, mid, terms, ring, h_buf, v_buf, pack_out, pack_in,
        red_held, red_slots, alpha_sum,
        ag_send, ag_recv, sib_send, sib_recv, rs_send, rs_recv, red_send, red_recv, turn_send, turn_recv,
        env_send, env_recv, load_sem, ag_credit, rs_credit):
    phys, rows, cols = h_buf.shape[1:]
    bonds = right_full.shape[0]
    bonds_l = left_own.shape[0]
    piece = rows // TREES
    slab = rows // PARTS
    octs = rows // 8
    pairs = pack_in.shape[2]
    last_step = LANCZOS_STEPS - 1
    z, y, x, k = (lax.axis_index(name) for name in ('z', 'y', 'x', 'k'))
    other = 1 - k

    x_at, y_at = ([lax.rem(pos + d, RING) for d in range(RING)] for pos in (x, y))
    k_at = (k, other)

    def step_to(axis, sign):
        return {axis: {'x': x_at, 'y': y_at}[axis][sign % RING]}

    phases = (
        (num_z, z, lambda i: {'z': i}),
        (RING * RING * CORES, (x * CORES + k) * RING + y,
         lambda i: {'x': lax.div(i, CORES * RING), 'k': lax.rem(lax.div(i, RING), CORES), 'y': lax.rem(i, RING)}),
    )
    bases = (0, num_z)
    barrier = pltpu.get_barrier_semaphore()
    def repeat(lo, hi, fn):
        def body(i, c):
            fn(i)
            return c
        lax.fori_loop(lo, hi, body, 0)

    for count, me, device in phases:
        def enter(d, count=count, me=me, device=device):
            pl.semaphore_signal(barrier, inc=1, device_id=device(lax.rem(me + d, count)), device_id_type=MESH_IDS)
        repeat(1, count, enter)

    own_rows = pl.multiple_of(y * rows, rows)
    load_left = pltpu.make_async_copy(left_ref.at[:, pl.ds(own_rows, rows), :], left_own, load_sem.at[0])
    load_left.start()
    load_right = pltpu.make_async_copy(right_ref, right_full.at[:, pl.ds(y * RING, RING)], load_sem.at[1])
    load_right.start()

    lane = lax.broadcasted_iota(jnp.int32, (rows, LANES), 1)

    def pack(which, value):
        def body(pair):
            halves = [value(2 * pair), value(jnp.minimum(2 * pair + 1, phys - 1))]
            for target in range(RING):
                tile, half = divmod(target * rows, LANES)
                first, second = (v[:, tile * LANES:(tile + 1) * LANES] for v in halves)
                if half == 0:
                    second = pltpu.roll(second, rows, 1)
                else:
                    first = pltpu.roll(first, rows, 1)
                pack_out[which, target, pair] = jnp.where(lane < rows, first, second)
        repeat(0, pairs, body)

    def turn_copy(which, src, dst, d, device):
        return pltpu.make_async_remote_copy(
            src_ref=pack_out.at[which, src], dst_ref=pack_in.at[which, dst],
            send_sem=turn_send.at[which, d], recv_sem=turn_recv.at[which, dst],
            device_id=device, device_id_type=MESH_IDS)

    def turn_start(which):
        for d in range(1, RING):
            peer = y_at[d]
            turn_copy(which, peer, y, d, {'y': peer}).start()
        pack_in[which, y] = pack_out[which, y]

    def turn_finish(which):
        for d in range(1, RING):
            peer = y_at[d]
            copy = turn_copy(which, peer, peer, d, {'y': peer})
            copy.wait_send()
            copy.wait_recv()

    def turned(which, pair):
        return jnp.concatenate([pack_in[which, i, pair] for i in range(RING)], axis=0)

    with scope('pack'):
        pack(0, lambda p: psi_ref[p])
    with scope('entry_barrier'):
        pl.semaphore_wait(barrier, sum(count - 1 for count, _, _ in phases))
    turn_start(0)

    up, down, far = y_at[1], y_at[3], y_at[2]
    strip = right_full.shape[-1] // ENV_PIECES

    def env_copy(kind, c, block, device, count=1, core=None):
        span = pl.ds(c * strip, strip)
        row = k if core is None else core
        view = right_full.at[:, pl.ds(block, count), pl.ds(row, 1), :, span]
        return pltpu.make_async_remote_copy(
            src_ref=view, dst_ref=view, send_sem=env_send.at[kind, c], recv_sem=env_recv.at[kind, c],
            device_id=device, device_id_type=MESH_IDS)

    def block_of(owner, d):
        return owner * RING + x_at[d]

    TAKEN = (0, 1)

    def env_start(c):
        for d in TAKEN:
            env_copy(d, c, block_of(y, d), {'y': up}).start()
            env_copy(2 + d, c, block_of(y, d), {'y': down}).start()

    def env_pass_x(c, i, owner):
        env_copy(6 + i, c, block_of(owner, 0), {'x': x_at[1]}).start()
        env_copy(9 + i, c, block_of(owner, 1), {'x': x_at[3]}).start()

    def env_pass(c):
        for d in TAKEN:
            env_copy(d, c, block_of(down, d), {'y': up}).wait_recv()
            env_copy(2 + d, c, block_of(up, d), {'y': down}).wait_recv()
        env_copy(4, c, block_of(down, 0), {'y': up}).start()
        env_copy(5, c, block_of(up, 1), {'y': down}).start()
        env_pass_x(c, 0, down)
        env_pass_x(c, 1, up)

    def env_far(c):
        env_copy(4, c, block_of(far, 0), {'y': up}).wait_recv()
        env_copy(5, c, block_of(far, 1), {'y': down}).wait_recv()
        env_pass_x(c, 2, far)

    def env_share(c):
        for i, owner in enumerate((down, up, far)):
            env_copy(6 + i, c, block_of(owner, 3), {'x': x_at[1]}).wait_recv()
            env_copy(9 + i, c, block_of(owner, 2), {'x': x_at[3]}).wait_recv()
            env_copy(12 + i, c, owner * RING, {'k': other}, RING).start()

    def env_done(c):
        for i, owner in enumerate((down, up, far)):
            env_copy(12 + i, c, owner * RING, {'k': other}, RING, other).wait_recv()

    env_events = (env_start, env_pass, env_far, env_share, env_done)

    def env_before(step):
        for c in range(ENV_PIECES):
            if ENV_STEPS[0][c] == step:
                env_start(c)

    def env_sent(c):
        for kind in range(12):
            env_copy(kind, c, 0, {'k': other}).wait_send()
        for i in range(3):
            env_copy(12 + i, c, 0, {'k': other}, RING).wait_send()

    load_right.wait()
    env_before(0)
    h_buf[1] = jnp.zeros(h_buf.shape[1:], jnp.float32)
    v_buf[...] = jnp.zeros(v_buf.shape, jnp.float32)

    def sum_start(which, phase, value):
        count, me, device = phases[phase]
        red_held[which, phase] = value

        def send(d):
            pltpu.make_async_remote_copy(
                src_ref=red_held.at[which, phase], dst_ref=red_slots.at[which, bases[phase] + me],
                send_sem=red_send.at[which, bases[phase] + d], recv_sem=red_recv.at[which, bases[phase] + me],
                device_id=device(lax.rem(me + d, count)), device_id_type=MESH_IDS).start()
        repeat(1, count, send)
        red_slots[which, bases[phase] + me] = value

    def sum_finish(which, phase):
        count, me, device = phases[phase]

        def wait(d):
            peer = lax.rem(me + d, count)
            copy = pltpu.make_async_remote_copy(
                src_ref=red_held.at[which, phase], dst_ref=red_slots.at[which, bases[phase] + peer],
                send_sem=red_send.at[which, bases[phase] + d], recv_sem=red_recv.at[which, bases[phase] + peer],
                device_id=device(peer), device_id_type=MESH_IDS)
            copy.wait_send()
            copy.wait_recv()
        repeat(1, count, wait)
        return red_slots[which, bases[phase]:bases[phase] + count].sum(0)

    def mean_of(value):
        return jnp.broadcast_to(jnp.sum(value, axis=(0, 1), keepdims=True) * (1.0 / num_elems), TILE)

    def only(tile):
        return tile[:1, :1]

    def fold(values):
        lanes = values.reshape(-1, 8, cols).sum(0)
        tile = lanes[:, :LANES]
        for c in range(LANES, cols, LANES):
            tile = tile + lanes[:, c:c + LANES]
        return tile

    def gather_copy(message):
        index = INDEX[message]
        return pltpu.make_async_remote_copy(
            src_ref=gath.at[0, INDEX[source_of(message)]], dst_ref=gath.at[0, index],
            send_sem=ag_send.at[MESSAGES.index(message)], recv_sem=ag_recv.at[MESSAGES.index(message)],
            device_id=step_to(*LINKS[message]), device_id_type=MESH_IDS)

    def gather_sent(index):
        pltpu.make_async_remote_copy(
            src_ref=gath.at[0, index], dst_ref=gath.at[0, index], send_sem=ag_send.at[index], recv_sem=ag_recv.at[index],
            device_id=step_to(*ALL_LINKS[0]), device_id_type=MESH_IDS).wait_send()

    def sibling_copy(index):
        span = pl.ds(index * GROUP, GROUP)
        return pltpu.make_async_remote_copy(
            src_ref=gath.at[0, span], dst_ref=gath.at[1, span],
            send_sem=sib_send.at[index], recv_sem=sib_recv.at[index],
            device_id={'k': other}, device_id_type=MESH_IDS)

    def groups_after(held, sequence):
        done = {}
        held = set(held)
        for message in sequence:
            held.add(message)
            for i in range(BLOCKS):
                group = HELD[i * GROUP:(i + 1) * GROUP]
                if message in group and held.issuperset(group):
                    done.setdefault(message, []).append(i)
        return done

    def take(message, groups):
        if message in LINKS:
            gather_copy(message).wait_recv()
        for sent in SENDS.get(message, ()):
            gather_copy(sent).start()
        for i in groups.get(message, ()):
            sibling_copy(i).start()

    def own_parts(s):
        each = TREES // PARTS
        return [(s * each + i, 0, 0) for i in range(each)]

    with scope('left'):
        load_left.wait()
    order = []
    for first, count in CHUNKS:
        order += [(dk, message) for dk in range(CORES) for message in HELD[first:first + count]]
    per_tile = LANES // piece
    lanes = lax.broadcasted_iota(jnp.int32, (rows, LANES), 1)

    left_tiles = {
        (dx, dk, dy): pl.multiple_of(lax.div((x_at[dx] * CORES + k_at[dk]) * RING + y_at[dy], 2) * LANES, LANES)
        for dx in range(RING) for dk in range(CORES) for dy in range(RING)}

    def left_rows(l, c):
        for tile in range(left_own.shape[2] // LANES):
            at = slice(tile * LANES, (tile + 1) * LANES)
            plain = left_own[l, :, at]
            rolled = pltpu.roll(plain, rows, 1)
            left_turn[0, :, at] = jnp.where(lax.rem(y, 2) == 0, plain, rolled)
            left_turn[1, :, at] = jnp.where(lax.rem(y, 2) == 0, rolled, plain)
        for tile in range(left_perm.shape[2] // LANES):
            result = None
            for i in range(per_tile):
                dk, message = order[tile * per_tile + i]
                _, dx, dy = message
                values = left_turn[dy % 2, :, pl.ds(left_tiles[dx, dk, dy], LANES)]
                if i != message[0]:
                    values = pltpu.roll(values, (i - message[0]) * piece % LANES, 1)
                result = values if i == 0 else jnp.where(lanes >= i * piece, values, result)
            left_perm[l, :, tile * LANES:(tile + 1) * LANES] = result
        return c

    with scope('left_order'):
        lax.fori_loop(0, bonds_l, left_rows, 0)

    with scope('mpo'):
        rows_out = lax.dot_general(
            spread_out_ref[...], mpo_ref[...], (((1,), (1,)), ((), ())), precision=FULL_PREC,
            preferred_element_type=jnp.float32)
        wide = dot(rows_out, spread_in_ref[...])
        n_out, n_in = w_mat.shape
        same = jnp.broadcast_to(same_ref[...][None], (n_out // 8, 8, n_in)).reshape(n_out, n_in)
        w_mat[...] = wide * same

    with scope('turn_wait'):
        turn_finish(0)
    with scope('turn'):
        def unpack(pair):
            block = jnp.transpose(turned(0, pair))
            for i, p in enumerate((2 * pair, jnp.minimum(2 * pair + 1, phys - 1))):
                h_buf[0, p] = block[i * rows:(i + 1) * rows, :]
                for part in range(TREES):
                    span = slice(i * rows + part * piece, i * rows + (part + 1) * piece)
                    gath[0, INDEX[part, 0, 0], p] = block[span, :]
        repeat(0, pairs, unpack)
    own = [message for message in HELD if message not in LINKS]
    groups = groups_after((), own + MESSAGES[:EARLY])
    for message in own:
        take(message, groups)

    env_before(1)
    with scope('gather_early'):
        for message in MESSAGES[:EARLY]:
            take(message, groups)

    def stage_one(first, count, p, fresh):
        depth = count * piece
        rhs = jnp.concatenate(
            [gath[dk, pl.ds(first, count), p].reshape(depth, cols) for dk in range(CORES)], axis=0)
        column = pl.multiple_of(first * CORES * piece, LANES)
        lhs = left_perm[:, :, pl.ds(column, CORES * depth)].reshape(bonds_l * rows, CORES * depth)
        res = dot(lhs, rhs).reshape(bonds_l, octs, 8, cols)
        acc[p] = jnp.where(fresh, 0.0, acc[p]) + res

    def at_steps(i, events):
        steps = sorted(events)

        def run(steps):
            if len(steps) > 1:
                middle = len(steps) // 2
                lax.cond(i < steps[middle], lambda: run(steps[:middle]), lambda: run(steps[middle:]))
            else:
                for step in steps:
                    @pl.when(i == step)
                    def _():
                        for event in events[step]:
                            event()

        run(steps)

    def way(s):
        return 1 - 2 * lax.rem(s, 2)

    def ring_side(s, n):
        return way(s) * (1 - 2 * lax.rem(n, 2))

    def ring_block(s, n):
        return lax.rem(z + num_z + ring_side(s, n) * (num_z // 2 - lax.div(n + 1, 2)), num_z)

    def ring_copy(src, s, n, h):
        return pltpu.make_async_remote_copy(
            src_ref=src, dst_ref=ring.at[s, n, h], send_sem=rs_send.at[s, n, h], recv_sem=rs_recv.at[s, n, h],
            device_id={'z': lax.rem(z + num_z + ring_side(s, n), num_z)}, device_id_type=MESH_IDS)

    def ring_wait(s, n, h):
        ring_copy(terms.at[s, n, h], s, n, h).wait_recv()

    def ring_pass(s, n, h):
        with scope('ring_pass'):
            ring_wait(s, n - 2, h)
            ring[s, n - 2, h] = ring[s, n - 2, h] + terms[s, n, h]
            ring_copy(ring.at[s, n - 2, h], s, n, h).start()

    def middle(o):
        res = dot(w_mat[...], acc[:, :, o].reshape(phys * bonds_l * 8, cols)).reshape(bonds, phys, 8, cols)
        for r in range(bonds):
            mid[:, o, :, r * cols:(r + 1) * cols] = res[r]

    def last_stage(s, which):
        lhs = mid[:, pl.ds(s * STREAMS, STREAMS)].reshape(phys * slab, bonds * cols)
        for n in which:
            first = pl.multiple_of(ring_block(s, n) * cols, cols)
            rhs = right_full[:, :, :, :, pl.ds(first, cols)].reshape(bonds * cols, cols)
            res = dot(lhs, rhs).reshape(phys, STREAMS, 8, cols)
            for h in range(STREAMS):
                terms[s, n, h] = res[:, h]

    def new_direction(cur, alpha, beta_prev):
        nxt = 1 - cur
        a, b = only(alpha), only(beta_prev)
        def body(p, total):
            w = h_buf[cur, p] - a * v_buf[cur, p] - b * v_buf[nxt, p]
            v_buf[nxt, p] = w
            return total + fold(w * w)

        return lax.fori_loop(0, phys, body, jnp.zeros(TILE, jnp.float32))

    def step(j, carry):
        alpha_part, beta_prev = carry
        cur = lax.rem(j, 2)
        nxt = 1 - cur
        more = j < last_step

        def alpha_z():
            sum_start(0, 1, sum_finish(0, 0))

        def alpha_plane():
            alpha = mean_of(sum_finish(0, 1))
            scal_ref[0, j] = alpha
            sum_start(1, 0, new_direction(cur, alpha, beta_prev))

        def beta_z():
            sum_start(1, 1, sum_finish(1, 0))

        def in_first(event, *what):
            @pl.when(j == 0)
            def _():
                event(*what)

        sum_start(0, 0, alpha_part)
        queue = MESSAGES[EARLY:]
        groups = groups_after(own + MESSAGES[:EARLY], queue)
        wide_steps = 3 * phys
        each = 3 if phys % 3 == 0 else 1
        half_steps = 2 * phys // each
        events = {}
        hooks = dict(zip(HOOKS, (alpha_z, alpha_plane, beta_z)))
        for n, count in enumerate(DURING_ONE):
            at = n * phys // 9 if n < 27 else wide_steps + (n - 27) * half_steps // 6
            at = events.setdefault(at, [])
            at += [functools.partial(take, message, groups) for message in queue[:count]]
            queue = queue[count:]
            for event, steps in zip(env_events, ENV_STEPS):
                at += [functools.partial(in_first, event, c) for c in range(ENV_PIECES) if steps[c] == n + ENV_LEAD]
            if n in CHUNK_STEPS:
                first, count = CHUNKS[CHUNK_STEPS.index(n)]
                at += [sibling_copy(i).wait_recv for i in range(first // GROUP, (first + count) // GROUP)]
            if n in hooks:
                at.append(hooks[n])

        def wide_step(i):
            with scope('events_wide'):
                at_steps(i, {n: e for n, e in events.items() if n < wide_steps})
            with scope('one_wide'):
                stage_one(lax.div(i, phys) * WIDE, WIDE, lax.rem(i, phys), i < phys)

        def half_step(i):
            with scope('events_half'):
                at_steps(i, {n - wide_steps: e for n, e in events.items() if n >= wide_steps})

            with scope('one_half'):
                chunk, p = lax.div(i * each, phys), lax.rem(i * each, phys)
                for q in range(each):
                    stage_one(3 * WIDE + chunk * (WIDE // 2), WIDE // 2, p + q, i < 0)

        repeat(0, wide_steps, wide_step)
        repeat(0, half_steps, half_step)
        with scope('gather_sent'):
            repeat(0, len(MESSAGES), gather_sent)
            repeat(0, BLOCKS, lambda i: sibling_copy(i).wait_send())

        @pl.when(more)
        def _():
            for link in ALL_LINKS:
                pl.semaphore_signal(ag_credit, inc=1, device_id=step_to(*link), device_id_type=MESH_IDS)
            pl.semaphore_signal(ag_credit, inc=1, device_id={'k': other}, device_id_type=MESH_IDS)

        @pl.when(j > 0)
        def _():
            pl.semaphore_wait(rs_credit, 2)

        def scale():
            beta = jnp.sqrt(mean_of(sum_finish(1, 1)))
            scal_ref[1, j] = beta
            inv = only(1.0 / beta)

            def normalize(p):
                v_buf[nxt, p] = v_buf[nxt, p] * inv
            repeat(0, phys, normalize)

            @pl.when(more)
            def _():
                pl.semaphore_wait(ag_credit, len(ALL_LINKS) + 1)

            @pl.when(j == last_step)
            def _():
                pack(1, lambda p: v_buf[nxt, p])
                turn_start(1)

        def finish(s):
            if s == 0:
                scale()
            with scope('ring_end'):
                for h in range(STREAMS):
                    for n in range(max(num_z - 3, 0), num_z - 1):
                        ring_wait(s, n, h)
            alpha, beta = scal_ref[0, j], scal_ref[1, j]
            a, b, inv = only(alpha), only(beta_prev), only(1.0 / beta)
            span = slice(s * slab, (s + 1) * slab)

            def body(p, total):
                new = []
                for h in range(STREAMS):
                    at = slice(s * slab + 8 * h, s * slab + 8 * h + 8)
                    g_new = terms[s, num_z - 1, h, p]
                    for n in range(max(num_z - 3, 0), num_z - 1):
                        g_new = g_new + ring[s, n, h, p]
                    new.append((g_new - a * h_buf[cur, p, at, :] - b * h_buf[nxt, p, at, :]) * inv)
                h_new = jnp.concatenate(new, axis=0)
                h_buf[nxt, p, span, :] = h_new
                for i, message in enumerate(own_parts(s)):
                    gath[0, INDEX[message], p] = h_new[i * piece:(i + 1) * piece]
                return total + fold(v_buf[nxt, p, span, :] * h_new)

            total = lax.fori_loop(0, phys, body, jnp.zeros(TILE, jnp.float32))
            alpha_sum[...] = total if s == 0 else alpha_sum[...] + total

            @pl.when(more)
            def _():
                for message in own_parts(s):
                    take(message, next_groups)

        def early(message):
            @pl.when(more)
            def _():
                take(message, next_groups)

        def happen(event):
            {'pass': ring_pass, 'finish': finish, 'early': early}[event[0]](*event[1:])

        pairs_z = num_z // 2
        ring_steps = PARTS * pairs_z
        pairs_at = []
        for s in PAIR_ORDER:
            if sum(s == other_s for other_s, _ in pairs_at) < pairs_z:
                pairs_at.append((s, sum(s == other_s for other_s, _ in pairs_at)))
        slots = {pair: i for i, pair in enumerate(pairs_at)}
        events = {}
        for s in range(PARTS):
            for n in range(2, num_z - 1):
                at = slots[s, n // 2] + LAGS[s][n - 2]
                events.setdefault(at, []).extend(('pass', s, n, h) for h in range(STREAMS))
            events.setdefault(FINISH[s] * pairs_z // SPAN, []).append(('finish', s))
        tail = [event for at in sorted(events) if at >= ring_steps for event in events.pop(at)]
        queue = MESSAGES[:EARLY]
        for at, count in enumerate(DURING_RING):
            events.setdefault(at * pairs_z // SPAN, []).extend(('early', message) for message in queue[:count])
            queue = queue[count:]
        mixed = []
        spare = list(DURING_TAIL)
        for i, event in enumerate(tail):
            mixed.append(event)
            count = len(queue) if i == len(tail) - 1 else spare.pop(0) if spare else 0
            mixed += [('early', message) for message in queue[:count]]
            queue = queue[count:]
        tail = mixed
        sequence = [event for at in sorted(events) for event in events[at]] + tail
        sequence = [
            message for kind, *what in sequence if kind != 'pass'
            for message in (own_parts(*what) if kind == 'finish' else what)]
        next_groups = groups_after((), sequence)

        def ring_step(i):
            s, t = pairs_at[0]
            for n, pair in enumerate(pairs_at):
                s, t = jnp.where(i == n, pair[0], s), jnp.where(i == n, pair[1], t)

            @pl.when(t == 0)
            def _():
                with scope('middle'):
                    for o in range(STREAMS):
                        middle(s * STREAMS + o)

            with scope('last_stage'):
                last_stage(s, (2 * t, 2 * t + 1))

            @pl.when(t == 0)
            def _():
                for n in range(min(2, num_z - 1)):
                    for h in range(STREAMS):
                        ring_copy(terms.at[s, n, h], s, n, h).start()

            with scope('events_ring'):
                at_steps(i, {at: [functools.partial(happen, event) for event in events[at]] for at in events})

        repeat(0, ring_steps, ring_step)
        with scope('tail'):
            for event in tail:
                happen(event)

        def ring_sent(i):
            s, n = lax.div(i, num_z - 1), lax.rem(i, num_z - 1)
            for h in range(STREAMS):
                ring_copy(terms.at[s, n, h], s, n, h).wait_send()
        repeat(0, PARTS * (num_z - 1), ring_sent)

        @pl.when(more)
        def _():
            for sign in (1, num_z - 1):
                pl.semaphore_signal(
                    rs_credit, inc=1, device_id={'z': lax.rem(z + sign, num_z)}, device_id_type=MESH_IDS)

        return alpha_sum[...], jnp.where(j > 0, scal_ref[1, j], 0.0)

    zero = jnp.zeros(TILE, jnp.float32)
    _, beta_prev = lax.fori_loop(0, LANCZOS_STEPS, step, (zero, zero))
    repeat(0, ENV_PIECES, env_sent)

    cur = LANCZOS_STEPS % 2
    shift = only(scal_ref[0, last_step])
    b = only(beta_prev)

    def end_body(p, sums):
        h, v = h_buf[cur, p], v_buf[cur, p]
        d = h - shift * v - b * v_buf[1 - cur, p]
        h_buf[1 - cur, p] = d
        return tuple(total + fold(term) for total, term in zip(sums, (v * h, d * d, d * v, v * v)))

    sums = lax.fori_loop(0, phys, end_body, (zero,) * 4)
    row = lax.broadcasted_iota(jnp.int32, TILE, 0)

    def squeeze(tile):
        tile = tile + pltpu.roll(tile, 4, 0)
        return tile + pltpu.roll(tile, 2, 0)

    packed = squeeze(sums[0])
    for i in range(1, 4):
        packed = jnp.where(row >= 2 * i, squeeze(sums[i]), packed)
    with scope('end_sum'):
        sum_start(0, 0, packed)
        pack(0, lambda p: h_buf[1 - cur, p])
        turn_start(0)
        sum_start(0, 1, sum_finish(0, 0))
        packed = sum_finish(0, 1)
    v_h, d_d, d_v, v_v = (mean_of(jnp.where((row >= 2 * i) & (row < 2 * i + 2), packed, 0.0)) for i in range(4))
    delta = v_h - shift
    beta = jnp.sqrt(d_d - 2.0 * delta * d_v + delta * delta * v_v)
    scal_ref[0, LANCZOS_STEPS] = v_h
    scal_ref[1, LANCZOS_STEPS] = beta
    inv = only(1.0 / beta)
    delta = only(delta)
    with scope('end_turn_wait'):
        turn_finish(1)
        turn_finish(0)
    with scope('end_turn'):
        def end_unpack(pair):
            block = jnp.transpose((turned(0, pair) - delta * turned(1, pair)) * inv)
            for i, p in enumerate((2 * pair, jnp.minimum(2 * pair + 1, phys - 1))):
                out_ref[p] = block[i * rows:(i + 1) * rows, :]
        repeat(0, pairs, end_unpack)


def solution(mesh):
    grid = fine_mesh(mesh)
    num_z = grid.shape['z']

    def local_run(psi_blk, left_blk, right_blk, mpo_pair):
        full_rows, n_s, n_u, local_cols = psi_blk.shape
        phys = n_s * n_u
        rows = full_rows // RING
        cols = local_cols * RING
        bonds_l, bonds_r = left_blk.shape[1], right_blk.shape[1]
        full_a, full_b = left_blk.shape[2], right_blk.shape[2]
        psi = psi_blk.transpose(1, 2, 3, 0).reshape(phys, local_cols, full_rows)
        left = left_blk.transpose(1, 0, 2)
        right = right_blk.transpose(1, 0, 2).reshape(bonds_r, RING, CORES, 8, full_b)
        mpo = mpo_pair.transpose(0, 2, 3, 4, 5, 1).reshape(bonds_l * phys, phys * bonds_r)
        eye = np.eye(8, dtype=np.float32)
        one = np.ones((1, 8), np.float32)
        order_out = np.arange(phys * bonds_r).reshape(phys, bonds_r).T.ravel()
        order_in = np.arange(bonds_l * phys).reshape(bonds_l, phys).T.ravel()
        spread_out = np.kron(np.eye(order_out.size, dtype=np.float32)[order_out], one.T)
        spread_in = np.kron(np.eye(order_in.size, dtype=np.float32)[:, order_in], one)
        same = np.tile(eye, (1, phys * bonds_l))
        red = num_z + RING * RING * CORES
        pairs = (phys + 1) // 2
        f32 = jnp.float32
        out, scal = pl.pallas_call(
            functools.partial(lanczos_kernel, float(psi_blk.size * grid.size), num_z),
            out_shape=(
                jax.ShapeDtypeStruct((phys, local_cols, full_rows), f32),
                jax.ShapeDtypeStruct((2, LANCZOS_STEPS + 1) + TILE, f32),
            ),
            in_specs=[
                pl.BlockSpec(memory_space=pltpu.VMEM),
                pl.BlockSpec(memory_space=pl.ANY),
                pl.BlockSpec(memory_space=pl.ANY),
            ] + [pl.BlockSpec(memory_space=pltpu.VMEM)] * 4,
            out_specs=(pl.BlockSpec(memory_space=pltpu.VMEM), pl.BlockSpec(memory_space=pltpu.VMEM)),
            scratch_shapes=[
                pltpu.VMEM((CORES, len(HELD), phys, rows // TREES, cols), f32),
                pltpu.VMEM((bonds_r, BLOCKS, CORES, 8, full_b), f32),
                pltpu.VMEM((bonds_l, rows, full_a), f32),
                pltpu.VMEM((2, rows, full_a), f32),
                pltpu.VMEM((bonds_l, rows, full_a), f32),
                pltpu.VMEM((bonds_r * phys * 8, phys * bonds_l * 8), f32),
                pltpu.VMEM((phys, bonds_l, rows // 8, 8, cols), f32),
                pltpu.VMEM((phys, rows // 8, 8, bonds_r * cols), f32),
                pltpu.VMEM((PARTS, num_z, STREAMS, phys, 8, cols), f32),
                pltpu.VMEM((PARTS, num_z - 1, STREAMS, phys, 8, cols), f32),
                pltpu.VMEM((2, phys, rows, cols), f32),
                pltpu.VMEM((2, phys, rows, cols), f32),
                pltpu.VMEM((2, RING, pairs, rows, LANES), f32),
                pltpu.VMEM((2, RING, pairs, rows, LANES), f32),
                pltpu.VMEM((2, 2) + TILE, f32),
                pltpu.VMEM((2, red) + TILE, f32),
                pltpu.VMEM(TILE, f32),
                pltpu.SemaphoreType.DMA((len(MESSAGES),)),
                pltpu.SemaphoreType.DMA((len(MESSAGES),)),
                pltpu.SemaphoreType.DMA((BLOCKS,)),
                pltpu.SemaphoreType.DMA((BLOCKS,)),
                pltpu.SemaphoreType.DMA((PARTS, num_z - 1, STREAMS)),
                pltpu.SemaphoreType.DMA((PARTS, num_z - 1, STREAMS)),
                pltpu.SemaphoreType.DMA((2, red)),
                pltpu.SemaphoreType.DMA((2, red)),
                pltpu.SemaphoreType.DMA((2, RING)),
                pltpu.SemaphoreType.DMA((2, RING)),
                pltpu.SemaphoreType.DMA((15, ENV_PIECES)),
                pltpu.SemaphoreType.DMA((15, ENV_PIECES)),
                pltpu.SemaphoreType.DMA((2,)),
                pltpu.SemaphoreType.REGULAR,
                pltpu.SemaphoreType.REGULAR,
            ],
            compiler_params=pltpu.CompilerParams(
                collective_id=0, has_side_effects=True, vmem_limit_bytes=67043328),
        )(psi, left, right, mpo, spread_out, spread_in, same)
        result = out.reshape(n_s, n_u, local_cols, full_rows).transpose(3, 0, 1, 2)
        return scal[0, 1:, 0, 0], scal[1, 1:, 0, 0], result

    return jax.shard_map(
        local_run, mesh=grid,
        in_specs=(P(('x', 'k'), None, None, ('z', 'y')), P(('x', 'k'), None, None), P(('z', 'y'), None, None), P()),
        out_specs=(P(), P(), P(('x', 'k'), None, None, ('z', 'y'))), check_vma=False)
```
